32 devices in a mesh: dp: 16 (over z, y, core), mp: 2 (over x).
Axes of the slice: x: 2, y: 2, z: 4, core: 2. Of those that a mesh axis runs over, the one named last changes fastest.
Arguments:
- layer_input: bfloat16 [24576, 768], P('dp'), may hold values from -6 to 6
- doc_lengths: int32 [48, 8], P('dp'), may hold values from 1 to 256, 512 in all within a row
- q_weight: bfloat16 [768, 768], P(None, 'mp'), may hold values from -0.3125 to 0.3125
- q_bias: bfloat16 [768], P('mp'), may hold values from -3 to 3
- k_weight: bfloat16 [768, 768], P(None, 'mp'), may hold values from -0.3125 to 0.3125
- v_weight: bfloat16 [768, 768], P(None, 'mp'), may hold values from -0.21875 to 0.21875
- v_bias: bfloat16 [768], P('mp'), may hold values from -3 to 3
- out_weight: bfloat16 [768, 768], P('mp'), may hold values from -1.75 to 1.75
- out_bias: bfloat16 [768], replicated, may hold values from -3 to 3
- attn_gain: bfloat16 [768], replicated, may hold values from 0.5 to 1.5
- attn_shift: bfloat16 [768], replicated, may hold values from -3 to 3
- up_weight: bfloat16 [768, 3072], P(None, 'mp'), may hold values from -0.21875 to 0.21875
- up_bias: bfloat16 [3072], P('mp'), may hold values from -3 to 3
- down_weight: bfloat16 [3072, 768], P('mp'), may hold values from -0.109375 to 0.109375
- down_bias: bfloat16 [768], replicated, may hold values from -3 to 3
- ffn_gain: bfloat16 [768], replicated, may hold values from 0.5 to 1.5
- ffn_shift: bfloat16 [768], replicated, may hold values from -3 to 3
- cotangent: bfloat16 [24576, 768], P('dp'), may hold values from -6 to 6
Outputs:
- layer_output: bfloat16 [24576, 768], P('dp')
- input_grad: bfloat16 [24576, 768], P('dp')
- q_weight_grad: float32 [768, 768], P('dp', 'mp')
- q_bias_grad: float32 [768], P('mp')
- k_weight_grad: float32 [768, 768], P('dp', 'mp')
- v_weight_grad: float32 [768, 768], P('dp', 'mp')
- v_bias_grad: float32 [768], P('mp')
- out_weight_grad: float32 [768, 768], P('mp', 'dp')
- out_bias_grad: float32 [768], replicated
- attn_gain_grad: float32 [768], replicated
- attn_shift_grad: float32 [768], replicated
- up_weight_grad: float32 [768, 3072], P('dp', 'mp')
- up_bias_grad: float32 [3072], P('mp')
- down_weight_grad: float32 [3072, 768], P('mp', 'dp')
- down_bias_grad: float32 [768], replicated
- ffn_gain_grad: float32 [768], replicated
- ffn_shift_grad: float32 [768], replicated
The draws below stay inside these ranges and needn't reach their ends.
Inputs may be any that keep to these rules, and one draw needn't show every extreme that they name: Each row of doc_lengths sums to 512, and each row holds one document of exactly 256 tokens.
All inputs are finite; a program needn't handle non-finite values.
Results may differ from the reference program's by a relative error of at most 0.019.
Values may be sent and summed in bfloat16 or wider, within the bound.
A program may use at most 192 MiB of HBM per device.

```python
import math
import jax
import jax.numpy as jnp
import numpy as np
from jax import lax

D = 768
H = 12
HD = 64
FF = 3072
LEN = 512
DOCS = 8
HH = 768
MOST_DOC = 256
ROWS = 48
TOKENS = 24576
N_MP = 2


def shard_levels(own_key, extent, split, smallest, largest):
    def one(dim, parts):
        steps = jax.random.uniform(jax.random.fold_in(jax.random.fold_in(own_key, 6), dim), (parts,), jnp.float32, smallest / len(split), largest / len(split))
        return jnp.repeat(jnp.exp(steps), extent[dim] // parts).reshape((-1,) + (1,) * (len(extent) - dim - 1))

    level = one(*split[0])
    for cut in split[1:]:
        level = level * one(*cut)
    return level


def profile(count, total, reach, slope):
    weights = [(1 << 20) // math.isqrt(rank ** slope) + 1 for rank in range(2, count + 1)]
    spare, counts = total - reach - (count - 1), [1] * (count - 1)
    while spare > 0:
        candidates = [i for i in range(count - 1) if counts[i] < reach]
        whole, remaining = sum([weights[i] for i in candidates]), spare
        for i in candidates:
            more = min(reach - counts[i], max(1, remaining * weights[i] // whole), spare)
            counts[i] = counts[i] + more
            spare = spare - more
    return np.array([reach] + counts)


def uneven_parts(stream_key, number_of, total, reach, slope):
    if number_of == 2:
        one = jax.random.randint(stream_key, (), max(1, total - reach), min(reach, total - 1) + 1)
        return jnp.stack([one, total - one])
    sizes = jnp.asarray(profile(number_of, total, reach, slope), jnp.int32)
    pairs = (number_of - 1) // 2
    source_of, taker = sizes[1:1 + 2 * pairs:2], sizes[2:2 + 2 * pairs:2]
    room = jnp.minimum(source_of - 1, reach - taker)
    shifted = jax.random.randint(jax.random.fold_in(stream_key, 1), (pairs,), 0, 1 << 20) % (room + 1)
    sizes = sizes.at[1:1 + 2 * pairs:2].set(source_of - shifted).at[2:2 + 2 * pairs:2].set(taker + shifted)
    return sizes[jax.random.permutation(jax.random.fold_in(stream_key, 2), number_of)]


def normal_values(rng, shape, deviation, most, pieces=(), kind=jnp.bfloat16):
    array = deviation * jax.random.normal(rng, shape, jnp.float32)
    if pieces:
        array = array * shard_levels(rng, shape, pieces, -0.22, 0.18)
    return jnp.clip(array, -most, most).astype(kind)


def setup_inputs(seed: int = 0) -> dict:
    streams_of = jax.random.split(jax.random.key(seed), 19)
    layer_input = normal_values(streams_of[0], (TOKENS, D), 1.0, 6.0, ((0, 16),))
    doc_lengths = jax.vmap(lambda own: uneven_parts(own, DOCS, LEN, MOST_DOC, 2))(jax.random.split(streams_of[1], ROWS)).reshape((ROWS, DOCS)).astype(jnp.int32)
    q_weight = normal_values(streams_of[2], (D, HH), (D // 2) ** -0.5, 0.3125, ((1, 2),))
    q_bias = normal_values(streams_of[3], (HH,), 0.5, 3.0, ((0, 2),))
    k_weight = normal_values(streams_of[4], (D, HH), (D // 2) ** -0.5, 0.3125, ((1, 2),))
    v_weight = normal_values(streams_of[5], (D, HH), D ** -0.5, 0.21875, ((1, 2),))
    v_bias = normal_values(streams_of[6], (HH,), 0.5, 3.0, ((0, 2),))
    out_weight = normal_values(streams_of[7], (HH, D), (max(HH // 64, 1)) ** -0.5, 1.75, ((0, 2),))
    out_bias = normal_values(streams_of[8], (D,), 0.5, 3.0)
    attn_gain = jnp.clip(1.0 + 0.1 * jax.random.normal(streams_of[9], (D,), jnp.float32), 0.5, 1.5).astype(jnp.bfloat16)
    attn_shift = normal_values(streams_of[10], (D,), 0.5, 3.0)
    up_weight = normal_values(streams_of[11], (D, FF), D ** -0.5, 0.21875, ((1, 2),))
    up_bias = normal_values(streams_of[12], (FF,), 0.5, 3.0, ((0, 2),))
    down_weight = normal_values(streams_of[13], (FF, D), FF ** -0.5, 0.109375, ((0, 2),))
    down_bias = normal_values(streams_of[14], (D,), 0.5, 3.0)
    ffn_gain = jnp.clip(1.0 + 0.1 * jax.random.normal(streams_of[15], (D,), jnp.float32), 0.5, 1.5).astype(jnp.bfloat16)
    ffn_shift = normal_values(streams_of[16], (D,), 0.5, 3.0)
    cotangent = normal_values(streams_of[17], (TOKENS, D), 1.0, 6.0, ((0, 16),))
    return dict(layer_input=layer_input, doc_lengths=doc_lengths, q_weight=q_weight, q_bias=q_bias, k_weight=k_weight, v_weight=v_weight, v_bias=v_bias, out_weight=out_weight, out_bias=out_bias, attn_gain=attn_gain, attn_shift=attn_shift, up_weight=up_weight, up_bias=up_bias, down_weight=down_weight, down_bias=down_bias, ffn_gain=ffn_gain, ffn_shift=ffn_shift, cotangent=cotangent)


@jax.custom_vjp
def low(v):
    return lax.optimization_barrier(v.astype(jnp.bfloat16)).astype(jnp.float32)

@jax.custom_vjp
def low_back(v):
    return v

def low_keep(v):
    return (low(v), None)

def low_pass(kept, grad):
    return (grad,)

def back_keep(v):
    return (v, None)

def back_low(kept, grad):
    return (low(grad),)
low.defvjp(low_keep, low_pass)
low_back.defvjp(back_keep, back_low)
EPS = 1e-12
GELU_C = 0.7978845608028654
HIGH = lax.Precision.HIGHEST

def matmul(a, b):
    return jnp.dot(a, b, precision=HIGH, preferred_element_type=jnp.float32)

def layer_norm(v, gain, shift):
    mean = lax.optimization_barrier(jnp.mean(v, -1, keepdims=True))
    centred = v - mean
    var = lax.optimization_barrier(jnp.mean(centred * centred, -1, keepdims=True))
    return centred * lax.rsqrt(var + EPS) * gain + shift

def gelu_new(v):
    return 0.5 * v * (1.0 + jnp.tanh(GELU_C * (v + 0.044715 * v * v * v)))

def same_doc(lengths):
    ends = jnp.cumsum(lengths, axis=-1, dtype=jnp.int32)
    place = jnp.arange(LEN, dtype=jnp.int32)
    segment = lax.optimization_barrier(jnp.sum((place[None, :, None] >= ends[:, None, :]).astype(jnp.int32), -1, dtype=jnp.int32))
    return segment[:, :, None] == segment[:, None, :]

def forward(inputs, params, mask):
    q_weight, q_bias, k_weight, v_weight, v_bias, out_weight, out_bias, attn_gain, attn_shift, up_weight, up_bias, down_weight, down_bias, ffn_gain, ffn_shift = params
    rows = mask.shape[0]
    query = low_back(low(0.125 * (matmul(inputs, q_weight) + q_bias)))
    key = low_back(low(matmul(inputs, k_weight)))
    value = low_back(low(matmul(inputs, v_weight) + v_bias))
    query = query.reshape(rows, LEN, H, HD)
    key = key.reshape(rows, LEN, H, HD)
    value = value.reshape(rows, LEN, H, HD)
    scores = low_back(jnp.einsum('rqhd,rkhd->rhqk', query, key, precision=HIGH))
    scores = jnp.where(mask[:, None], scores, -1000000000.0)
    top = lax.optimization_barrier(jnp.max(scores, -1, keepdims=True))
    expo = jnp.exp(scores - top)
    probs = expo / lax.optimization_barrier(jnp.sum(expo, -1, keepdims=True))
    context = jnp.einsum('rhqk,rkhd->rqhd', low(probs), value, precision=HIGH)
    context = low_back(low(context.reshape(rows * LEN, HH)))
    group = HH // N_MP
    attn = low(matmul(context[:, :group], out_weight[:group]))
    for index in range(1, N_MP):
        attn = attn + low(matmul(context[:, index * group:(index + 1) * group], out_weight[index * group:(index + 1) * group]))
    resid1 = inputs + low_back(attn) + out_bias
    normed1 = layer_norm(resid1, attn_gain, attn_shift)
    normed_low = low(normed1)
    upper = low_back(matmul(normed_low, up_weight)) + up_bias
    act = low(gelu_new(upper))
    width = FF // N_MP
    ffn = low(matmul(act[:, :width], down_weight[:width]))
    for index in range(1, N_MP):
        ffn = ffn + low(matmul(act[:, index * width:(index + 1) * width], down_weight[index * width:(index + 1) * width]))
    resid2 = normed1 + low_back(ffn) + down_bias
    return layer_norm(resid2, ffn_gain, ffn_shift)

def reference(layer_input, doc_lengths, q_weight, q_bias, k_weight, v_weight, v_bias, out_weight, out_bias, attn_gain, attn_shift, up_weight, up_bias, down_weight, down_bias, ffn_gain, ffn_shift, cotangent):
    params = tuple((a.astype(jnp.float32) for a in (q_weight, q_bias, k_weight, v_weight, v_bias, out_weight, out_bias, attn_gain, attn_shift, up_weight, up_bias, down_weight, down_bias, ffn_gain, ffn_shift)))
    group_rows = 8
    count = ROWS // group_rows
    inputs = layer_input.astype(jnp.float32).reshape(count, group_rows * LEN, D)
    grads_in = cotangent.astype(jnp.float32).reshape(count, group_rows * LEN, D)
    lengths = doc_lengths.reshape(count, group_rows, DOCS)

    def step(carry, item):
        block_in, block_len, block_grad = item
        mask = same_doc(block_len)
        result, pull = jax.vjp(lambda a, p: forward(a, p, mask), block_in, params)
        grad_in, grad_params = pull(block_grad)
        carry = tuple((c + g for c, g in zip(carry, grad_params)))
        return (carry, (result.astype(jnp.bfloat16), grad_in.astype(jnp.bfloat16)))
    start = tuple((jnp.zeros_like(p) for p in params))
    totals, (results, grad_inputs) = lax.scan(step, start, (inputs, lengths, grads_in))
    layer_output = results.reshape(TOKENS, D)
    input_grad = grad_inputs.reshape(TOKENS, D)
    return (layer_output, input_grad, totals[0], totals[1], totals[2], totals[3], totals[4], totals[5], totals[6], totals[7], totals[8], totals[9], totals[10], totals[11], totals[12], totals[13], totals[14])
```

```python
import functools

import jax
import jax.numpy as jnp
from jax import lax
from jax.experimental import pallas as pl
from jax.experimental.pallas import tpu as pltpu
from jax.sharding import PartitionSpec as P

HD = 64
PAIR = 2 * HD
EPS = 1e-12
GELU_C = 0.7978845608028654
F32 = jnp.float32
BF16 = jnp.bfloat16
CHUNK = 512
VMEM_LIMIT = 60 * 1024 * 1024


def mm(a, b):
    return jnp.dot(a, b, preferred_element_type=F32)


def mm_t(a, b):
    return lax.dot_general(a, b, (((1,), (1,)), ((), ())), preferred_element_type=F32)


def t_mm(a, b):
    return lax.dot_general(a, b, (((0,), (0,)), ((), ())), preferred_element_type=F32)


def halves(v):
    lane = lax.broadcasted_iota(jnp.int32, v.shape, 1)
    zero = jnp.zeros_like(v)
    return jnp.where(lane < HD, v, zero), jnp.where(lane < HD, zero, v)


def attention_forward(
    x_ref, w_ref, b_ref, wo_ref, seg_c_ref, seg_r_ref, bo_ref, gain_ref, shift_ref,
    qkv_ref, p_ref, ctx_ref, xhat_ref, rstd_ref, low_ref,
):
    seqs, length = seg_c_ref.shape[0], seg_c_ref.shape[1]
    groups, width = wo_ref.shape[0], wo_ref.shape[1]
    pairs = width // PAIR

    @pl.loop(0, seqs)
    def _(s):
        rows = pl.ds(pl.multiple_of(s * length, length), length)
        x = x_ref[rows, :]
        mask = seg_c_ref[s] == seg_r_ref[s]
        attn = x.astype(F32) + bo_ref[...]
        for g in range(groups):
            y = mm(x, w_ref[g]) + b_ref[g]
            query = (0.125 * y[:, :width]).astype(BF16)
            key = y[:, width : 2 * width].astype(BF16)
            value = y[:, 2 * width :].astype(BF16)
            qkv_ref[g, rows, :width] = query
            qkv_ref[g, rows, width : 2 * width] = key
            qkv_ref[g, rows, 2 * width :] = value
            parts = []
            for p in range(pairs):
                at = slice(p * PAIR, (p + 1) * PAIR)
                k = key[:, at]
                both = None
                for h, (q, v) in enumerate(zip(halves(query[:, at]), halves(value[:, at]))):
                    scores = jnp.where(mask, mm_t(q, k), -1000000000.0)
                    expo = jnp.exp(scores - jnp.max(scores, -1, keepdims=True))
                    probs = (expo * (1.0 / jnp.sum(expo, -1, keepdims=True))).astype(BF16)
                    p_ref[s, (g * pairs + p) * 2 + h] = probs
                    part = mm(probs, v)
                    both = part if both is None else both + part
                parts.append(both.astype(BF16))
            ctx = jnp.concatenate(parts, 1)
            ctx_ref[g, rows, :] = ctx
            attn = attn + mm(ctx, wo_ref[g])
        mean = jnp.mean(attn, -1, keepdims=True)
        centred = attn - mean
        rstd = lax.rsqrt(jnp.mean(centred * centred, -1, keepdims=True) + EPS)
        xhat = centred * rstd
        xhat_ref[rows, :] = xhat
        rstd_ref[rows, :] = rstd
        low_ref[rows, :] = (xhat * gain_ref[...] + shift_ref[...]).astype(BF16)


def norm_backward(xhat, rstd, gain, grad):
    scaled = grad * gain
    return rstd * (
        scaled
        - jnp.mean(scaled, -1, keepdims=True)
        - xhat * jnp.mean(scaled * xhat, -1, keepdims=True)
    )


def feed_forward(
    low_ref, xhat_ref, rstd_ref, up_ref, ub_ref, down_ref, vec_ref, cot_ref,
    out_ref, gd_ref, gu_ref, d_resid_ref, small_ref, ubg_ref,
    act_ref, slope_ref, acc_ref, dffn_ref, dffn_t_ref, low_t_ref,
):
    tokens, width = low_ref.shape
    groups, hidden = up_ref.shape[0], up_ref.shape[2]
    step = min(CHUNK, hidden)
    per = hidden // step
    block = 256
    low_t_ref[...] = low_ref[...].T
    acc_ref[...] = jnp.zeros_like(acc_ref)

    @pl.loop(0, groups * per)
    def _(i):
        g = i // per
        at = pl.ds(pl.multiple_of((i % per) * step, step), step)

        @pl.loop(0, tokens // block)
        def _(b):
            rows = pl.ds(pl.multiple_of(b * block, block), block)
            u = mm(low_ref[rows, :], up_ref[g, :, at]) + ub_ref[g, :, at]
            square = u * u
            t = jnp.tanh(GELU_C * (u + 0.044715 * square * u))
            half = 0.5 * (1.0 + t)
            act = (u * half).astype(BF16)
            act_ref[g, rows, at] = act
            slope = half + (0.5 * GELU_C) * u * (1.0 - t * t) * (1.0 + 0.134145 * square)
            slope_ref[g, rows, at] = slope.astype(BF16)
            acc_ref[rows, :] += mm(act, down_ref[g, at, :])

    small_ref[...] = jnp.zeros_like(small_ref)
    attn_gain, attn_shift = vec_ref[0:1, :], vec_ref[1:2, :]
    down_bias = vec_ref[2:3, :]
    ffn_gain, ffn_shift = vec_ref[3:4, :], vec_ref[4:5, :]

    @pl.loop(0, tokens // block)
    def _(b):
        rows = pl.ds(pl.multiple_of(b * block, block), block)
        resid = xhat_ref[rows, :] * attn_gain + attn_shift + acc_ref[rows, :] + down_bias
        centred = resid - jnp.mean(resid, -1, keepdims=True)
        rstd = lax.rsqrt(jnp.mean(centred * centred, -1, keepdims=True) + EPS)
        xhat = centred * rstd
        out_ref[rows, :] = (xhat * ffn_gain + ffn_shift).astype(BF16)
        cot = cot_ref[rows, :].astype(F32)
        grad = norm_backward(xhat, rstd, ffn_gain, cot)
        acc_ref[rows, :] = grad
        dffn_ref[rows, :] = grad.astype(BF16)
        small_ref[3:4, :] += jnp.sum(grad, 0, keepdims=True)
        small_ref[4:5, :] += jnp.sum(cot * xhat, 0, keepdims=True)
        small_ref[5:6, :] += jnp.sum(cot, 0, keepdims=True)

    dffn_t_ref[...] = dffn_ref[...].T

    @pl.loop(0, groups * per)
    def _(i):
        g = i // per
        at = pl.ds(pl.multiple_of((i % per) * step, step), step)
        total = jnp.zeros((1, step), F32)
        for b in range(tokens // block):
            rows = slice(b * block, (b + 1) * block)
            d_upper = mm_t(dffn_ref[rows, :], down_ref[g, at, :]) * slope_ref[g, rows, at].astype(F32)
            total = total + jnp.sum(d_upper, 0, keepdims=True)
            d_low = d_upper.astype(BF16)
            slope_ref[g, rows, at] = d_low
            acc_ref[rows, :] += mm_t(d_low, up_ref[g, :, at])
        ubg_ref[g, :, at] = total
        for b in range(width // block):
            rows = slice(b * block, (b + 1) * block)
            gd_ref[g, rows, at] = mm(dffn_t_ref[rows, :], act_ref[g, :, at]).astype(BF16)
            gu_ref[g, rows, at] = mm(low_t_ref[rows, :], slope_ref[g, :, at]).astype(BF16)

    @pl.loop(0, tokens // block)
    def _(b):
        rows = pl.ds(pl.multiple_of(b * block, block), block)
        d_normed = acc_ref[rows, :]
        xhat = xhat_ref[rows, :]
        grad = norm_backward(xhat, rstd_ref[rows, :], attn_gain, d_normed)
        d_resid_ref[rows, :] = grad
        small_ref[0:1, :] += jnp.sum(grad, 0, keepdims=True)
        small_ref[1:2, :] += jnp.sum(d_normed * xhat, 0, keepdims=True)
        small_ref[2:3, :] += jnp.sum(d_normed, 0, keepdims=True)


def attention_backward(
    x_ref, d_resid_ref, w_ref, wo_ref, qkv_ref, p_ref, ctx_ref,
    in_ref, gq_ref, go_ref, bg_ref,
    dq_ref, dattn_t_ref, x_t_ref,
):
    seqs, length = p_ref.shape[0], p_ref.shape[2]
    groups, width = wo_ref.shape[0], wo_ref.shape[1]
    model = x_ref.shape[1]
    pairs = width // PAIR
    block = 256
    x_t_ref[...] = x_ref[...].T

    @pl.loop(0, seqs)
    def _(s):
        rows = pl.ds(pl.multiple_of(s * length, length), length)
        d_resid = d_resid_ref[rows, :]
        d_attn = d_resid.astype(BF16)
        dattn_t_ref[:, rows] = d_attn.T
        total = d_resid
        for g in range(groups):
            d_ctx = mm_t(d_attn, wo_ref[g]).astype(BF16)
            for p in range(pairs):
                at = slice(p * PAIR, (p + 1) * PAIR)
                q_at, k_at, v_at = (slice(o * width + p * PAIR, o * width + (p + 1) * PAIR) for o in range(3))
                value = qkv_ref[g, rows, v_at]
                q_pair = halves(qkv_ref[g, rows, q_at])
                k_pair = halves(qkv_ref[g, rows, k_at])
                c_pair = halves(d_ctx[:, at])
                dq = dk = dv = None
                for h in range(2):
                    low = p_ref[s, (g * pairs + p) * 2 + h]
                    probs = low.astype(F32)
                    d_probs = mm_t(c_pair[h], value)
                    inner = jnp.sum(probs * d_probs, -1, keepdims=True)
                    d_scores = (probs * (d_probs - inner)).astype(BF16)
                    dv_h = t_mm(low, c_pair[h])
                    dq_h = mm(d_scores, k_pair[h])
                    dk_h = t_mm(d_scores, q_pair[h])
                    dq = dq_h if dq is None else dq + dq_h
                    dk = dk_h if dk is None else dk + dk_h
                    dv = dv_h if dv is None else dv + dv_h
                dq_ref[g, rows, q_at] = (0.125 * dq).astype(BF16)
                dq_ref[g, rows, k_at] = dk.astype(BF16)
                dq_ref[g, rows, v_at] = dv.astype(BF16)
            total = total + mm_t(dq_ref[g, rows, :], w_ref[g])
        in_ref[rows, :] = total.astype(BF16)

    for g in range(groups):
        bg_ref[g] = jnp.sum(dq_ref[g].astype(F32), 0, keepdims=True)

        @pl.loop(0, model // block)
        def _(b):
            rows = pl.ds(pl.multiple_of(b * block, block), block)
            gq_ref[g, rows, :] = mm(x_t_ref[rows, :], dq_ref[g]).astype(BF16)
            go_ref[g, rows, :] = mm(dattn_t_ref[rows, :], ctx_ref[g]).astype(BF16)


def call(kernel, outs, scratch, flops, *args):
    shapes = [jax.ShapeDtypeStruct(s, d) for s, d in outs]
    moved = sum(a.size * a.dtype.itemsize for a in args) + sum(s.size * s.dtype.itemsize for s in shapes)
    vmem = pl.BlockSpec(memory_space=pltpu.VMEM)
    return pl.pallas_call(
        kernel,
        out_shape=shapes,
        in_specs=[vmem] * len(args),
        out_specs=[vmem] * len(shapes),
        scratch_shapes=[pltpu.VMEM(s, d) for s, d in scratch],
        compiler_params=pltpu.CompilerParams(vmem_limit_bytes=VMEM_LIMIT),
        cost_estimate=pl.CostEstimate(flops=flops, bytes_accessed=moved, transcendentals=0),
    )(*args)


def factors_of(n):
    found = []
    while n > 4 or (n > 1 and len(found) < 2):
        found.append(2)
        n //= 2
    return found + ([n] if n > 1 else [])


def swap(v):
    return lax.ppermute(v, "mp", [(0, 1), (1, 0)])


def shift_dp(v, n, stride, factor, k):
    def target(d):
        i = (d // stride) % factor
        return d + ((i + k) % factor - i) * stride

    return lax.ppermute(v, "dp", [(d, target(d)) for d in range(n)])


def with_peer(own, n):
    core = lax.axis_index("dp") % 2
    half = own.shape[0] // 2
    mine = swap(lax.dynamic_slice_in_dim(own, core * half, half, 0))
    other = shift_dp(mine, n, 1, 2, 1)
    first = core == 0
    peer = jnp.concatenate([jnp.where(first, mine, other), jnp.where(first, other, mine)], 0)
    return jnp.stack([own, peer])


def reduce_to_owner(grad, n):
    index = lax.axis_index("dp")
    rows = grad.shape[1] // n
    left = grad.reshape(2, n, rows, grad.shape[2])
    stride = 1
    for factor in factors_of(n):
        parts = left.reshape(2, left.shape[1] // factor, factor, rows, left.shape[3])
        i = (index // stride) % factor

        def pick(at):
            return lax.dynamic_index_in_dim(parts, at, 2, keepdims=False)

        total = pick(i).astype(F32)
        for k in range(1, factor):
            total = total + shift_dp(pick((i + k) % factor), n, stride, factor, k).astype(F32)
        left = total.astype(BF16)
        stride *= factor
    left = left.reshape(2, rows, left.shape[3])
    return left[0].astype(F32) + swap(left[1]).astype(F32)


def per_device(
    n, layer_input, doc_lengths, q_weight, q_bias, k_weight, v_weight, v_bias, out_weight, out_bias,
    attn_gain, attn_shift, up_weight, up_bias, down_weight, down_bias, ffn_gain, ffn_shift, cotangent,
):
    rows = doc_lengths.shape[0]
    tokens, model = layer_input.shape
    length = tokens // rows
    part = length // 2
    mine = rows * part
    width = q_weight.shape[1]
    hidden = up_weight.shape[1]
    heads = width // HD
    x_index = lax.axis_index("mp")

    ends = jnp.cumsum(doc_lengths, axis=-1, dtype=jnp.int32)
    start = jnp.sum(jnp.where(doc_lengths == part, ends - part, 0), -1)
    place = jnp.arange(length, dtype=jnp.int32)
    segment = jnp.sum((place[None, :, None] >= ends[:, None, :]).astype(jnp.int32), -1, dtype=jnp.int32)
    before = place[None, :part] < start[:, None]
    from_high = before != (x_index == 1)

    def take(v):
        v = v.reshape(rows, 2, part, model)
        return jnp.where(from_high[:, :, None], v[:, 1], v[:, 0]).reshape(mine, model)

    def give(own):
        own = own.reshape(rows, part, model)
        other = swap(own)
        low = jnp.where(from_high[:, :, None], other, own)
        high = jnp.where(from_high[:, :, None], own, other)
        return jnp.stack([low, high], 1).reshape(tokens, model)

    seg = jnp.where(from_high, segment[:, part:], segment[:, :part])

    w_qkv = with_peer(jnp.concatenate([q_weight, k_weight, v_weight], 1), n)
    w_out = with_peer(out_weight, n)
    w_up = with_peer(up_weight, n)
    w_down = with_peer(down_weight, n)
    own_bias = jnp.concatenate([q_bias, v_bias, up_bias])
    bias = jnp.stack([own_bias, swap(own_bias)]).astype(F32)[:, None, :]
    b_qkv = jnp.concatenate([bias[..., :width], jnp.zeros_like(bias[..., :width]), bias[..., width : 2 * width]], -1)
    b_up = bias[..., 2 * width :]
    vectors = jnp.stack([attn_gain, attn_shift, down_bias, ffn_gain, ffn_shift]).astype(F32)

    x = take(layer_input)
    cot = take(cotangent)
    qkv, probs, ctx, xhat, rstd, low = call(
        attention_forward,
        [
            ((2, mine, 3 * width), BF16),
            ((rows, 2 * heads, part, part), BF16),
            ((2, mine, width), BF16),
            ((mine, model), F32),
            ((mine, 1), F32),
            ((mine, model), BF16),
        ],
        [],
        2 * mine * model * 8 * width,
        x, w_qkv, b_qkv, w_out, seg[:, :, None], seg[:, None, :],
        out_bias.astype(F32)[None], vectors[0:1], vectors[1:2],
    )
    output, g_down, g_up, d_resid, small, up_bias_grad = call(
        feed_forward,
        [
            ((mine, model), BF16),
            ((2, model, hidden), BF16),
            ((2, model, hidden), BF16),
            ((mine, model), F32),
            ((8, model), F32),
            ((2, 1, hidden), F32),
        ],
        [
            ((2, mine, hidden), BF16),
            ((2, mine, hidden), BF16),
            ((mine, model), F32),
            ((mine, model), BF16),
            ((model, mine), BF16),
            ((model, mine), BF16),
        ],
        2 * mine * model * 2 * hidden * 6,
        low, xhat, rstd, w_up, b_up, w_down, vectors, cot,
    )
    layer_output = give(output)
    down_weight_grad = reduce_to_owner(g_down, n).T
    up_weight_grad = reduce_to_owner(g_up, n)
    grad_in, g_qkv, g_out, bias_grad = call(
        attention_backward,
        [
            ((mine, model), BF16),
            ((2, model, 3 * width), BF16),
            ((2, model, width), BF16),
            ((2, 1, 3 * width), F32),
        ],
        [((2, mine, 3 * width), BF16), ((model, mine), BF16), ((model, mine), BF16)],
        2 * mine * model * 16 * width,
        x, d_resid, w_qkv, w_out, qkv, probs, ctx,
    )
    input_grad = give(grad_in)
    g_attn = reduce_to_owner(jnp.concatenate([g_qkv, g_out], -1), n)
    sums = jnp.concatenate([bias_grad[:, 0, :width], bias_grad[:, 0, 2 * width :], up_bias_grad[:, 0]], -1)
    sums = jnp.where(x_index == 0, sums, sums[::-1])
    sums, small = lax.psum((sums, small), ("dp", "mp"))
    sums = lax.dynamic_index_in_dim(sums, x_index, 0, keepdims=False)
    return (
        layer_output,
        input_grad,
        g_attn[:, :width],
        sums[:width],
        g_attn[:, width : 2 * width],
        g_attn[:, 2 * width : 3 * width],
        sums[width : 2 * width],
        g_attn[:, 3 * width :].T,
        small[0],
        small[1],
        small[2],
        up_weight_grad,
        sums[2 * width :],
        down_weight_grad,
        small[3],
        small[4],
        small[5],
    )


def solution(mesh):
    in_specs = (
        P("dp", None), P("dp", None), P(None, "mp"), P("mp"), P(None, "mp"), P(None, "mp"), P("mp"),
        P("mp", None), P(), P(), P(), P(None, "mp"), P("mp"), P("mp", None), P(), P(), P(), P("dp", None),
    )
    out_specs = (
        P("dp", None), P("dp", None), P("dp", "mp"), P("mp"), P("dp", "mp"), P("dp", "mp"), P("mp"),
        P("mp", "dp"), P(), P(), P(), P("dp", "mp"), P("mp"), P("mp", "dp"), P(), P(), P(),
    )
    return jax.shard_map(
        functools.partial(per_device, mesh.shape["dp"]),
        mesh=mesh, in_specs=in_specs, out_specs=out_specs, check_vma=False,
    )
```

```python
import functools

import jax
import jax.numpy as jnp
from jax import lax
from jax.experimental import pallas as pl
from jax.experimental.pallas import tpu as pltpu
from jax.sharding import PartitionSpec as P

HD = 64
PAIR = 2 * HD
EPS = 1e-12
GELU_C = 0.7978845608028654
F32 = jnp.float32
BF16 = jnp.bfloat16
CHUNK = 512
VMEM_LIMIT = 60 * 1024 * 1024
MESH = pl.DeviceIdType.MESH


def mm(a, b):
    return jnp.dot(a, b, preferred_element_type=F32)


def mm_t(a, b):
    return lax.dot_general(a, b, (((1,), (1,)), ((), ())), preferred_element_type=F32)


def t_mm(a, b):
    return lax.dot_general(a, b, (((0,), (0,)), ((), ())), preferred_element_type=F32)


def halves(v):
    lane = lax.broadcasted_iota(jnp.int32, v.shape, 1)
    zero = jnp.zeros_like(v)
    return jnp.where(lane < HD, v, zero), jnp.where(lane < HD, zero, v)


def attention_forward(
    x_ref, w_ref, b_ref, wo_ref, seg_c_ref, seg_r_ref, bo_ref, gain_ref, shift_ref,
    qkv_ref, p_ref, ctx_ref, xhat_ref, rstd_ref, low_ref,
):
    seqs, length = seg_c_ref.shape[0], seg_c_ref.shape[1]
    groups, width = wo_ref.shape[0], wo_ref.shape[1]
    pairs = width // PAIR

    @pl.loop(0, seqs)
    def _(s):
        rows = pl.ds(pl.multiple_of(s * length, length), length)
        x = x_ref[rows, :]
        mask = seg_c_ref[s] == seg_r_ref[s]
        attn = x.astype(F32) + bo_ref[...]
        for g in range(groups):
            y = mm(x, w_ref[g]) + b_ref[g]
            query = (0.125 * y[:, :width]).astype(BF16)
            key = y[:, width : 2 * width].astype(BF16)
            value = y[:, 2 * width :].astype(BF16)
            qkv_ref[g, rows, :width] = query
            qkv_ref[g, rows, width : 2 * width] = key
            qkv_ref[g, rows, 2 * width :] = value
            parts = []
            for p in range(pairs):
                at = slice(p * PAIR, (p + 1) * PAIR)
                k = key[:, at]
                both = None
                for h, (q, v) in enumerate(zip(halves(query[:, at]), halves(value[:, at]))):
                    scores = jnp.where(mask, mm_t(q, k), -1000000000.0)
                    expo = jnp.exp(scores - jnp.max(scores, -1, keepdims=True))
                    probs = (expo * (1.0 / jnp.sum(expo, -1, keepdims=True))).astype(BF16)
                    p_ref[s, (g * pairs + p) * 2 + h] = probs
                    part = mm(probs, v)
                    both = part if both is None else both + part
                parts.append(both.astype(BF16))
            ctx = jnp.concatenate(parts, 1)
            ctx_ref[g, rows, :] = ctx
            attn = attn + mm(ctx, wo_ref[g])
        mean = jnp.mean(attn, -1, keepdims=True)
        centred = attn - mean
        rstd = lax.rsqrt(jnp.mean(centred * centred, -1, keepdims=True) + EPS)
        xhat = centred * rstd
        xhat_ref[rows, :] = xhat
        rstd_ref[rows, :] = rstd
        low_ref[rows, :] = (xhat * gain_ref[...] + shift_ref[...]).astype(BF16)


def norm_backward(xhat, rstd, gain, grad):
    scaled = grad * gain
    return rstd * (
        scaled
        - jnp.mean(scaled, -1, keepdims=True)
        - xhat * jnp.mean(scaled * xhat, -1, keepdims=True)
    )


def add_rows(dst, src, offset, step):
    step = min(step, dst.shape[0])

    @pl.loop(0, dst.shape[0] // step)
    def _(i):
        here = pl.ds(pl.multiple_of(i * step, step), step)
        there = pl.ds(pl.multiple_of(offset + i * step, step), step)
        dst[here, :] = (dst[here, :].astype(F32) + src[there, :].astype(F32)).astype(dst.dtype)


def store_by_owner(dst, value, at, n):
    rows = value.shape[0] // n
    for d in range(n):
        place = (d % 2) * (n // 2) + (d // 2 % 2) * (n // 4) + d // 4
        dst[place * rows : (place + 1) * rows, at] = value[d * rows : (d + 1) * rows, :]


def feed_forward(
    n, low_ref, xhat_ref, rstd_ref, up_ref, ub_ref, down_ref, vec_ref, cot_ref,
    out_ref, gd_ref, gu_ref, d_resid_ref, small_ref, ubg_ref,
    act_ref, slope_ref, acc_ref, dffn_ref, dffn_t_ref, low_t_ref,
):
    tokens, width = low_ref.shape
    groups, hidden = up_ref.shape[0], up_ref.shape[2]
    step = min(CHUNK, hidden)
    per = hidden // step
    block = 256
    def put(dst, v):
        if n:
            store_by_owner(dst, v, slice(None), n)
        else:
            dst[...] = v

    put(low_t_ref, low_ref[...].T)
    acc_ref[...] = jnp.zeros_like(acc_ref)

    @pl.loop(0, groups * per)
    def _(i):
        g = i // per
        at = pl.ds(pl.multiple_of((i % per) * step, step), step)

        @pl.loop(0, tokens // block)
        def _(b):
            rows = pl.ds(pl.multiple_of(b * block, block), block)
            u = mm(low_ref[rows, :], up_ref[g, :, at]) + ub_ref[g, :, at]
            square = u * u
            t = jnp.tanh(GELU_C * (u + 0.044715 * square * u))
            half = 0.5 * (1.0 + t)
            act = (u * half).astype(BF16)
            act_ref[g, rows, at] = act
            slope = half + (0.5 * GELU_C) * u * (1.0 - t * t) * (1.0 + 0.134145 * square)
            slope_ref[g, rows, at] = slope.astype(BF16)
            acc_ref[rows, :] += mm(act, down_ref[g, at, :])

    small_ref[...] = jnp.zeros_like(small_ref)
    attn_gain, attn_shift = vec_ref[0:1, :], vec_ref[1:2, :]
    down_bias = vec_ref[2:3, :]
    ffn_gain, ffn_shift = vec_ref[3:4, :], vec_ref[4:5, :]

    @pl.loop(0, tokens // block)
    def _(b):
        rows = pl.ds(pl.multiple_of(b * block, block), block)
        resid = xhat_ref[rows, :] * attn_gain + attn_shift + acc_ref[rows, :] + down_bias
        centred = resid - jnp.mean(resid, -1, keepdims=True)
        rstd = lax.rsqrt(jnp.mean(centred * centred, -1, keepdims=True) + EPS)
        xhat = centred * rstd
        out_ref[rows, :] = (xhat * ffn_gain + ffn_shift).astype(BF16)
        cot = cot_ref[rows, :].astype(F32)
        grad = norm_backward(xhat, rstd, ffn_gain, cot)
        acc_ref[rows, :] = grad
        dffn_ref[rows, :] = grad.astype(BF16)
        small_ref[3:4, :] += jnp.sum(grad, 0, keepdims=True)
        small_ref[4:5, :] += jnp.sum(cot * xhat, 0, keepdims=True)
        small_ref[5:6, :] += jnp.sum(cot, 0, keepdims=True)

    put(dffn_t_ref, dffn_ref[...].T)

    @pl.loop(0, groups * per)
    def _(i):
        g = i // per
        at = pl.ds(pl.multiple_of((i % per) * step, step), step)
        total = jnp.zeros((1, step), F32)
        for b in range(tokens // block):
            rows = slice(b * block, (b + 1) * block)
            d_upper = mm_t(dffn_ref[rows, :], down_ref[g, at, :]) * slope_ref[g, rows, at].astype(F32)
            total = total + jnp.sum(d_upper, 0, keepdims=True)
            d_low = d_upper.astype(BF16)
            slope_ref[g, rows, at] = d_low
            acc_ref[rows, :] += mm_t(d_low, up_ref[g, :, at])
        ubg_ref[g, :, at] = total
        for b in range(width // block):
            rows = slice(b * block, (b + 1) * block)
            gd_ref[g, rows, at] = mm(dffn_t_ref[rows, :], act_ref[g, :, at]).astype(BF16)
            gu_ref[g, rows, at] = mm(low_t_ref[rows, :], slope_ref[g, :, at]).astype(BF16)

    @pl.loop(0, tokens // block)
    def _(b):
        rows = pl.ds(pl.multiple_of(b * block, block), block)
        d_normed = acc_ref[rows, :]
        xhat = xhat_ref[rows, :]
        grad = norm_backward(xhat, rstd_ref[rows, :], attn_gain, d_normed)
        d_resid_ref[rows, :] = grad
        small_ref[0:1, :] += jnp.sum(grad, 0, keepdims=True)
        small_ref[1:2, :] += jnp.sum(d_normed * xhat, 0, keepdims=True)
        small_ref[2:3, :] += jnp.sum(d_normed, 0, keepdims=True)


def backward_sequence(s, put, d_resid_ref, w_ref, wo_ref, qkv_ref, p_ref, in_ref, dq_ref):
    length, groups, width = p_ref.shape[2], wo_ref.shape[0], wo_ref.shape[1]
    pairs = width // PAIR
    rows = pl.ds(pl.multiple_of(s * length, length), length)
    d_resid = d_resid_ref[rows, :]
    d_attn = d_resid.astype(BF16)
    put(d_attn.T, rows)
    total = d_resid
    for g in range(groups):
        d_ctx = mm_t(d_attn, wo_ref[g]).astype(BF16)
        for p in range(pairs):
            at = slice(p * PAIR, (p + 1) * PAIR)
            q_at, k_at, v_at = (slice(o * width + p * PAIR, o * width + (p + 1) * PAIR) for o in range(3))
            value = qkv_ref[g, rows, v_at]
            q_pair = halves(qkv_ref[g, rows, q_at])
            k_pair = halves(qkv_ref[g, rows, k_at])
            c_pair = halves(d_ctx[:, at])
            dq = dk = dv = None
            for h in range(2):
                low = p_ref[s, (g * pairs + p) * 2 + h]
                probs = low.astype(F32)
                d_probs = mm_t(c_pair[h], value)
                inner = jnp.sum(probs * d_probs, -1, keepdims=True)
                d_scores = (probs * (d_probs - inner)).astype(BF16)
                dv_h = t_mm(low, c_pair[h])
                dq_h = mm(d_scores, k_pair[h])
                dk_h = t_mm(d_scores, q_pair[h])
                dq = dq_h if dq is None else dq + dq_h
                dk = dk_h if dk is None else dk + dk_h
                dv = dv_h if dv is None else dv + dv_h
            dq_ref[g, rows, q_at] = (0.125 * dq).astype(BF16)
            dq_ref[g, rows, k_at] = dk.astype(BF16)
            dq_ref[g, rows, v_at] = dv.astype(BF16)
        total = total + mm_t(dq_ref[g, rows, :], w_ref[g])
    in_ref[rows, :] = total.astype(BF16)


def weight_products(g, x_t_ref, dattn_t_ref, dq_ref, ctx_ref, ga_ref):
    block, wide = 256, dq_ref.shape[2]

    @pl.loop(0, x_t_ref.shape[0] // block)
    def _(b):
        rows = pl.ds(pl.multiple_of(b * block, block), block)
        ga_ref[g, rows, :wide] = mm(x_t_ref[rows, :], dq_ref[g]).astype(BF16)
        ga_ref[g, rows, wide:] = mm(dattn_t_ref[rows, :], ctx_ref[g]).astype(BF16)


def attention_backward_plain(
    x_ref, d_resid_ref, w_ref, wo_ref, qkv_ref, p_ref, ctx_ref,
    in_ref, ga_ref, bg_ref,
    dq_ref, dattn_t_ref, x_t_ref,
):
    groups, width = wo_ref.shape[0], wo_ref.shape[1]
    x_t_ref[...] = x_ref[...].T

    def put(v, at):
        dattn_t_ref[:, at] = v

    @pl.loop(0, p_ref.shape[0])
    def _(s):
        backward_sequence(s, put, d_resid_ref, w_ref, wo_ref, qkv_ref, p_ref, in_ref, dq_ref)

    for g in range(groups):
        bg_ref[g] = jnp.sum(dq_ref[g].astype(F32), 0, keepdims=True)
        weight_products(g, x_t_ref, dattn_t_ref, dq_ref, ctx_ref, ga_ref)


def attention_backward(
    n, x_ref, d_resid_ref, w_ref, wo_ref, qkv_ref, p_ref, ctx_ref, small_ref, ubg_ref, gd_ref, gu_ref, own_ref,
    in_ref, in_peer_ref, out_peer_ref, rd_ref, ru_ref, ra_ref, sums_ref,
    dq_ref, dattn_t_ref, x_t_ref, ga_ref, kept, half, quarter, owned, shard, tiny, tiny_1, tiny_2, tiny_x, tiny_z,
    send, recv, send_z, recv_z, send_in, recv_in, local,
):
    seqs, length = p_ref.shape[0], p_ref.shape[2]
    groups, width = wo_ref.shape[0], wo_ref.shape[1]
    model = x_ref.shape[1]
    rows_own = model // n
    depth = n // 4
    index = lax.axis_index("dp")
    x_index = lax.axis_index("mp")
    core, line, rest = index % 2, index // 2 % 2, index // 4
    to_core = {"dp": index + 1 - 2 * core}
    to_line = {"dp": index + 2 - 4 * line}
    to_x = {"mp": 1 - x_index}

    def to_rest(k):
        return {"dp": (rest + k) % depth * 4 + index % 4}

    barrier = pltpu.get_barrier_semaphore()
    peers = [to_core, to_line, to_x] + [to_rest(k) for k in range(1, depth)]
    for peer in peers:
        pl.semaphore_signal(barrier, inc=1, device_id=peer, device_id_type=MESH)
    pl.semaphore_wait(barrier, len(peers))

    def remote(src, dst, s, r, device):
        return pltpu.make_async_remote_copy(
            src_ref=src, dst_ref=dst, send_sem=s, recv_sem=r, device_id=device, device_id_type=MESH
        )

    n_half, n_quarter = model // 2, model // 4
    sources = (gd_ref, gu_ref, ga_ref)

    def by_core(t):
        there = pl.ds(pl.multiple_of((1 - core) * n_half, n_half), n_half)
        return remote(sources[t].at[:, there, :], half.at[t], send.at[0, t], recv.at[0, t], to_core)

    def by_line(t):
        there = pl.ds(pl.multiple_of((1 - line) * n_quarter, n_quarter), n_quarter)
        return remote(half.at[t, :, there, :], quarter.at[t], send.at[1, t], recv.at[1, t], to_line)

    def by_x(t):
        return remote(quarter.at[t, 1], owned.at[t], send.at[2, t], recv.at[2, t], to_x)

    def by_rest(t, k):
        there = pl.ds(pl.multiple_of((rest + k) % depth * rows_own, rows_own), rows_own)
        return remote(
            owned.at[t, there, :], shard.at[t, k - 1], send_z.at[t, k - 1], recv_z.at[t, k - 1], to_rest(k)
        )

    def keep(t):
        here = pl.ds(pl.multiple_of(core * n_half, n_half), n_half)
        return pltpu.make_async_copy(sources[t].at[:, here, :], kept.at[t], local.at[t])

    def after_core(t):
        by_core(t).wait_recv()
        if t < 2:
            keep(t).wait()
        for g in range(groups):
            if t < 2:
                add_rows(half.at[t, g], kept.at[t, g], 0, 96)
            else:
                add_rows(half.at[t, g], ga_ref.at[g], core * n_half, 96)
        by_line(t).start()

    def after_line(t):
        by_line(t).wait_recv()
        for g in range(groups):
            add_rows(quarter.at[t, g], half.at[t, g], line * n_quarter, 96)
        by_x(t).start()

    def after_x(t):
        by_x(t).wait_recv()
        add_rows(owned.at[t], quarter.at[t, 0], 0, 96)
        for k in range(1, depth):
            by_rest(t, k).start()

    def after_rest(t, out):
        total = owned[t, pl.ds(pl.multiple_of(rest * rows_own, rows_own), rows_own), :].astype(F32)
        for k in range(1, depth):
            by_rest(t, k).wait_recv()
            total = total + shard[t, k - 1].astype(F32)
        out[...] = total

    def send_output():
        return remote(own_ref, out_peer_ref, send.at[3, 0], recv.at[3, 0], to_x)

    def send_input(s):
        rows = pl.ds(pl.multiple_of(s * length, length), length)
        return remote(in_ref.at[rows, :], in_peer_ref.at[rows, :], send_in.at[s], recv_in.at[s], to_x)

    for t in range(2):
        by_core(t).start()
        keep(t).start()
    send_output().start()
    store_by_owner(x_t_ref, x_ref[...].T, slice(None), n)

    @pl.loop(0, seqs)
    def _(s):
        backward_sequence(
            s, lambda v, at: store_by_owner(dattn_t_ref, v, at, n),
            d_resid_ref, w_ref, wo_ref, qkv_ref, p_ref, in_ref, dq_ref,
        )
        send_input(s).start()

        for t in range(2):

            @pl.when(s == min(t, seqs - 1))
            def _():
                after_core(t)

    for g in range(groups):
        column = jnp.sum(dq_ref[g].astype(F32), 0, keepdims=True)
        tiny[g] = jnp.zeros_like(tiny[g])
        tiny[g, 0:1, :width] = column[:, :width]
        tiny[g, 0:1, width:] = column[:, 2 * width :]
        tiny[g, 1:2, :] = ubg_ref[g, :, :model]
        tiny[g, 2:3, :] = ubg_ref[g, :, model:]

        weight_products(g, x_t_ref, dattn_t_ref, dq_ref, ctx_ref, ga_ref)

    tiny[2] = small_ref[...]

    tiny_core = remote(tiny, tiny_1, send.at[3, 1], recv.at[3, 1], to_core)
    tiny_line = remote(tiny_1, tiny_2, send.at[3, 2], recv.at[3, 2], to_line)
    tiny_over = remote(tiny_2.at[1:3], tiny_x, send.at[4, 0], recv.at[4, 0], to_x)

    def tiny_rest(k):
        return remote(tiny_x, tiny_z.at[k - 1], send_z.at[3, k - 1], recv_z.at[3, k - 1], to_rest(k))

    by_core(2).start()
    tiny_core.start()
    after_line(0)
    after_core(2)
    tiny_core.wait_recv()
    tiny_1[...] += tiny[...]
    tiny_line.start()
    after_line(1)
    after_x(0)
    tiny_line.wait_recv()
    tiny_2[...] += tiny_1[...]
    tiny_over.start()
    after_x(1)
    after_rest(0, rd_ref)
    tiny_over.wait_recv()
    tiny_x[0] += tiny_2[0]
    tiny_x[1] += tiny_2[2]
    for k in range(1, depth):
        tiny_rest(k).start()
    after_line(2)
    after_rest(1, ru_ref)
    after_x(2)
    total = tiny_x[...]
    for k in range(1, depth):
        tiny_rest(k).wait_recv()
        total = total + tiny_z[k - 1]
    sums_ref[...] = total
    after_rest(2, ra_ref)
    for s in range(seqs):
        send_input(s).wait_recv()
        send_input(s).wait_send()
    send_output().wait()
    for t in range(3):
        by_core(t).wait_send()
        by_line(t).wait_send()
        by_x(t).wait_send()
        for k in range(1, depth):
            by_rest(t, k).wait_send()
    tiny_core.wait_send()
    tiny_line.wait_send()
    tiny_over.wait_send()
    for k in range(1, depth):
        tiny_rest(k).wait_send()


def call(kernel, outs, scratch, flops, *args, far=(), far_out=(), collective=None):
    shapes = [jax.ShapeDtypeStruct(s, d) for s, d in outs]
    moved = sum(a.size * a.dtype.itemsize for a in args) + sum(s.size * s.dtype.itemsize for s in shapes)
    vmem = pl.BlockSpec(memory_space=pltpu.VMEM)
    return pl.pallas_call(
        kernel,
        out_shape=shapes,
        in_specs=[pl.BlockSpec(memory_space=pl.ANY) if i in far else vmem for i in range(len(args))],
        out_specs=[pl.BlockSpec(memory_space=pl.ANY) if i in far_out else vmem for i in range(len(shapes))],
        scratch_shapes=[pltpu.VMEM(*s) if isinstance(s, tuple) else s for s in scratch],
        compiler_params=pltpu.CompilerParams(
            vmem_limit_bytes=VMEM_LIMIT, collective_id=collective, has_side_effects=collective is not None
        ),
        cost_estimate=pl.CostEstimate(flops=flops, bytes_accessed=moved, transcendentals=0),
    )(*args)


def factors_of(n):
    found = []
    while n > 4 or (n > 1 and len(found) < 2):
        found.append(2)
        n //= 2
    return found + ([n] if n > 1 else [])


def swap(v):
    return lax.ppermute(v, "mp", [(0, 1), (1, 0)])


def shift_dp(v, n, stride, factor, k):
    def target(d):
        i = (d // stride) % factor
        return d + ((i + k) % factor - i) * stride

    return lax.ppermute(v, "dp", [(d, target(d)) for d in range(n)])


def with_peer(own, n):
    core = lax.axis_index("dp") % 2
    half = own.shape[0] // 2
    mine = swap(lax.dynamic_slice_in_dim(own, core * half, half, 0))
    other = shift_dp(mine, n, 1, 2, 1)
    first = core == 0
    peer = jnp.concatenate([jnp.where(first, mine, other), jnp.where(first, other, mine)], 0)
    return jnp.stack([own, peer])


def reduce_to_owner(grad, n):
    index = lax.axis_index("dp")
    rows = grad.shape[1] // n
    left = grad.reshape(2, n, rows, grad.shape[2])
    stride = 1
    for factor in factors_of(n):
        parts = left.reshape(2, left.shape[1] // factor, factor, rows, left.shape[3])
        i = (index // stride) % factor

        def pick(at):
            return lax.dynamic_index_in_dim(parts, at, 2, keepdims=False)

        total = pick(i).astype(F32)
        for k in range(1, factor):
            total = total + shift_dp(pick((i + k) % factor), n, stride, factor, k).astype(F32)
        left = total.astype(BF16)
        stride *= factor
    left = left.reshape(2, rows, left.shape[3])
    return left[0].astype(F32) + swap(left[1]).astype(F32)


def per_device(
    n, layer_input, doc_lengths, q_weight, q_bias, k_weight, v_weight, v_bias, out_weight, out_bias,
    attn_gain, attn_shift, up_weight, up_bias, down_weight, down_bias, ffn_gain, ffn_shift, cotangent,
):
    rows = doc_lengths.shape[0]
    tokens, model = layer_input.shape
    length = tokens // rows
    part = length // 2
    mine = rows * part
    width = q_weight.shape[1]
    hidden = up_weight.shape[1]
    heads = width // HD
    x_index = lax.axis_index("mp")

    ends = jnp.cumsum(doc_lengths, axis=-1, dtype=jnp.int32)
    start = jnp.sum(jnp.where(doc_lengths == part, ends - part, 0), -1)
    place = jnp.arange(length, dtype=jnp.int32)
    segment = jnp.sum((place[None, :, None] >= ends[:, None, :]).astype(jnp.int32), -1, dtype=jnp.int32)
    before = place[None, :part] < start[:, None]
    from_high = before != (x_index == 1)

    def take(v):
        v = v.reshape(rows, 2, part, model)
        return jnp.where(from_high[:, :, None], v[:, 1], v[:, 0]).reshape(mine, model)

    def give(own, other):
        own, other = own.reshape(rows, part, model), other.reshape(rows, part, model)
        low = jnp.where(from_high[:, :, None], other, own)
        high = jnp.where(from_high[:, :, None], own, other)
        return jnp.stack([low, high], 1).reshape(tokens, model)

    seg = jnp.where(from_high, segment[:, part:], segment[:, :part])

    w_qkv = with_peer(jnp.concatenate([q_weight, k_weight, v_weight], 1), n)
    w_out = with_peer(out_weight, n)
    w_up = with_peer(up_weight, n)
    w_down = with_peer(down_weight, n)
    own_bias = jnp.concatenate([q_bias, v_bias, up_bias])
    bias = jnp.stack([own_bias, swap(own_bias)]).astype(F32)[:, None, :]
    b_qkv = jnp.concatenate([bias[..., :width], jnp.zeros_like(bias[..., :width]), bias[..., width : 2 * width]], -1)
    b_up = bias[..., 2 * width :]
    vectors = jnp.stack([attn_gain, attn_shift, down_bias, ffn_gain, ffn_shift]).astype(F32)

    x = take(layer_input)
    cot = take(cotangent)
    qkv, probs, ctx, xhat, rstd, low = call(
        attention_forward,
        [
            ((2, mine, 3 * width), BF16),
            ((rows, 2 * heads, part, part), BF16),
            ((2, mine, width), BF16),
            ((mine, model), F32),
            ((mine, 1), F32),
            ((mine, model), BF16),
        ],
        [],
        2 * mine * model * 8 * width,
        x, w_qkv, b_qkv, w_out, seg[:, :, None], seg[:, None, :],
        out_bias.astype(F32)[None], vectors[0:1], vectors[1:2],
    )
    remote = (model // n) % 16 == 0 and n % 4 == 0 and n > 4 and hidden == 2 * model and 4 * width == hidden
    output, g_down, g_up, d_resid, small, up_bias_grad = call(
        functools.partial(feed_forward, n if remote else 0),
        [
            ((mine, model), BF16),
            ((2, model, hidden), BF16),
            ((2, model, hidden), BF16),
            ((mine, model), F32),
            ((8, model), F32),
            ((2, 1, hidden), F32),
        ],
        [
            ((2, mine, hidden), BF16),
            ((2, mine, hidden), BF16),
            ((mine, model), F32),
            ((mine, model), BF16),
            ((model, mine), BF16),
            ((model, mine), BF16),
        ],
        2 * mine * model * 2 * hidden * 6,
        low, xhat, rstd, w_up, b_up, w_down, vectors, cot,
    )
    scratch = [((2, mine, 3 * width), BF16), ((model, mine), BF16), ((model, mine), BF16)]
    flops = 2 * mine * model * 16 * width
    if remote:
        depth = n // 4
        dma = pltpu.SemaphoreType.DMA
        grad_in, grad_in_peer, output_peer, g_down, g_up, g_attn, sums = call(
            functools.partial(attention_backward, n),
            [((mine, model), BF16)] * 3 + [((model // n, hidden), F32)] * 3 + [((2, 8, model), F32)],
            scratch + [
                ((2, model, hidden), BF16),
                ((2, 2, model // 2, hidden), BF16),
                ((3, 2, model // 2, hidden), BF16),
                ((3, 2, model // 4, hidden), BF16),
                ((3, model // 4, hidden), BF16),
                ((3, depth - 1, model // n, hidden), BF16),
                ((3, 8, model), F32),
                ((3, 8, model), F32),
                ((3, 8, model), F32),
                ((2, 8, model), F32),
                ((depth - 1, 2, 8, model), F32),
                dma((5, 3)), dma((5, 3)), dma((4, depth - 1)), dma((4, depth - 1)), dma((rows,)), dma((rows,)), dma((2,)),
            ],
            flops,
            x, d_resid, w_qkv, w_out, qkv, probs, ctx, small, up_bias_grad, g_down, g_up, output,
            far=(9, 10, 11), far_out=(1, 2), collective=0,
        )
        sums, small = sums[0, :3].reshape(-1), sums[1]
    else:
        output_peer = swap(output)
        grad_in, g_attn, bias_grad = call(
            attention_backward_plain,
            [((mine, model), BF16), ((2, model, 4 * width), BF16), ((2, 1, 3 * width), F32)],
            scratch, flops, x, d_resid, w_qkv, w_out, qkv, probs, ctx,
        )
        grad_in_peer = swap(grad_in)
        g_down, g_up, g_attn = (reduce_to_owner(v, n) for v in (g_down, g_up, g_attn))
        sums = jnp.concatenate([bias_grad[:, 0, :width], bias_grad[:, 0, 2 * width :], up_bias_grad[:, 0]], -1)
        sums = jnp.where(x_index == 0, sums, sums[::-1])
        sums, small = lax.psum((sums, small), ("dp", "mp"))
        sums = lax.dynamic_index_in_dim(sums, x_index, 0, keepdims=False)
    layer_output = give(output, output_peer)
    input_grad = give(grad_in, grad_in_peer)
    down_weight_grad = g_down.T
    up_weight_grad = g_up
    return (
        layer_output,
        input_grad,
        g_attn[:, :width],
        sums[:width],
        g_attn[:, width : 2 * width],
        g_attn[:, 2 * width : 3 * width],
        sums[width : 2 * width],
        g_attn[:, 3 * width :].T,
        small[0],
        small[1],
        small[2],
        up_weight_grad,
        sums[2 * width :],
        down_weight_grad,
        small[3],
        small[4],
        small[5],
    )


def solution(mesh):
    in_specs = (
        P("dp", None), P("dp", None), P(None, "mp"), P("mp"), P(None, "mp"), P(None, "mp"), P("mp"),
        P("mp", None), P(), P(), P(), P(None, "mp"), P("mp"), P("mp", None), P(), P(), P(), P("dp", None),
    )
    out_specs = (
        P("dp", None), P("dp", None), P("dp", "mp"), P("mp"), P("dp", "mp"), P("dp", "mp"), P("mp"),
        P("mp", "dp"), P(), P(), P(), P("dp", "mp"), P("mp"), P("mp", "dp"), P(), P(), P(),
    )
    return jax.shard_map(
        functools.partial(per_device, mesh.shape["dp"]),
        mesh=mesh, in_specs=in_specs, out_specs=out_specs, check_vma=False,
    )
```

```python
import functools

import jax
import jax.numpy as jnp
from jax import lax
from jax.experimental import pallas as pl
from jax.experimental.pallas import tpu as pltpu
from jax.sharding import PartitionSpec as P

HD = 64
PAIR = 2 * HD
EPS = 1e-12
GELU_C = 0.7978845608028654
F32 = jnp.float32
BF16 = jnp.bfloat16
CHUNK = 512
VMEM_LIMIT = 67043328
MESH = pl.DeviceIdType.MESH


def mm(a, b):
    return jnp.dot(a, b, preferred_element_type=F32)


def mm_t(a, b):
    return lax.dot_general(a, b, (((1,), (1,)), ((), ())), preferred_element_type=F32)


def t_mm(a, b):
    return lax.dot_general(a, b, (((0,), (0,)), ((), ())), preferred_element_type=F32)


def halves(v):
    lane = lax.broadcasted_iota(jnp.int32, v.shape, 1)
    zero = jnp.zeros_like(v)
    return jnp.where(lane < HD, v, zero), jnp.where(lane < HD, zero, v)


def attention_forward(
    x_ref, w_ref, b_ref, wo_ref, seg_c_ref, seg_r_ref, bo_ref, gain_ref, shift_ref,
    qkv_ref, p_ref, ctx_ref, xhat_ref, rstd_ref, low_ref,
):
    seqs, length = seg_c_ref.shape[0], seg_c_ref.shape[1]
    groups, width = wo_ref.shape[0], wo_ref.shape[1]
    pairs = width // PAIR

    @pl.loop(0, seqs)
    def _(s):
        rows = pl.ds(pl.multiple_of(s * length, length), length)
        x = x_ref[rows, :]
        mask = seg_c_ref[s] == seg_r_ref[s]
        attn = x.astype(F32) + bo_ref[...]
        for g in range(groups):
            y = mm(x, w_ref[g]) + b_ref[g]
            query = (0.125 * y[:, :width]).astype(BF16)
            key = y[:, width : 2 * width].astype(BF16)
            value = y[:, 2 * width :].astype(BF16)
            qkv_ref[g, rows, :width] = query
            qkv_ref[g, rows, width : 2 * width] = key
            qkv_ref[g, rows, 2 * width :] = value
            parts = []
            for p in range(pairs):
                at = slice(p * PAIR, (p + 1) * PAIR)
                k = key[:, at]
                both = None
                for h, (q, v) in enumerate(zip(halves(query[:, at]), halves(value[:, at]))):
                    scores = jnp.where(mask, mm_t(q, k), -1000000000.0)
                    expo = jnp.exp(scores - jnp.max(scores, -1, keepdims=True))
                    probs = (expo * (1.0 / jnp.sum(expo, -1, keepdims=True))).astype(BF16)
                    p_ref[s, (g * pairs + p) * 2 + h] = probs
                    part = mm(probs, v)
                    both = part if both is None else both + part
                parts.append(both.astype(BF16))
            ctx = jnp.concatenate(parts, 1)
            ctx_ref[g, rows, :] = ctx
            attn = attn + mm(ctx, wo_ref[g])
        mean = jnp.mean(attn, -1, keepdims=True)
        centred = attn - mean
        rstd = lax.rsqrt(jnp.mean(centred * centred, -1, keepdims=True) + EPS)
        xhat = centred * rstd
        xhat_ref[rows, :] = xhat
        rstd_ref[rows, :] = rstd
        low_ref[rows, :] = (xhat * gain_ref[...] + shift_ref[...]).astype(BF16)


def norm_backward(xhat, rstd, gain, grad):
    scaled = grad * gain
    return rstd * (
        scaled
        - jnp.mean(scaled, -1, keepdims=True)
        - xhat * jnp.mean(scaled * xhat, -1, keepdims=True)
    )


def add_rows(dst, src, offset, step):
    step = min(step, dst.shape[0])

    @pl.loop(0, dst.shape[0] // step)
    def _(i):
        here = pl.ds(pl.multiple_of(i * step, step), step)
        there = pl.ds(pl.multiple_of(offset + i * step, step), step)
        dst[here, :] = (dst[here, :].astype(F32) + src[there, :].astype(F32)).astype(dst.dtype)


def store_by_owner(dst, value, at, n):
    rows = value.shape[0] // n
    for d in range(n):
        place = (d % 2) * (n // 2) + (d // 2 % 2) * (n // 4) + d // 4
        dst[place * rows : (place + 1) * rows, at] = value[d * rows : (d + 1) * rows, :]


def feed_forward(
    low_ref, xhat_ref, rstd_ref, up_ref, ub_ref, down_ref, vec_ref, cot_ref,
    out_ref, gd_ref, gu_ref, d_resid_ref, small_ref, ubg_ref,
    act_ref, slope_ref, acc_ref, dffn_ref, dffn_t_ref, low_t_ref,
):
    tokens, width = low_ref.shape
    groups, hidden = up_ref.shape[0], up_ref.shape[2]
    step = min(CHUNK, hidden)
    per = hidden // step
    block = 256
    low_t_ref[...] = low_ref[...].T
    acc_ref[...] = jnp.zeros_like(acc_ref)

    @pl.loop(0, groups * per)
    def _(i):
        g = i // per
        at = pl.ds(pl.multiple_of((i % per) * step, step), step)

        @pl.loop(0, tokens // block)
        def _(b):
            rows = pl.ds(pl.multiple_of(b * block, block), block)
            u = mm(low_ref[rows, :], up_ref[g, :, at]) + ub_ref[g, :, at]
            square = u * u
            t = jnp.tanh(GELU_C * (u + 0.044715 * square * u))
            half = 0.5 * (1.0 + t)
            act = (u * half).astype(BF16)
            act_ref[g, rows, at] = act
            slope = half + (0.5 * GELU_C) * u * (1.0 - t * t) * (1.0 + 0.134145 * square)
            slope_ref[g, rows, at] = slope.astype(BF16)
            acc_ref[rows, :] += mm(act, down_ref[g, at, :])

    small_ref[...] = jnp.zeros_like(small_ref)
    attn_gain, attn_shift = vec_ref[0:1, :], vec_ref[1:2, :]
    down_bias = vec_ref[2:3, :]
    ffn_gain, ffn_shift = vec_ref[3:4, :], vec_ref[4:5, :]

    @pl.loop(0, tokens // block)
    def _(b):
        rows = pl.ds(pl.multiple_of(b * block, block), block)
        resid = xhat_ref[rows, :] * attn_gain + attn_shift + acc_ref[rows, :] + down_bias
        centred = resid - jnp.mean(resid, -1, keepdims=True)
        rstd = lax.rsqrt(jnp.mean(centred * centred, -1, keepdims=True) + EPS)
        xhat = centred * rstd
        out_ref[rows, :] = (xhat * ffn_gain + ffn_shift).astype(BF16)
        cot = cot_ref[rows, :].astype(F32)
        grad = norm_backward(xhat, rstd, ffn_gain, cot)
        acc_ref[rows, :] = grad
        dffn_ref[rows, :] = grad.astype(BF16)
        small_ref[3:4, :] += jnp.sum(grad, 0, keepdims=True)
        small_ref[4:5, :] += jnp.sum(cot * xhat, 0, keepdims=True)
        small_ref[5:6, :] += jnp.sum(cot, 0, keepdims=True)

    dffn_t_ref[...] = dffn_ref[...].T

    @pl.loop(0, groups * per)
    def _(i):
        g = i // per
        at = pl.ds(pl.multiple_of((i % per) * step, step), step)
        total = jnp.zeros((1, step), F32)
        for b in range(tokens // block):
            rows = slice(b * block, (b + 1) * block)
            d_upper = mm_t(dffn_ref[rows, :], down_ref[g, at, :]) * slope_ref[g, rows, at].astype(F32)
            total = total + jnp.sum(d_upper, 0, keepdims=True)
            d_low = d_upper.astype(BF16)
            slope_ref[g, rows, at] = d_low
            acc_ref[rows, :] += mm_t(d_low, up_ref[g, :, at])
        ubg_ref[g, :, at] = total
        for b in range(width // block):
            rows = slice(b * block, (b + 1) * block)
            gd_ref[g, rows, at] = mm(dffn_t_ref[rows, :], act_ref[g, :, at]).astype(BF16)
            gu_ref[g, rows, at] = mm(low_t_ref[rows, :], slope_ref[g, :, at]).astype(BF16)

    @pl.loop(0, tokens // block)
    def _(b):
        rows = pl.ds(pl.multiple_of(b * block, block), block)
        d_normed = acc_ref[rows, :]
        xhat = xhat_ref[rows, :]
        grad = norm_backward(xhat, rstd_ref[rows, :], attn_gain, d_normed)
        d_resid_ref[rows, :] = grad
        small_ref[0:1, :] += jnp.sum(grad, 0, keepdims=True)
        small_ref[1:2, :] += jnp.sum(d_normed * xhat, 0, keepdims=True)
        small_ref[2:3, :] += jnp.sum(d_normed, 0, keepdims=True)


def backward_sequence(s, put, d_resid_ref, w_ref, wo_ref, qkv_ref, p_ref, in_ref, dq_ref):
    length, groups, width = p_ref.shape[2], wo_ref.shape[0], wo_ref.shape[1]
    pairs = width // PAIR
    rows = pl.ds(pl.multiple_of(s * length, length), length)
    d_resid = d_resid_ref[rows, :]
    d_attn = d_resid.astype(BF16)
    put(d_attn.T, rows)
    total = d_resid
    for g in range(groups):
        d_ctx = mm_t(d_attn, wo_ref[g]).astype(BF16)
        for p in range(pairs):
            at = slice(p * PAIR, (p + 1) * PAIR)
            q_at, k_at, v_at = (slice(o * width + p * PAIR, o * width + (p + 1) * PAIR) for o in range(3))
            value = qkv_ref[g, rows, v_at]
            q_pair = halves(qkv_ref[g, rows, q_at])
            k_pair = halves(qkv_ref[g, rows, k_at])
            c_pair = halves(d_ctx[:, at])
            dq = dk = dv = None
            for h in range(2):
                low = p_ref[s, (g * pairs + p) * 2 + h]
                probs = low.astype(F32)
                d_probs = mm_t(c_pair[h], value)
                inner = jnp.sum(probs * d_probs, -1, keepdims=True)
                d_scores = (probs * (d_probs - inner)).astype(BF16)
                dv_h = t_mm(low, c_pair[h])
                dq_h = mm(d_scores, k_pair[h])
                dk_h = t_mm(d_scores, q_pair[h])
                dq = dq_h if dq is None else dq + dq_h
                dk = dk_h if dk is None else dk + dk_h
                dv = dv_h if dv is None else dv + dv_h
            dq_ref[g, rows, q_at] = (0.125 * dq).astype(BF16)
            dq_ref[g, rows, k_at] = dk.astype(BF16)
            dq_ref[g, rows, v_at] = dv.astype(BF16)
        total = total + mm_t(dq_ref[g, rows, :], w_ref[g])
    in_ref[rows, :] = total.astype(BF16)


def weight_products(g, x_t_ref, dattn_t_ref, dq_ref, ctx_ref, ga_ref):
    block, wide = 256, dq_ref.shape[2]

    @pl.loop(0, x_t_ref.shape[0] // block)
    def _(b):
        rows = pl.ds(pl.multiple_of(b * block, block), block)
        ga_ref[g, rows, :wide] = mm(x_t_ref[rows, :], dq_ref[g]).astype(BF16)
        ga_ref[g, rows, wide:] = mm(dattn_t_ref[rows, :], ctx_ref[g]).astype(BF16)


def attention_backward_plain(
    x_ref, d_resid_ref, w_ref, wo_ref, qkv_ref, p_ref, ctx_ref,
    in_ref, ga_ref, bg_ref,
    dq_ref, dattn_t_ref, x_t_ref,
):
    groups, width = wo_ref.shape[0], wo_ref.shape[1]
    x_t_ref[...] = x_ref[...].T

    def put(v, at):
        dattn_t_ref[:, at] = v

    @pl.loop(0, p_ref.shape[0])
    def _(s):
        backward_sequence(s, put, d_resid_ref, w_ref, wo_ref, qkv_ref, p_ref, in_ref, dq_ref)

    for g in range(groups):
        bg_ref[g] = jnp.sum(dq_ref[g].astype(F32), 0, keepdims=True)
        weight_products(g, x_t_ref, dattn_t_ref, dq_ref, ctx_ref, ga_ref)


def whole_layer(
    n, x_ref, cot_ref, seg_c_ref, seg_r_ref, bias_ref, vec_ref, wq_hbm, wk_hbm, wv_hbm, wo_hbm, up_hbm, down_hbm,
    out_ref, out_peer_ref, in_ref, in_peer_ref, rd_ref, ru_ref, ra_ref, rb_ref, sums_ref,
    w_ref, wo_ref, up_ref, down_ref, bias_2, qkv_ref, p_ref, ctx_ref, xhat_ref, rstd_ref, low_ref, act_ref, slope_ref,
    acc_ref, dffn_ref, t_low_ref, t_grad_ref, small_ref, *rest_refs,
):
    ways = ("line", "x", "line", "x")
    half, mid, owned, shard = rest_refs[0:4], rest_refs[4:8], rest_refs[8:12], rest_refs[12:16]
    tiny, tiny_1, tiny_2, tiny_x, tiny_z = rest_refs[16:21]
    send, recv, send_z, recv_z, send_in, recv_in, g_send, g_recv, g_local = rest_refs[21:]
    seqs, length = seg_c_ref.shape[0], seg_c_ref.shape[1]
    groups, width, model = wo_ref.shape
    hidden = up_ref.shape[2]
    pairs = width // PAIR
    tokens = seqs * length
    step = hidden // 3
    block = 256
    rows_own = model // n
    depth = n // 4
    index = lax.axis_index("dp")
    x_index = lax.axis_index("mp")
    core, line, rest = index % 2, index // 2 % 2, index // 4
    to_core = {"dp": index + 1 - 2 * core}
    to_line = {"dp": index + 2 - 4 * line}
    to_x = {"mp": 1 - x_index}

    def to_rest(k):
        return {"dp": (rest + k) % depth * 4 + index % 4}

    barrier = pltpu.get_barrier_semaphore()
    peers = [to_core, to_line, to_x] + [to_rest(k) for k in range(1, depth)]
    for peer in peers:
        pl.semaphore_signal(barrier, inc=1, device_id=peer, device_id_type=MESH)
    pl.semaphore_wait(barrier, len(peers))

    def remote(src, dst, s, r, device):
        return pltpu.make_async_remote_copy(
            src_ref=src, dst_ref=dst, send_sem=s, recv_sem=r, device_id=device, device_id_type=MESH
        )

    def columns(c):
        return pl.ds(pl.multiple_of(c * step, step), step)

    def ends_of(kind, c, piece):
        if kind < 3:
            size = model // 4
            rows = pl.ds(pl.multiple_of(piece * size, size), size)
            return (wq_hbm, wk_hbm, wv_hbm)[kind].at[rows, :], w_ref.at[1, rows, kind * width : (kind + 1) * width]
        if kind == 3:
            size = width // 4
            rows = pl.ds(pl.multiple_of(piece * size, size), size)
            return wo_hbm.at[rows, :], wo_ref.at[1, rows, :]
        if kind == 4:
            size = model // 4
            rows = pl.ds(pl.multiple_of(piece * size, size), size)
            return up_hbm.at[rows, columns(c)], up_ref.at[1, rows, columns(c)]
        size = step // 4
        rows = pl.ds(pl.multiple_of(c * step + piece * size, size), size)
        return down_hbm.at[rows, :], down_ref.at[1, rows, :]

    def slot(kind, c):
        return kind if kind < 4 else (4 + c if kind == 4 else 7 + c)

    def over_x(kind, c=0):
        src, dst = ends_of(kind, c, 2 * line + core)
        i = slot(kind, c)
        return remote(src, dst, g_send.at[0, i], g_recv.at[0, i], to_x)

    def pass_on(kind, c, hop):
        at = ends_of(kind, c, 2 * (1 - line) + core if hop == 3 else 2 * line + core)[1]
        i = slot(kind, c)
        return remote(at, at, g_send.at[hop, i], g_recv.at[hop, i], to_line if hop == 2 else to_core)

    def first_hop(kind, c=0):
        over_x(kind, c).wait_recv()
        pass_on(kind, c, 2).start()
        pass_on(kind, c, 1).start()

    def second_hop(kind, c=0):
        pass_on(kind, c, 2).wait_recv()
        pass_on(kind, c, 3).start()

    def complete(kind, c=0):
        pass_on(kind, c, 1).wait_recv()
        pass_on(kind, c, 3).wait_recv()

    def sent(kind, c=0):
        over_x(kind, c).wait_send()
        for hop in (1, 2, 3):
            pass_on(kind, c, hop).wait_send()

    bias_over = remote(bias_ref, bias_2, send.at[4, 0], recv.at[4, 0], to_x)
    bias_over.start()
    for kind in range(4):
        over_x(kind).start()
    for c in range(3):
        over_x(4, c).start()
        over_x(5, c).start()
    own_copies = [
        pltpu.make_async_copy(src, dst, g_local.at[i])
        for i, (src, dst) in enumerate(
            [(w, w_ref.at[0, :, o * width : (o + 1) * width]) for o, w in enumerate((wq_hbm, wk_hbm, wv_hbm))]
            + [(wo_hbm, wo_ref.at[0]), (up_hbm, up_ref.at[0]), (down_hbm, down_ref.at[0])]
        )
    ]
    for copy in own_copies:
        copy.start()

    n_half, n_quarter = model // 2, model // 4
    cut = hidden // 2
    sources = (act_ref, slope_ref, up_ref.at[:, :, :cut], up_ref.at[:, :, cut:])

    def by_core(t):
        there = pl.ds(pl.multiple_of((1 - core) * n_half, n_half), n_half)
        return remote(sources[t].at[:, there, :], half[t], send.at[0, t], recv.at[0, t], to_core)

    def by_first(t):
        if ways[t] == "line":
            there = pl.ds(pl.multiple_of((1 - line) * n_quarter, n_quarter), n_quarter)
            return remote(half[t].at[:, there, :], mid[t], send.at[1, t], recv.at[1, t], to_line)
        return remote(half[t].at[1], mid[t], send.at[1, t], recv.at[1, t], to_x)

    def by_second(t):
        if ways[t] == "line":
            return remote(mid[t].at[1], owned[t], send.at[2, t], recv.at[2, t], to_x)
        there = pl.ds(pl.multiple_of((1 - line) * n_quarter, n_quarter), n_quarter)
        return remote(mid[t].at[there, :], owned[t], send.at[2, t], recv.at[2, t], to_line)

    def by_rest(t, k):
        there = pl.ds(pl.multiple_of((rest + k) % depth * rows_own, rows_own), rows_own)
        return remote(owned[t].at[there, :], shard[t].at[k - 1], send_z.at[t, k - 1], recv_z.at[t, k - 1], to_rest(k))

    def after_core(t):
        by_core(t).wait_recv()
        for g in range(groups):
            add_rows(half[t].at[g], sources[t].at[g], core * n_half, 96)
        by_first(t).start()

    def after_first(t):
        by_first(t).wait_recv()
        if ways[t] == "line":
            for g in range(groups):
                add_rows(mid[t].at[g], half[t].at[g], line * n_quarter, 96)
        else:
            add_rows(mid[t], half[t].at[0], 0, 96)
        by_second(t).start()

    def after_second(t):
        by_second(t).wait_recv()
        if ways[t] == "line":
            add_rows(owned[t], mid[t].at[0], 0, 96)
        else:
            add_rows(owned[t], mid[t], line * n_quarter, 96)
        for k in range(1, depth):
            by_rest(t, k).start()

    def after_rest(t, out):
        total = owned[t][pl.ds(pl.multiple_of(rest * rows_own, rows_own), rows_own), :].astype(F32)
        for k in range(1, depth):
            by_rest(t, k).wait_recv()
            total = total + shard[t][k - 1].astype(F32)
        out[...] = total

    def send_output(b):
        rows = pl.ds(pl.multiple_of(b * length, length), length)
        return remote(out_ref.at[rows, :], out_peer_ref.at[rows, :], send_in.at[1, b], recv_in.at[1, b], to_x)

    def send_input(s):
        rows = pl.ds(pl.multiple_of(s * length, length), length)
        return remote(in_ref.at[rows, :], in_peer_ref.at[rows, :], send_in.at[0, s], recv_in.at[0, s], to_x)

    attn_gain, attn_shift, down_bias = vec_ref[0:1, :], vec_ref[1:2, :], vec_ref[2:3, :]
    ffn_gain, ffn_shift, out_bias = vec_ref[3:4, :], vec_ref[4:5, :], vec_ref[5:6, :]

    def attend(s, g, biases):
        rows = pl.ds(pl.multiple_of(s * length, length), length)
        x = x_ref[rows, :]
        mask = seg_c_ref[s] == seg_r_ref[s]
        y = mm(x, w_ref[g])
        query = (0.125 * (y[:, :width] + biases[0:1, :width])).astype(BF16)
        key = y[:, width : 2 * width].astype(BF16)
        value = (y[:, 2 * width :] + biases[0:1, width : 2 * width]).astype(BF16)
        qkv_ref[g, rows, :width] = query
        qkv_ref[g, rows, width : 2 * width] = key
        qkv_ref[g, rows, 2 * width :] = value
        parts = []
        for p in range(pairs):
            at = slice(p * PAIR, (p + 1) * PAIR)
            k = key[:, at]
            both = None
            for h, (q, v) in enumerate(zip(halves(query[:, at]), halves(value[:, at]))):
                scores = jnp.where(mask, mm_t(q, k), -1000000000.0)
                expo = jnp.exp(scores - jnp.max(scores, -1, keepdims=True))
                probs = (expo * (1.0 / jnp.sum(expo, -1, keepdims=True))).astype(BF16)
                p_ref[s, (g * pairs + p) * 2 + h] = probs
                part = mm(probs, v)
                both = part if both is None else both + part
            parts.append(both.astype(BF16))
        ctx = jnp.concatenate(parts, 1)
        ctx_ref[g, rows, :] = ctx
        return mm(ctx, wo_ref[g])

    for copy in own_copies[:4]:
        copy.wait()

    @pl.loop(0, seqs)
    def _(s):
        rows = pl.ds(pl.multiple_of(s * length, length), length)
        acc_ref[rows, :] = x_ref[rows, :].astype(F32) + out_bias + attend(s, 0, bias_ref)
        for kind in range(3):

            @pl.when(s == min(kind, seqs - 1))
            def _():
                first_hop(kind)

    first_hop(3)
    for kind in range(4):
        second_hop(kind)
    for kind in range(4):
        complete(kind)
    bias_over.wait()

    @pl.loop(0, seqs)
    def _(s):
        rows = pl.ds(pl.multiple_of(s * length, length), length)
        attn = acc_ref[rows, :] + attend(s, 1, bias_2)
        centred = attn - jnp.mean(attn, -1, keepdims=True)
        rstd = lax.rsqrt(jnp.mean(centred * centred, -1, keepdims=True) + EPS)
        xhat = centred * rstd
        xhat_ref[rows, :] = xhat
        rstd_ref[rows, :] = rstd
        low_ref[rows, :] = (xhat * attn_gain + attn_shift).astype(BF16)

        @pl.when(s == min(1, seqs - 1))
        def _():
            first_hop(4, 0)
            first_hop(5, 0)

    for copy in own_copies[4:]:
        copy.wait()
    store_by_owner(t_low_ref, low_ref[...].T, slice(None), n)

    def expand(c, g, biases):
        at = columns(c)
        bias_at = pl.ds(pl.multiple_of(2 * width + c * step, 128), step)

        @pl.loop(0, tokens // block)
        def _(b):
            rows = pl.ds(pl.multiple_of(b * block, block), block)
            u = mm(low_ref[rows, :], up_ref[g, :, at]) + biases[0:1, bias_at]
            square = u * u
            t = jnp.tanh(GELU_C * (u + 0.044715 * square * u))
            gate = 0.5 * (1.0 + t)
            act = (u * gate).astype(BF16)
            act_ref[g, rows, at] = act
            slope = gate + (0.5 * GELU_C) * u * (1.0 - t * t) * (1.0 + 0.134145 * square)
            slope_ref[g, rows, at] = slope.astype(BF16)
            acc_ref[rows, :] += mm(act, down_ref[g, at, :])

    acc_ref[...] = jnp.zeros_like(acc_ref)

    @pl.loop(0, 3)
    def _(c):
        expand(c, 0, bias_ref)

        @pl.when(c == 0)
        def _():
            first_hop(4, 1)
            first_hop(5, 1)

        @pl.when(c == 1)
        def _():
            second_hop(4, 0)
            second_hop(5, 0)

        @pl.when(c == 2)
        def _():
            first_hop(4, 2)
            first_hop(5, 2)
            second_hop(4, 1)
            second_hop(5, 1)

    @pl.loop(0, 3)
    def _(c):
        @pl.when(c == 2)
        def _():
            second_hop(4, 2)
            second_hop(5, 2)

        complete(4, c)
        complete(5, c)
        expand(c, 1, bias_2)

    small_ref[...] = jnp.zeros_like(small_ref)

    @pl.loop(0, seqs)
    def _(b):
        rows = pl.ds(pl.multiple_of(b * length, length), length)
        resid = xhat_ref[rows, :] * attn_gain + attn_shift + acc_ref[rows, :] + down_bias
        centred = resid - jnp.mean(resid, -1, keepdims=True)
        rstd = lax.rsqrt(jnp.mean(centred * centred, -1, keepdims=True) + EPS)
        xhat = centred * rstd
        out_ref[rows, :] = (xhat * ffn_gain + ffn_shift).astype(BF16)
        cot = cot_ref[rows, :].astype(F32)
        grad = norm_backward(xhat, rstd, ffn_gain, cot)
        acc_ref[rows, :] = grad
        dffn_ref[rows, :] = grad.astype(BF16)
        small_ref[3:4, :] += jnp.sum(grad, 0, keepdims=True)
        small_ref[4:5, :] += jnp.sum(cot * xhat, 0, keepdims=True)
        small_ref[5:6, :] += jnp.sum(cot, 0, keepdims=True)
        send_output(b).start()

    store_by_owner(t_grad_ref, dffn_ref[...].T, slice(None), n)

    def product(left, place, g, at):
        made = [
            mm(left[b * block : (b + 1) * block, :], place[g, :, at]).astype(BF16) for b in range(model // block)
        ]
        for b, value in enumerate(made):
            place[g, b * block : (b + 1) * block, at] = value

    tiny[...] = jnp.zeros_like(tiny)
    for g in range(groups):

        @pl.loop(0, 3)
        def _(c):
            product(t_grad_ref, act_ref, g, columns(c))

    by_core(0).start()
    for g in range(groups):

        @pl.loop(0, 3)
        def _(c):
            at = columns(c)
            total = jnp.zeros((1, step), F32)
            for b in range(tokens // block):
                rows = slice(b * block, (b + 1) * block)
                d_upper = mm_t(dffn_ref[rows, :], down_ref[g, at, :]) * slope_ref[g, rows, at].astype(F32)
                total = total + jnp.sum(d_upper, 0, keepdims=True)
                d_low = d_upper.astype(BF16)
                slope_ref[g, rows, at] = d_low
                acc_ref[rows, :] += mm_t(d_low, up_ref[g, :, at])
            tiny[3 + g, 0:1, at] = total
            product(t_low_ref, slope_ref, g, at)
            if g == 0:

                @pl.when(c == 1)
                def _():
                    after_core(0)

    by_core(1).start()

    @pl.loop(0, seqs)
    def _(b):
        rows = pl.ds(pl.multiple_of(b * length, length), length)
        d_normed = acc_ref[rows, :]
        xhat = xhat_ref[rows, :]
        grad = norm_backward(xhat, rstd_ref[rows, :], attn_gain, d_normed)
        acc_ref[rows, :] = grad
        small_ref[0:1, :] += jnp.sum(grad, 0, keepdims=True)
        small_ref[1:2, :] += jnp.sum(d_normed * xhat, 0, keepdims=True)
        small_ref[2:3, :] += jnp.sum(d_normed, 0, keepdims=True)

    store_by_owner(t_low_ref, x_ref[...].T, slice(None), n)

    @pl.loop(0, seqs)
    def _(s):
        backward_sequence(
            s, lambda v, at: store_by_owner(t_grad_ref, v, at, n),
            acc_ref, w_ref, wo_ref, qkv_ref, p_ref, in_ref, qkv_ref,
        )
        send_input(s).start()

        @pl.when(s == 0)
        def _():
            after_core(1)

        @pl.when(s == min(1, seqs - 1))
        def _():
            after_first(0)

        @pl.when(s == min(2, seqs - 1))
        def _():
            after_second(0)

    for kind in range(4):
        sent(kind)
    for c in range(3):
        sent(4, c)
        sent(5, c)
    for g in range(groups):
        weight_products(g, t_low_ref, t_grad_ref, qkv_ref, ctx_ref, up_ref)
    by_core(2).start()
    by_core(3).start()
    for g in range(groups):
        column = jnp.sum(qkv_ref[g].astype(F32), 0, keepdims=True)
        tiny[g, 0:1, :width] = column[:, :width]
        tiny[g, 0:1, width : 2 * width] = column[:, 2 * width :]
        tiny[g, 1:2, :] = tiny[3 + g, 0:1, :]
    tiny[2, :, :model] = small_ref[...]

    tiny_core = remote(tiny.at[0:3], tiny_1, send.at[3, 1], recv.at[3, 1], to_core)
    tiny_line = remote(tiny_1, tiny_2, send.at[3, 2], recv.at[3, 2], to_line)
    tiny_over = remote(tiny_2.at[1:3], tiny_x, send.at[3, 3], recv.at[3, 3], to_x)

    def tiny_rest(k):
        return remote(tiny_x, tiny_z.at[k - 1], send_z.at[4, k - 1], recv_z.at[4, k - 1], to_rest(k))

    tiny_core.start()
    after_core(2)
    after_core(3)
    tiny_core.wait_recv()
    tiny_1[...] += tiny[0:3]
    tiny_line.start()
    after_first(1)
    after_first(2)
    tiny_line.wait_recv()
    tiny_2[...] += tiny_1[...]
    tiny_over.start()
    after_first(3)
    after_rest(0, rd_ref)
    after_second(1)
    tiny_over.wait_recv()
    tiny_x[0] += tiny_2[0]
    tiny_x[1] += tiny_2[2]
    for k in range(1, depth):
        tiny_rest(k).start()
    after_second(2)
    after_second(3)
    after_rest(1, ru_ref)
    total = tiny_x[...]
    for k in range(1, depth):
        tiny_rest(k).wait_recv()
        total = total + tiny_z[k - 1]
    sums_ref[...] = total
    after_rest(2, ra_ref)
    after_rest(3, rb_ref)
    for s in range(seqs):
        send_output(s).wait()
        send_input(s).wait()
    for t in range(4):
        by_core(t).wait_send()
        by_first(t).wait_send()
        by_second(t).wait_send()
        for k in range(1, depth):
            by_rest(t, k).wait_send()
    tiny_core.wait_send()
    tiny_line.wait_send()
    tiny_over.wait_send()
    for k in range(1, depth):
        tiny_rest(k).wait_send()


def call(kernel, outs, scratch, flops, *args, far=(), far_out=(), collective=None):
    shapes = [jax.ShapeDtypeStruct(s, d) for s, d in outs]
    moved = sum(a.size * a.dtype.itemsize for a in args) + sum(s.size * s.dtype.itemsize for s in shapes)
    vmem = pl.BlockSpec(memory_space=pltpu.VMEM)
    return pl.pallas_call(
        kernel,
        out_shape=shapes,
        in_specs=[pl.BlockSpec(memory_space=pl.ANY) if i in far else vmem for i in range(len(args))],
        out_specs=[pl.BlockSpec(memory_space=pl.ANY) if i in far_out else vmem for i in range(len(shapes))],
        scratch_shapes=[pltpu.VMEM(*s) if isinstance(s, tuple) else s for s in scratch],
        compiler_params=pltpu.CompilerParams(
            vmem_limit_bytes=VMEM_LIMIT, collective_id=collective, has_side_effects=collective is not None
        ),
        cost_estimate=pl.CostEstimate(flops=flops, bytes_accessed=moved, transcendentals=0),
    )(*args)


def factors_of(n):
    found = []
    while n > 4 or (n > 1 and len(found) < 2):
        found.append(2)
        n //= 2
    return found + ([n] if n > 1 else [])


def swap(v):
    return lax.ppermute(v, "mp", [(0, 1), (1, 0)])


def shift_dp(v, n, stride, factor, k):
    def target(d):
        i = (d // stride) % factor
        return d + ((i + k) % factor - i) * stride

    return lax.ppermute(v, "dp", [(d, target(d)) for d in range(n)])


def with_peer(own, n):
    core = lax.axis_index("dp") % 2
    half = own.shape[0] // 2
    mine = swap(lax.dynamic_slice_in_dim(own, core * half, half, 0))
    other = shift_dp(mine, n, 1, 2, 1)
    first = core == 0
    peer = jnp.concatenate([jnp.where(first, mine, other), jnp.where(first, other, mine)], 0)
    return jnp.stack([own, peer])


def reduce_to_owner(grad, n):
    index = lax.axis_index("dp")
    rows = grad.shape[1] // n
    left = grad.reshape(2, n, rows, grad.shape[2])
    stride = 1
    for factor in factors_of(n):
        parts = left.reshape(2, left.shape[1] // factor, factor, rows, left.shape[3])
        i = (index // stride) % factor

        def pick(at):
            return lax.dynamic_index_in_dim(parts, at, 2, keepdims=False)

        total = pick(i).astype(F32)
        for k in range(1, factor):
            total = total + shift_dp(pick((i + k) % factor), n, stride, factor, k).astype(F32)
        left = total.astype(BF16)
        stride *= factor
    left = left.reshape(2, rows, left.shape[3])
    return left[0].astype(F32) + swap(left[1]).astype(F32)


def per_device(
    n, layer_input, doc_lengths, q_weight, q_bias, k_weight, v_weight, v_bias, out_weight, out_bias,
    attn_gain, attn_shift, up_weight, up_bias, down_weight, down_bias, ffn_gain, ffn_shift, cotangent,
):
    rows = doc_lengths.shape[0]
    tokens, model = layer_input.shape
    length = tokens // rows
    part = length // 2
    mine = rows * part
    width = q_weight.shape[1]
    hidden = up_weight.shape[1]
    heads = width // HD
    x_index = lax.axis_index("mp")

    ends = jnp.cumsum(doc_lengths, axis=-1, dtype=jnp.int32)
    start = jnp.sum(jnp.where(doc_lengths == part, ends - part, 0), -1)
    place = jnp.arange(length, dtype=jnp.int32)
    segment = jnp.sum((place[None, :, None] >= ends[:, None, :]).astype(jnp.int32), -1, dtype=jnp.int32)
    before = place[None, :part] < start[:, None]
    from_high = before != (x_index == 1)

    def take(v):
        v = v.reshape(rows, 2, part, model)
        return jnp.where(from_high[:, :, None], v[:, 1], v[:, 0]).reshape(mine, model)

    def give(own, other):
        own, other = own.reshape(rows, part, model), other.reshape(rows, part, model)
        low = jnp.where(from_high[:, :, None], other, own)
        high = jnp.where(from_high[:, :, None], own, other)
        return jnp.stack([low, high], 1).reshape(tokens, model)

    seg = jnp.where(from_high, segment[:, part:], segment[:, :part])

    x = take(layer_input)
    cot = take(cotangent)
    own_bias = jnp.concatenate([q_bias, v_bias, up_bias])
    remote = (
        (model // n) % 16 == 0 and n % 4 == 0 and n > 4
        and hidden == 2 * model and 4 * width == hidden and hidden % 384 == 0 and rows >= 3
    )
    if remote:
        depth = n // 4
        dma = pltpu.SemaphoreType.DMA
        wide = (hidden, hidden, model, model)
        quarter = model // 4
        vectors = jnp.stack([attn_gain, attn_shift, down_bias, ffn_gain, ffn_shift, out_bias]).astype(F32)
        output, output_peer, grad_in, grad_in_peer, g_down, g_up, g_first, g_last, sums = call(
            functools.partial(whole_layer, n),
            [((mine, model), BF16)] * 4
            + [((model // n, c), F32) for c in wide]
            + [((2, 8, hidden), F32)],
            [
                ((2, model, 3 * width), BF16),
                ((2, width, model), BF16),
                ((2, model, hidden), BF16),
                ((2, hidden, model), BF16),
                ((1, 2 * width + hidden), F32),
                ((2, mine, 3 * width), BF16),
                ((rows, 2 * heads, part, part), BF16),
                ((2, mine, width), BF16),
                ((mine, model), F32),
                ((mine, 1), F32),
                ((mine, model), BF16),
                ((2, model, hidden), BF16),
                ((2, model, hidden), BF16),
                ((mine, model), F32),
                ((mine, model), BF16),
                ((model, mine), BF16),
                ((model, mine), BF16),
                ((8, model), F32),
            ]
            + [((2, model // 2, c), BF16) for c in wide]
            + [((2, quarter, c) if i % 2 == 0 else (2 * quarter, c), BF16) for i, c in enumerate(wide)]
            + [((quarter, c), BF16) for c in wide]
            + [((depth - 1, model // n, c), BF16) for c in wide]
            + [
                ((5, 8, hidden), F32),
                ((3, 8, hidden), F32),
                ((3, 8, hidden), F32),
                ((2, 8, hidden), F32),
                ((depth - 1, 2, 8, hidden), F32),
                dma((5, 4)), dma((5, 4)), dma((5, depth - 1)), dma((5, depth - 1)), dma((2, rows)), dma((2, rows)),
                dma((4, 10)), dma((4, 10)), dma((6,)),
            ],
            2 * mine * model * (24 * width + 12 * hidden),
            x, cot, seg[:, :, None], seg[:, None, :], own_bias.astype(F32)[None], vectors,
            q_weight, k_weight, v_weight, out_weight, up_weight, down_weight,
            far=(6, 7, 8, 9, 10, 11), far_out=(1, 3), collective=0,
        )
        g_attn = jnp.concatenate([g_first, g_last], -1)
        small = sums[1, :, :model]
        sums = jnp.concatenate([sums[0, 0, : 2 * width], sums[0, 1]])
    else:
        w_qkv = with_peer(jnp.concatenate([q_weight, k_weight, v_weight], 1), n)
        w_out = with_peer(out_weight, n)
        w_up = with_peer(up_weight, n)
        w_down = with_peer(down_weight, n)
        bias = jnp.stack([own_bias, swap(own_bias)]).astype(F32)[:, None, :]
        b_qkv = jnp.concatenate([bias[..., :width], jnp.zeros_like(bias[..., :width]), bias[..., width : 2 * width]], -1)
        b_up = bias[..., 2 * width :]
        vectors = jnp.stack([attn_gain, attn_shift, down_bias, ffn_gain, ffn_shift]).astype(F32)

        qkv, probs, ctx, xhat, rstd, low = call(
            attention_forward,
            [
                ((2, mine, 3 * width), BF16),
                ((rows, 2 * heads, part, part), BF16),
                ((2, mine, width), BF16),
                ((mine, model), F32),
                ((mine, 1), F32),
                ((mine, model), BF16),
            ],
            [],
            2 * mine * model * 8 * width,
            x, w_qkv, b_qkv, w_out, seg[:, :, None], seg[:, None, :],
            out_bias.astype(F32)[None], vectors[0:1], vectors[1:2],
        )
        output, g_down, g_up, d_resid, small, up_bias_grad = call(
            feed_forward,
            [
                ((mine, model), BF16),
                ((2, model, hidden), BF16),
                ((2, model, hidden), BF16),
                ((mine, model), F32),
                ((8, model), F32),
                ((2, 1, hidden), F32),
            ],
            [
                ((2, mine, hidden), BF16),
                ((2, mine, hidden), BF16),
                ((mine, model), F32),
                ((mine, model), BF16),
                ((model, mine), BF16),
                ((model, mine), BF16),
            ],
            2 * mine * model * 2 * hidden * 6,
            low, xhat, rstd, w_up, b_up, w_down, vectors, cot,
        )
        scratch = [((2, mine, 3 * width), BF16), ((model, mine), BF16), ((model, mine), BF16)]
        flops = 2 * mine * model * 16 * width
        output_peer = swap(output)
        grad_in, g_attn, bias_grad = call(
            attention_backward_plain,
            [((mine, model), BF16), ((2, model, 4 * width), BF16), ((2, 1, 3 * width), F32)],
            scratch, flops, x, d_resid, w_qkv, w_out, qkv, probs, ctx,
        )
        grad_in_peer = swap(grad_in)
        g_down, g_up, g_attn = (reduce_to_owner(v, n) for v in (g_down, g_up, g_attn))
        sums = jnp.concatenate([bias_grad[:, 0, :width], bias_grad[:, 0, 2 * width :], up_bias_grad[:, 0]], -1)
        sums = jnp.where(x_index == 0, sums, sums[::-1])
        sums, small = lax.psum((sums, small), ("dp", "mp"))
        sums = lax.dynamic_index_in_dim(sums, x_index, 0, keepdims=False)
    layer_output = give(output, output_peer)
    input_grad = give(grad_in, grad_in_peer)
    down_weight_grad = g_down.T
    up_weight_grad = g_up
    return (
        layer_output,
        input_grad,
        g_attn[:, :width],
        sums[:width],
        g_attn[:, width : 2 * width],
        g_attn[:, 2 * width : 3 * width],
        sums[width : 2 * width],
        g_attn[:, 3 * width :].T,
        small[0],
        small[1],
        small[2],
        up_weight_grad,
        sums[2 * width :],
        down_weight_grad,
        small[3],
        small[4],
        small[5],
    )


def solution(mesh):
    in_specs = (
        P("dp", None), P("dp", None), P(None, "mp"), P("mp"), P(None, "mp"), P(None, "mp"), P("mp"),
        P("mp", None), P(), P(), P(), P(None, "mp"), P("mp"), P("mp", None), P(), P(), P(), P("dp", None),
    )
    out_specs = (
        P("dp", None), P("dp", None), P("dp", "mp"), P("mp"), P("dp", "mp"), P("dp", "mp"), P("mp"),
        P("mp", "dp"), P(), P(), P(), P("dp", "mp"), P("mp"), P("mp", "dp"), P(), P(), P(),
    )
    return jax.shard_map(
        functools.partial(per_device, mesh.shape["dp"]),
        mesh=mesh, in_specs=in_specs, out_specs=out_specs, check_vma=False,
    )
```

```python
import functools

import jax
import jax.numpy as jnp
from jax import lax
from jax.experimental import pallas as pl
from jax.experimental.pallas import tpu as pltpu
from jax.sharding import PartitionSpec as P

HD = 64
PAIR = 2 * HD
EPS = 1e-12
GELU_C = 0.7978845608028654
F32 = jnp.float32
BF16 = jnp.bfloat16
CHUNK = 512
VMEM_LIMIT = 67043328
MESH = pl.DeviceIdType.MESH


def mm(a, b):
    return jnp.dot(a, b, preferred_element_type=F32)


def mm_t(a, b):
    return lax.dot_general(a, b, (((1,), (1,)), ((), ())), preferred_element_type=F32)


def t_mm(a, b):
    return lax.dot_general(a, b, (((0,), (0,)), ((), ())), preferred_element_type=F32)


def halves(v):
    lane = lax.broadcasted_iota(jnp.int32, v.shape, 1)
    zero = jnp.zeros_like(v)
    return jnp.where(lane < HD, v, zero), jnp.where(lane < HD, zero, v)


def attention_forward(
    x_ref, w_ref, b_ref, wo_ref, seg_c_ref, seg_r_ref, bo_ref, gain_ref, shift_ref,
    qkv_ref, p_ref, ctx_ref, xhat_ref, rstd_ref, low_ref,
):
    seqs, length = seg_c_ref.shape[0], seg_c_ref.shape[1]
    groups, width = wo_ref.shape[0], wo_ref.shape[1]
    pairs = width // PAIR

    @pl.loop(0, seqs)
    def _(s):
        rows = pl.ds(pl.multiple_of(s * length, length), length)
        x = x_ref[rows, :]
        mask = seg_c_ref[s] == seg_r_ref[s]
        attn = x.astype(F32) + bo_ref[...]
        for g in range(groups):
            y = mm(x, w_ref[g]) + b_ref[g]
            query = (0.125 * y[:, :width]).astype(BF16)
            key = y[:, width : 2 * width].astype(BF16)
            value = y[:, 2 * width :].astype(BF16)
            qkv_ref[g, rows, :width] = query
            qkv_ref[g, rows, width : 2 * width] = key
            qkv_ref[g, rows, 2 * width :] = value
            parts = []
            for p in range(pairs):
                at = slice(p * PAIR, (p + 1) * PAIR)
                k = key[:, at]
                both = None
                for h, (q, v) in enumerate(zip(halves(query[:, at]), halves(value[:, at]))):
                    scores = jnp.where(mask, mm_t(q, k), -1000000000.0)
                    expo = jnp.exp(scores - jnp.max(scores, -1, keepdims=True))
                    probs = (expo * (1.0 / jnp.sum(expo, -1, keepdims=True))).astype(BF16)
                    p_ref[s, (g * pairs + p) * 2 + h] = probs
                    part = mm(probs, v)
                    both = part if both is None else both + part
                parts.append(both.astype(BF16))
            ctx = jnp.concatenate(parts, 1)
            ctx_ref[g, rows, :] = ctx
            attn = attn + mm(ctx, wo_ref[g])
        mean = jnp.mean(attn, -1, keepdims=True)
        centred = attn - mean
        rstd = lax.rsqrt(jnp.mean(centred * centred, -1, keepdims=True) + EPS)
        xhat = centred * rstd
        xhat_ref[rows, :] = xhat
        rstd_ref[rows, :] = rstd
        low_ref[rows, :] = (xhat * gain_ref[...] + shift_ref[...]).astype(BF16)


def norm_backward(xhat, rstd, gain, grad):
    scaled = grad * gain
    return rstd * (
        scaled
        - jnp.mean(scaled, -1, keepdims=True)
        - xhat * jnp.mean(scaled * xhat, -1, keepdims=True)
    )


def add_rows(dst, src, offset, step):
    step = min(step, dst.shape[0])

    @pl.loop(0, dst.shape[0] // step)
    def _(i):
        here = pl.ds(pl.multiple_of(i * step, step), step)
        there = pl.ds(pl.multiple_of(offset + i * step, step), step)
        dst[here, :] = (dst[here, :].astype(F32) + src[there, :].astype(F32)).astype(dst.dtype)


def store_by_owner(dst, value, at, n):
    rows = value.shape[0] // n
    for d in range(n):
        place = (d % 2) * (n // 2) + (d // 2 % 2) * (n // 4) + d // 4
        dst[place * rows : (place + 1) * rows, at] = value[d * rows : (d + 1) * rows, :]


def feed_forward(
    low_ref, xhat_ref, rstd_ref, up_ref, ub_ref, down_ref, vec_ref, cot_ref,
    out_ref, gd_ref, gu_ref, d_resid_ref, small_ref, ubg_ref,
    act_ref, slope_ref, acc_ref, dffn_ref, dffn_t_ref, low_t_ref,
):
    tokens, width = low_ref.shape
    groups, hidden = up_ref.shape[0], up_ref.shape[2]
    step = min(CHUNK, hidden)
    per = hidden // step
    block = 256
    low_t_ref[...] = low_ref[...].T
    acc_ref[...] = jnp.zeros_like(acc_ref)

    @pl.loop(0, groups * per)
    def _(i):
        g = i // per
        at = pl.ds(pl.multiple_of((i % per) * step, step), step)

        @pl.loop(0, tokens // block)
        def _(b):
            rows = pl.ds(pl.multiple_of(b * block, block), block)
            u = mm(low_ref[rows, :], up_ref[g, :, at]) + ub_ref[g, :, at]
            square = u * u
            t = jnp.tanh(GELU_C * (u + 0.044715 * square * u))
            half = 0.5 * (1.0 + t)
            act = (u * half).astype(BF16)
            act_ref[g, rows, at] = act
            slope = half + (0.5 * GELU_C) * u * (1.0 - t * t) * (1.0 + 0.134145 * square)
            slope_ref[g, rows, at] = slope.astype(BF16)
            acc_ref[rows, :] += mm(act, down_ref[g, at, :])

    small_ref[...] = jnp.zeros_like(small_ref)
    attn_gain, attn_shift = vec_ref[0:1, :], vec_ref[1:2, :]
    down_bias = vec_ref[2:3, :]
    ffn_gain, ffn_shift = vec_ref[3:4, :], vec_ref[4:5, :]

    @pl.loop(0, tokens // block)
    def _(b):
        rows = pl.ds(pl.multiple_of(b * block, block), block)
        resid = xhat_ref[rows, :] * attn_gain + attn_shift + acc_ref[rows, :] + down_bias
        centred = resid - jnp.mean(resid, -1, keepdims=True)
        rstd = lax.rsqrt(jnp.mean(centred * centred, -1, keepdims=True) + EPS)
        xhat = centred * rstd
        out_ref[rows, :] = (xhat * ffn_gain + ffn_shift).astype(BF16)
        cot = cot_ref[rows, :].astype(F32)
        grad = norm_backward(xhat, rstd, ffn_gain, cot)
        acc_ref[rows, :] = grad
        dffn_ref[rows, :] = grad.astype(BF16)
        small_ref[3:4, :] += jnp.sum(grad, 0, keepdims=True)
        small_ref[4:5, :] += jnp.sum(cot * xhat, 0, keepdims=True)
        small_ref[5:6, :] += jnp.sum(cot, 0, keepdims=True)

    dffn_t_ref[...] = dffn_ref[...].T

    @pl.loop(0, groups * per)
    def _(i):
        g = i // per
        at = pl.ds(pl.multiple_of((i % per) * step, step), step)
        total = jnp.zeros((1, step), F32)
        for b in range(tokens // block):
            rows = slice(b * block, (b + 1) * block)
            d_upper = mm_t(dffn_ref[rows, :], down_ref[g, at, :]) * slope_ref[g, rows, at].astype(F32)
            total = total + jnp.sum(d_upper, 0, keepdims=True)
            d_low = d_upper.astype(BF16)
            slope_ref[g, rows, at] = d_low
            acc_ref[rows, :] += mm_t(d_low, up_ref[g, :, at])
        ubg_ref[g, :, at] = total
        for b in range(width // block):
            rows = slice(b * block, (b + 1) * block)
            gd_ref[g, rows, at] = mm(dffn_t_ref[rows, :], act_ref[g, :, at]).astype(BF16)
            gu_ref[g, rows, at] = mm(low_t_ref[rows, :], slope_ref[g, :, at]).astype(BF16)

    @pl.loop(0, tokens // block)
    def _(b):
        rows = pl.ds(pl.multiple_of(b * block, block), block)
        d_normed = acc_ref[rows, :]
        xhat = xhat_ref[rows, :]
        grad = norm_backward(xhat, rstd_ref[rows, :], attn_gain, d_normed)
        d_resid_ref[rows, :] = grad
        small_ref[0:1, :] += jnp.sum(grad, 0, keepdims=True)
        small_ref[1:2, :] += jnp.sum(d_normed * xhat, 0, keepdims=True)
        small_ref[2:3, :] += jnp.sum(d_normed, 0, keepdims=True)


def backward_sequence(s, put, d_resid_ref, w_ref, wo_ref, qkv_ref, p_ref, in_ref, dq_ref):
    length, groups, width = p_ref.shape[2], wo_ref.shape[0], wo_ref.shape[1]
    pairs = width // PAIR
    rows = pl.ds(pl.multiple_of(s * length, length), length)
    d_resid = d_resid_ref[rows, :]
    d_attn = d_resid.astype(BF16)
    put(d_attn.T, rows)
    total = d_resid
    for g in range(groups):
        d_ctx = mm_t(d_attn, wo_ref[g]).astype(BF16)
        for p in range(pairs):
            at = slice(p * PAIR, (p + 1) * PAIR)
            q_at, k_at, v_at = (slice(o * width + p * PAIR, o * width + (p + 1) * PAIR) for o in range(3))
            value = qkv_ref[g, rows, v_at]
            q_pair = halves(qkv_ref[g, rows, q_at])
            k_pair = halves(qkv_ref[g, rows, k_at])
            c_pair = halves(d_ctx[:, at])
            dq = dk = dv = None
            for h in range(2):
                low = p_ref[s, (g * pairs + p) * 2 + h]
                probs = low.astype(F32)
                d_probs = mm_t(c_pair[h], value)
                inner = jnp.sum(probs * d_probs, -1, keepdims=True)
                d_scores = (probs * (d_probs - inner)).astype(BF16)
                dv_h = t_mm(low, c_pair[h])
                dq_h = mm(d_scores, k_pair[h])
                dk_h = t_mm(d_scores, q_pair[h])
                dq = dq_h if dq is None else dq + dq_h
                dk = dk_h if dk is None else dk + dk_h
                dv = dv_h if dv is None else dv + dv_h
            dq_ref[g, rows, q_at] = (0.125 * dq).astype(BF16)
            dq_ref[g, rows, k_at] = dk.astype(BF16)
            dq_ref[g, rows, v_at] = dv.astype(BF16)
        total = total + mm_t(dq_ref[g, rows, :], w_ref[g])
    in_ref[rows, :] = total.astype(BF16)


def weight_products(g, x_t_ref, dattn_t_ref, dq_ref, ctx_ref, ga_ref):
    block, wide = 256, dq_ref.shape[2]

    @pl.loop(0, x_t_ref.shape[0] // block)
    def _(b):
        rows = pl.ds(pl.multiple_of(b * block, block), block)
        ga_ref[g, rows, :wide] = mm(x_t_ref[rows, :], dq_ref[g]).astype(BF16)
        ga_ref[g, rows, wide:] = mm(dattn_t_ref[rows, :], ctx_ref[g]).astype(BF16)


def attention_backward_plain(
    x_ref, d_resid_ref, w_ref, wo_ref, qkv_ref, p_ref, ctx_ref,
    in_ref, ga_ref, bg_ref,
    dq_ref, dattn_t_ref, x_t_ref,
):
    groups, width = wo_ref.shape[0], wo_ref.shape[1]
    x_t_ref[...] = x_ref[...].T

    def put(v, at):
        dattn_t_ref[:, at] = v

    @pl.loop(0, p_ref.shape[0])
    def _(s):
        backward_sequence(s, put, d_resid_ref, w_ref, wo_ref, qkv_ref, p_ref, in_ref, dq_ref)

    for g in range(groups):
        bg_ref[g] = jnp.sum(dq_ref[g].astype(F32), 0, keepdims=True)
        weight_products(g, x_t_ref, dattn_t_ref, dq_ref, ctx_ref, ga_ref)


WAYS = ("yzx", "yxz", "yxz", "xyz")


def whole_layer(
    n, x_ref, cot_ref, seg_c_ref, seg_r_ref, bias_ref, vec_ref, wq_hbm, wk_hbm, wv_hbm, wo_hbm, up_hbm, down_hbm,
    out_ref, out_peer_ref, in_ref, in_peer_ref, rd_ref, ru_ref, ra_ref, rb_ref, sums_ref,
    w_ref, wo_ref, up_ref, down_ref, bias_2, qkv_ref, p_ref, ctx_ref, xhat_ref, rstd_ref, low_ref, act_ref, slope_ref,
    acc_ref, dffn_ref, t_low_ref, t_grad_ref, small_ref, *rest_refs,
):
    half, mid, owned, shard = rest_refs[0:4], rest_refs[4:8], rest_refs[8:12], rest_refs[12:16]
    tiny, tiny_1, tiny_2, tiny_x, tiny_z, last = rest_refs[16:22]
    send, recv, send_z, recv_z, send_in, recv_in, g_send, g_recv, g_local = rest_refs[22:]
    seqs, length = seg_c_ref.shape[0], seg_c_ref.shape[1]
    groups, width, model = wo_ref.shape
    hidden = up_ref.shape[2]
    pairs = width // PAIR
    tokens = seqs * length
    step = hidden // 3
    block = 256
    rows_own = model // n
    depth = n // 4
    index = lax.axis_index("dp")
    x_index = lax.axis_index("mp")
    core, line, rest = index % 2, index // 2 % 2, index // 4
    to_core = {"dp": index + 1 - 2 * core}
    to_line = {"dp": index + 2 - 4 * line}
    to_x = {"mp": 1 - x_index}

    def to_rest(k):
        return {"dp": (rest + k) % depth * 4 + index % 4}

    barrier = pltpu.get_barrier_semaphore()
    peers = [to_core, to_line, to_x] + [to_rest(k) for k in range(1, depth)]
    for peer in peers:
        pl.semaphore_signal(barrier, inc=1, device_id=peer, device_id_type=MESH)
    pl.semaphore_wait(barrier, len(peers))

    def remote(src, dst, s, r, device):
        return pltpu.make_async_remote_copy(
            src_ref=src, dst_ref=dst, send_sem=s, recv_sem=r, device_id=device, device_id_type=MESH
        )

    def columns(c):
        return pl.ds(pl.multiple_of(c * step, step), step)

    def ends_of(kind, c, piece):
        if kind < 3:
            size = model // 4
            rows = pl.ds(pl.multiple_of(piece * size, size), size)
            return (wq_hbm, wk_hbm, wv_hbm)[kind].at[rows, :], w_ref.at[1, rows, kind * width : (kind + 1) * width]
        if kind == 3:
            size = width // 4
            rows = pl.ds(pl.multiple_of(piece * size, size), size)
            return wo_hbm.at[rows, :], wo_ref.at[1, rows, :]
        if kind == 4:
            size = model // 4
            rows = pl.ds(pl.multiple_of(piece * size, size), size)
            return up_hbm.at[rows, columns(c)], up_ref.at[1, rows, columns(c)]
        size = step // 4
        rows = pl.ds(pl.multiple_of(c * step + piece * size, size), size)
        return down_hbm.at[rows, :], down_ref.at[1, rows, :]

    def slot(kind, c):
        return kind if kind < 4 else (4 + c if kind == 4 else 7 + c)

    def over_x(kind, c=0):
        src, dst = ends_of(kind, c, 2 * line + core)
        i = slot(kind, c)
        return remote(src, dst, g_send.at[0, i], g_recv.at[0, i], to_x)

    def pass_on(kind, c, hop):
        at = ends_of(kind, c, 2 * (1 - line) + core if hop == 3 else 2 * line + core)[1]
        i = slot(kind, c)
        return remote(at, at, g_send.at[hop, i], g_recv.at[hop, i], to_line if hop == 2 else to_core)

    def first_hop(kind, c=0):
        over_x(kind, c).wait_recv()
        pass_on(kind, c, 2).start()
        pass_on(kind, c, 1).start()

    def second_hop(kind, c=0):
        pass_on(kind, c, 2).wait_recv()
        pass_on(kind, c, 3).start()

    def complete(kind, c=0):
        pass_on(kind, c, 1).wait_recv()
        pass_on(kind, c, 3).wait_recv()

    def sent(kind, c=0):
        over_x(kind, c).wait_send()
        for hop in (1, 2, 3):
            pass_on(kind, c, hop).wait_send()

    bias_over = remote(bias_ref, bias_2, send.at[4, 0], recv.at[4, 0], to_x)
    bias_over.start()
    for kind in range(4):
        over_x(kind).start()
    for c in range(3):
        over_x(4, c).start()
        over_x(5, c).start()
    own_copies = [
        pltpu.make_async_copy(src, dst, g_local.at[i])
        for i, (src, dst) in enumerate(
            [(w, w_ref.at[0, :, o * width : (o + 1) * width]) for o, w in enumerate((wq_hbm, wk_hbm, wv_hbm))]
            + [(wo_hbm, wo_ref.at[0]), (up_hbm, up_ref.at[0]), (down_hbm, down_ref.at[0])]
        )
    ]
    for copy in own_copies:
        copy.start()

    n_half, n_quarter = model // 2, model // 4
    cut = hidden // 2
    sources = (act_ref, slope_ref, up_ref.at[:, :, :cut], up_ref.at[:, :, cut:])

    def by_core(t):
        there = pl.ds(pl.multiple_of((1 - core) * n_half, n_half), n_half)
        return remote(sources[t].at[:, there, :], half[t], send.at[0, t], recv.at[0, t], to_core)

    def quarter_of(place):
        return pl.ds(pl.multiple_of(place * n_quarter, n_quarter), n_quarter)

    def own_rows(place):
        return pl.ds(pl.multiple_of(place * rows_own, rows_own), rows_own)

    def by_first(t):
        if WAYS[t] == "xyz":
            return remote(half[t].at[1], mid[t], send.at[1, t], recv.at[1, t], to_x)
        return remote(half[t].at[:, quarter_of(1 - line), :], mid[t], send.at[1, t], recv.at[1, t], to_line)

    def by_second(t):
        if WAYS[t] == "xyz":
            return remote(mid[t].at[quarter_of(1 - line), :], owned[t], send.at[2, t], recv.at[2, t], to_line)
        if WAYS[t] == "yzx":
            return remote(owned[t].at[1], last, send.at[2, t], recv.at[2, t], to_x)
        return remote(mid[t].at[1], owned[t], send.at[2, t], recv.at[2, t], to_x)

    def by_rest(t, k):
        there = own_rows((rest + k) % depth)
        source = mid[t].at[:, there, :] if WAYS[t] == "yzx" else owned[t].at[there, :]
        return remote(source, shard[t].at[k - 1], send_z.at[t, k - 1], recv_z.at[t, k - 1], to_rest(k))

    def start_rest(t):
        for k in range(1, depth):
            by_rest(t, k).start()

    def rest_sum(t):
        if WAYS[t] == "yzx":
            total = mid[t][:, own_rows(rest), :].astype(F32)
        else:
            total = owned[t][own_rows(rest), :].astype(F32)
        for k in range(1, depth):
            by_rest(t, k).wait_recv()
            total = total + shard[t][k - 1].astype(F32)
        return total

    def after_core(t):
        by_core(t).wait_recv()
        for g in range(groups):
            add_rows(half[t].at[g], sources[t].at[g], core * n_half, 96)
        by_first(t).start()

    def after_first(t):
        by_first(t).wait_recv()
        if WAYS[t] == "xyz":
            add_rows(mid[t], half[t].at[0], 0, 96)
        else:
            for g in range(groups):
                add_rows(mid[t].at[g], half[t].at[g], line * n_quarter, 96)
        if WAYS[t] == "yzx":
            start_rest(t)
        else:
            by_second(t).start()

    def after_second(t, out):
        if WAYS[t] == "yzx":
            total = rest_sum(t)
            out[...] = total[0]
            owned[t][...] = total.astype(BF16)
            by_second(t).start()
            return
        by_second(t).wait_recv()
        if WAYS[t] == "xyz":
            add_rows(owned[t], mid[t], line * n_quarter, 96)
        else:
            add_rows(owned[t], mid[t].at[0], 0, 96)
        start_rest(t)

    def finish(t, out):
        if WAYS[t] == "yzx":
            by_second(t).wait_recv()
            out[...] += last[...].astype(F32)
        else:
            out[...] = rest_sum(t)

    def send_output(b):
        rows = pl.ds(pl.multiple_of(b * length, length), length)
        return remote(out_ref.at[rows, :], out_peer_ref.at[rows, :], send_in.at[1, b], recv_in.at[1, b], to_x)

    def send_input(s):
        rows = pl.ds(pl.multiple_of(s * length, length), length)
        return remote(in_ref.at[rows, :], in_peer_ref.at[rows, :], send_in.at[0, s], recv_in.at[0, s], to_x)

    attn_gain, attn_shift, down_bias = vec_ref[0:1, :], vec_ref[1:2, :], vec_ref[2:3, :]
    ffn_gain, ffn_shift, out_bias = vec_ref[3:4, :], vec_ref[4:5, :], vec_ref[5:6, :]

    def attend(s, g, biases):
        rows = pl.ds(pl.multiple_of(s * length, length), length)
        x = x_ref[rows, :]
        mask = seg_c_ref[s] == seg_r_ref[s]
        y = mm(x, w_ref[g])
        query = (0.125 * (y[:, :width] + biases[0:1, :width])).astype(BF16)
        key = y[:, width : 2 * width].astype(BF16)
        value = (y[:, 2 * width :] + biases[0:1, width : 2 * width]).astype(BF16)
        qkv_ref[g, rows, :width] = query
        qkv_ref[g, rows, width : 2 * width] = key
        qkv_ref[g, rows, 2 * width :] = value
        parts = []
        for p in range(pairs):
            at = slice(p * PAIR, (p + 1) * PAIR)
            k = key[:, at]
            both = None
            for h, (q, v) in enumerate(zip(halves(query[:, at]), halves(value[:, at]))):
                scores = jnp.where(mask, mm_t(q, k), -1000000000.0)
                expo = jnp.exp(scores - jnp.max(scores, -1, keepdims=True))
                probs = (expo * (1.0 / jnp.sum(expo, -1, keepdims=True))).astype(BF16)
                p_ref[s, (g * pairs + p) * 2 + h] = probs
                part = mm(probs, v)
                both = part if both is None else both + part
            parts.append(both.astype(BF16))
        ctx = jnp.concatenate(parts, 1)
        ctx_ref[g, rows, :] = ctx
        return mm(ctx, wo_ref[g])

    for copy in own_copies[:4]:
        copy.wait()

    @pl.loop(0, seqs)
    def _(s):
        rows = pl.ds(pl.multiple_of(s * length, length), length)
        acc_ref[rows, :] = x_ref[rows, :].astype(F32) + out_bias + attend(s, 0, bias_ref)
        for kind in range(3):

            @pl.when(s == min(kind, seqs - 1))
            def _():
                first_hop(kind)

    first_hop(3)
    for kind in range(4):
        second_hop(kind)
    for kind in range(4):
        complete(kind)
    bias_over.wait()

    @pl.loop(0, seqs)
    def _(s):
        rows = pl.ds(pl.multiple_of(s * length, length), length)
        attn = acc_ref[rows, :] + attend(s, 1, bias_2)
        centred = attn - jnp.mean(attn, -1, keepdims=True)
        rstd = lax.rsqrt(jnp.mean(centred * centred, -1, keepdims=True) + EPS)
        xhat = centred * rstd
        xhat_ref[rows, :] = xhat
        rstd_ref[rows, :] = rstd
        low_ref[rows, :] = (xhat * attn_gain + attn_shift).astype(BF16)

        @pl.when(s == min(1, seqs - 1))
        def _():
            first_hop(4, 0)
            first_hop(5, 0)

    for copy in own_copies[4:]:
        copy.wait()
    store_by_owner(t_low_ref, low_ref[...].T, slice(None), n)

    def expand(c, g, biases):
        at = columns(c)
        bias_at = pl.ds(pl.multiple_of(2 * width + c * step, 128), step)

        @pl.loop(0, tokens // block)
        def _(b):
            rows = pl.ds(pl.multiple_of(b * block, block), block)
            u = mm(low_ref[rows, :], up_ref[g, :, at]) + biases[0:1, bias_at]
            square = u * u
            t = jnp.tanh(GELU_C * (u + 0.044715 * square * u))
            gate = 0.5 * (1.0 + t)
            act = (u * gate).astype(BF16)
            act_ref[g, rows, at] = act
            slope = gate + (0.5 * GELU_C) * u * (1.0 - t * t) * (1.0 + 0.134145 * square)
            slope_ref[g, rows, at] = slope.astype(BF16)
            acc_ref[rows, :] += mm(act, down_ref[g, at, :])

    acc_ref[...] = jnp.zeros_like(acc_ref)

    @pl.loop(0, 3)
    def _(c):
        expand(c, 0, bias_ref)

        @pl.when(c == 0)
        def _():
            second_hop(4, 0)
            second_hop(5, 0)

        @pl.when(c == 1)
        def _():
            first_hop(4, 1)
            first_hop(5, 1)

    @pl.loop(0, 3)
    def _(c):
        complete(4, c)
        complete(5, c)
        expand(c, 1, bias_2)

        @pl.when(c == 0)
        def _():
            second_hop(4, 1)
            second_hop(5, 1)
            first_hop(4, 2)
            first_hop(5, 2)

        @pl.when(c == 1)
        def _():
            second_hop(4, 2)
            second_hop(5, 2)

    small_ref[...] = jnp.zeros_like(small_ref)

    @pl.loop(0, seqs)
    def _(b):
        rows = pl.ds(pl.multiple_of(b * length, length), length)
        resid = xhat_ref[rows, :] * attn_gain + attn_shift + acc_ref[rows, :] + down_bias
        centred = resid - jnp.mean(resid, -1, keepdims=True)
        rstd = lax.rsqrt(jnp.mean(centred * centred, -1, keepdims=True) + EPS)
        xhat = centred * rstd
        out_ref[rows, :] = (xhat * ffn_gain + ffn_shift).astype(BF16)
        cot = cot_ref[rows, :].astype(F32)
        grad = norm_backward(xhat, rstd, ffn_gain, cot)
        acc_ref[rows, :] = grad
        dffn_ref[rows, :] = grad.astype(BF16)
        small_ref[3:4, :] += jnp.sum(grad, 0, keepdims=True)
        small_ref[4:5, :] += jnp.sum(cot * xhat, 0, keepdims=True)
        small_ref[5:6, :] += jnp.sum(cot, 0, keepdims=True)
        send_output(b).start()

    store_by_owner(t_grad_ref, dffn_ref[...].T, slice(None), n)

    def product(left, place, g, at):
        made = [
            mm(left[b * block : (b + 1) * block, :], place[g, :, at]).astype(BF16) for b in range(model // block)
        ]
        for b, value in enumerate(made):
            place[g, b * block : (b + 1) * block, at] = value

    tiny[...] = jnp.zeros_like(tiny)
    for g in range(groups):

        @pl.loop(0, 3)
        def _(c):
            product(t_grad_ref, act_ref, g, columns(c))

    by_core(0).start()
    for g in range(groups):

        @pl.loop(0, 3)
        def _(c):
            at = columns(c)
            total = jnp.zeros((1, step), F32)
            for b in range(tokens // block):
                rows = slice(b * block, (b + 1) * block)
                d_upper = mm_t(dffn_ref[rows, :], down_ref[g, at, :]) * slope_ref[g, rows, at].astype(F32)
                total = total + jnp.sum(d_upper, 0, keepdims=True)
                d_low = d_upper.astype(BF16)
                slope_ref[g, rows, at] = d_low
                acc_ref[rows, :] += mm_t(d_low, up_ref[g, :, at])
            tiny[3 + g, 0:1, at] = total
            product(t_low_ref, slope_ref, g, at)
            if g == 0:

                @pl.when(c == 1)
                def _():
                    after_core(0)

    by_core(1).start()

    @pl.loop(0, seqs)
    def _(b):
        rows = pl.ds(pl.multiple_of(b * length, length), length)
        d_normed = acc_ref[rows, :]
        xhat = xhat_ref[rows, :]
        grad = norm_backward(xhat, rstd_ref[rows, :], attn_gain, d_normed)
        acc_ref[rows, :] = grad
        small_ref[0:1, :] += jnp.sum(grad, 0, keepdims=True)
        small_ref[1:2, :] += jnp.sum(d_normed * xhat, 0, keepdims=True)
        small_ref[2:3, :] += jnp.sum(d_normed, 0, keepdims=True)

    store_by_owner(t_low_ref, x_ref[...].T, slice(None), n)

    @pl.loop(0, seqs)
    def _(s):
        backward_sequence(
            s, lambda v, at: store_by_owner(t_grad_ref, v, at, n),
            acc_ref, w_ref, wo_ref, qkv_ref, p_ref, in_ref, qkv_ref,
        )
        send_input(s).start()

        @pl.when(s == 0)
        def _():
            after_core(1)

        @pl.when(s == min(1, seqs - 1))
        def _():
            after_first(0)

    for kind in range(4):
        sent(kind)
    for c in range(3):
        sent(4, c)
        sent(5, c)
    for g in range(groups):
        weight_products(g, t_low_ref, t_grad_ref, qkv_ref, ctx_ref, up_ref)
    by_core(2).start()
    by_core(3).start()
    for g in range(groups):
        column = jnp.sum(qkv_ref[g].astype(F32), 0, keepdims=True)
        tiny[g, 0:1, :width] = column[:, :width]
        tiny[g, 0:1, width : 2 * width] = column[:, 2 * width :]
        tiny[g, 1:2, :] = tiny[3 + g, 0:1, :]
    tiny[2, :, :model] = small_ref[...]

    tiny_core = remote(tiny.at[0:3], tiny_1, send.at[3, 1], recv.at[3, 1], to_core)
    tiny_line = remote(tiny_1, tiny_2, send.at[3, 2], recv.at[3, 2], to_line)
    tiny_over = remote(tiny_2.at[1:3], tiny_x, send.at[3, 3], recv.at[3, 3], to_x)

    def tiny_rest(k):
        return remote(tiny_x, tiny_z.at[k - 1], send_z.at[4, k - 1], recv_z.at[4, k - 1], to_rest(k))

    tiny_core.start()
    after_core(2)
    after_core(3)
    tiny_core.wait_recv()
    tiny_1[...] += tiny[0:3]
    tiny_line.start()
    after_first(1)
    after_second(0, rd_ref)
    tiny_line.wait_recv()
    tiny_2[...] += tiny_1[...]
    tiny_over.start()
    after_first(3)
    after_first(2)
    after_second(1, ru_ref)
    tiny_over.wait_recv()
    tiny_x[0] += tiny_2[0]
    tiny_x[1] += tiny_2[2]
    for k in range(1, depth):
        tiny_rest(k).start()
    finish(0, rd_ref)
    after_second(3, rb_ref)
    after_second(2, ra_ref)
    finish(1, ru_ref)
    total = tiny_x[...]
    for k in range(1, depth):
        tiny_rest(k).wait_recv()
        total = total + tiny_z[k - 1]
    sums_ref[...] = total
    finish(3, rb_ref)
    finish(2, ra_ref)
    for s in range(seqs):
        send_output(s).wait()
        send_input(s).wait()
    for t in range(4):
        by_core(t).wait_send()
        by_first(t).wait_send()
        by_second(t).wait_send()
        for k in range(1, depth):
            by_rest(t, k).wait_send()
    tiny_core.wait_send()
    tiny_line.wait_send()
    tiny_over.wait_send()
    for k in range(1, depth):
        tiny_rest(k).wait_send()


def call(kernel, outs, scratch, flops, *args, far=(), far_out=(), collective=None):
    shapes = [jax.ShapeDtypeStruct(s, d) for s, d in outs]
    moved = sum(a.size * a.dtype.itemsize for a in args) + sum(s.size * s.dtype.itemsize for s in shapes)
    vmem = pl.BlockSpec(memory_space=pltpu.VMEM)
    return pl.pallas_call(
        kernel,
        out_shape=shapes,
        in_specs=[pl.BlockSpec(memory_space=pl.ANY) if i in far else vmem for i in range(len(args))],
        out_specs=[pl.BlockSpec(memory_space=pl.ANY) if i in far_out else vmem for i in range(len(shapes))],
        scratch_shapes=[pltpu.VMEM(*s) if isinstance(s, tuple) else s for s in scratch],
        compiler_params=pltpu.CompilerParams(
            vmem_limit_bytes=VMEM_LIMIT, collective_id=collective, has_side_effects=collective is not None
        ),
        cost_estimate=pl.CostEstimate(flops=flops, bytes_accessed=moved, transcendentals=0),
    )(*args)


def factors_of(n):
    found = []
    while n > 4 or (n > 1 and len(found) < 2):
        found.append(2)
        n //= 2
    return found + ([n] if n > 1 else [])


def swap(v):
    return lax.ppermute(v, "mp", [(0, 1), (1, 0)])


def shift_dp(v, n, stride, factor, k):
    def target(d):
        i = (d // stride) % factor
        return d + ((i + k) % factor - i) * stride

    return lax.ppermute(v, "dp", [(d, target(d)) for d in range(n)])


def with_peer(own, n):
    core = lax.axis_index("dp") % 2
    half = own.shape[0] // 2
    mine = swap(lax.dynamic_slice_in_dim(own, core * half, half, 0))
    other = shift_dp(mine, n, 1, 2, 1)
    first = core == 0
    peer = jnp.concatenate([jnp.where(first, mine, other), jnp.where(first, other, mine)], 0)
    return jnp.stack([own, peer])


def reduce_to_owner(grad, n):
    index = lax.axis_index("dp")
    rows = grad.shape[1] // n
    left = grad.reshape(2, n, rows, grad.shape[2])
    stride = 1
    for factor in factors_of(n):
        parts = left.reshape(2, left.shape[1] // factor, factor, rows, left.shape[3])
        i = (index // stride) % factor

        def pick(at):
            return lax.dynamic_index_in_dim(parts, at, 2, keepdims=False)

        total = pick(i).astype(F32)
        for k in range(1, factor):
            total = total + shift_dp(pick((i + k) % factor), n, stride, factor, k).astype(F32)
        left = total.astype(BF16)
        stride *= factor
    left = left.reshape(2, rows, left.shape[3])
    return left[0].astype(F32) + swap(left[1]).astype(F32)


def per_device(
    n, layer_input, doc_lengths, q_weight, q_bias, k_weight, v_weight, v_bias, out_weight, out_bias,
    attn_gain, attn_shift, up_weight, up_bias, down_weight, down_bias, ffn_gain, ffn_shift, cotangent,
):
    rows = doc_lengths.shape[0]
    tokens, model = layer_input.shape
    length = tokens // rows
    part = length // 2
    mine = rows * part
    width = q_weight.shape[1]
    hidden = up_weight.shape[1]
    heads = width // HD
    x_index = lax.axis_index("mp")

    ends = jnp.cumsum(doc_lengths, axis=-1, dtype=jnp.int32)
    start = jnp.sum(jnp.where(doc_lengths == part, ends - part, 0), -1)
    place = jnp.arange(length, dtype=jnp.int32)
    segment = jnp.sum((place[None, :, None] >= ends[:, None, :]).astype(jnp.int32), -1, dtype=jnp.int32)
    before = place[None, :part] < start[:, None]
    from_high = before != (x_index == 1)

    def take(v):
        v = v.reshape(rows, 2, part, model)
        return jnp.where(from_high[:, :, None], v[:, 1], v[:, 0]).reshape(mine, model)

    def give(own, other):
        own, other = own.reshape(rows, part, model), other.reshape(rows, part, model)
        low = jnp.where(from_high[:, :, None], other, own)
        high = jnp.where(from_high[:, :, None], own, other)
        return jnp.stack([low, high], 1).reshape(tokens, model)

    seg = jnp.where(from_high, segment[:, part:], segment[:, :part])

    x = take(layer_input)
    cot = take(cotangent)
    own_bias = jnp.concatenate([q_bias, v_bias, up_bias])
    remote = (
        (model // n) % 16 == 0 and n % 4 == 0 and n > 4
        and hidden == 2 * model and 4 * width == hidden and hidden % 384 == 0 and rows >= 3
    )
    if remote:
        depth = n // 4
        dma = pltpu.SemaphoreType.DMA
        wide = (hidden, hidden, model, model)
        quarter = model // 4
        vectors = jnp.stack([attn_gain, attn_shift, down_bias, ffn_gain, ffn_shift, out_bias]).astype(F32)
        output, output_peer, grad_in, grad_in_peer, g_down, g_up, g_first, g_last, sums = call(
            functools.partial(whole_layer, n),
            [((mine, model), BF16)] * 4
            + [((model // n, c), F32) for c in wide]
            + [((2, 8, hidden), F32)],
            [
                ((2, model, 3 * width), BF16),
                ((2, width, model), BF16),
                ((2, model, hidden), BF16),
                ((2, hidden, model), BF16),
                ((1, 2 * width + hidden), F32),
                ((2, mine, 3 * width), BF16),
                ((rows, 2 * heads, part, part), BF16),
                ((2, mine, width), BF16),
                ((mine, model), F32),
                ((mine, 1), F32),
                ((mine, model), BF16),
                ((2, model, hidden), BF16),
                ((2, model, hidden), BF16),
                ((mine, model), F32),
                ((mine, model), BF16),
                ((model, mine), BF16),
                ((model, mine), BF16),
                ((8, model), F32),
            ]
            + [((2, model // 2, c), BF16) for c in wide]
            + [((2 * quarter, c) if w == "xyz" else (2, quarter, c), BF16) for w, c in zip(WAYS, wide)]
            + [((2, model // n, c) if w == "yzx" else (quarter, c), BF16) for w, c in zip(WAYS, wide)]
            + [((depth - 1,) + (2,) * (w == "yzx") + (model // n, c), BF16) for w, c in zip(WAYS, wide)]
            + [
                ((5, 8, hidden), F32),
                ((3, 8, hidden), F32),
                ((3, 8, hidden), F32),
                ((2, 8, hidden), F32),
                ((depth - 1, 2, 8, hidden), F32),
                ((model // n, hidden), BF16),
                dma((5, 4)), dma((5, 4)), dma((5, depth - 1)), dma((5, depth - 1)), dma((2, rows)), dma((2, rows)),
                dma((4, 10)), dma((4, 10)), dma((6,)),
            ],
            2 * mine * model * (24 * width + 12 * hidden),
            x, cot, seg[:, :, None], seg[:, None, :], own_bias.astype(F32)[None], vectors,
            q_weight, k_weight, v_weight, out_weight, up_weight, down_weight,
            far=(6, 7, 8, 9, 10, 11), far_out=(1, 3), collective=0,
        )
        g_attn = jnp.concatenate([g_first, g_last], -1)
        small = sums[1, :, :model]
        sums = jnp.concatenate([sums[0, 0, : 2 * width], sums[0, 1]])
    else:
        w_qkv = with_peer(jnp.concatenate([q_weight, k_weight, v_weight], 1), n)
        w_out = with_peer(out_weight, n)
        w_up = with_peer(up_weight, n)
        w_down = with_peer(down_weight, n)
        bias = jnp.stack([own_bias, swap(own_bias)]).astype(F32)[:, None, :]
        b_qkv = jnp.concatenate([bias[..., :width], jnp.zeros_like(bias[..., :width]), bias[..., width : 2 * width]], -1)
        b_up = bias[..., 2 * width :]
        vectors = jnp.stack([attn_gain, attn_shift, down_bias, ffn_gain, ffn_shift]).astype(F32)

        qkv, probs, ctx, xhat, rstd, low = call(
            attention_forward,
            [
                ((2, mine, 3 * width), BF16),
                ((rows, 2 * heads, part, part), BF16),
                ((2, mine, width), BF16),
                ((mine, model), F32),
                ((mine, 1), F32),
                ((mine, model), BF16),
            ],
            [],
            2 * mine * model * 8 * width,
            x, w_qkv, b_qkv, w_out, seg[:, :, None], seg[:, None, :],
            out_bias.astype(F32)[None], vectors[0:1], vectors[1:2],
        )
        output, g_down, g_up, d_resid, small, up_bias_grad = call(
            feed_forward,
            [
                ((mine, model), BF16),
                ((2, model, hidden), BF16),
                ((2, model, hidden), BF16),
                ((mine, model), F32),
                ((8, model), F32),
                ((2, 1, hidden), F32),
            ],
            [
                ((2, mine, hidden), BF16),
                ((2, mine, hidden), BF16),
                ((mine, model), F32),
                ((mine, model), BF16),
                ((model, mine), BF16),
                ((model, mine), BF16),
            ],
            2 * mine * model * 2 * hidden * 6,
            low, xhat, rstd, w_up, b_up, w_down, vectors, cot,
        )
        scratch = [((2, mine, 3 * width), BF16), ((model, mine), BF16), ((model, mine), BF16)]
        flops = 2 * mine * model * 16 * width
        output_peer = swap(output)
        grad_in, g_attn, bias_grad = call(
            attention_backward_plain,
            [((mine, model), BF16), ((2, model, 4 * width), BF16), ((2, 1, 3 * width), F32)],
            scratch, flops, x, d_resid, w_qkv, w_out, qkv, probs, ctx,
        )
        grad_in_peer = swap(grad_in)
        g_down, g_up, g_attn = (reduce_to_owner(v, n) for v in (g_down, g_up, g_attn))
        sums = jnp.concatenate([bias_grad[:, 0, :width], bias_grad[:, 0, 2 * width :], up_bias_grad[:, 0]], -1)
        sums = jnp.where(x_index == 0, sums, sums[::-1])
        sums, small = lax.psum((sums, small), ("dp", "mp"))
        sums = lax.dynamic_index_in_dim(sums, x_index, 0, keepdims=False)
    layer_output = give(output, output_peer)
    input_grad = give(grad_in, grad_in_peer)
    down_weight_grad = g_down.T
    up_weight_grad = g_up
    return (
        layer_output,
        input_grad,
        g_attn[:, :width],
        sums[:width],
        g_attn[:, width : 2 * width],
        g_attn[:, 2 * width : 3 * width],
        sums[width : 2 * width],
        g_attn[:, 3 * width :].T,
        small[0],
        small[1],
        small[2],
        up_weight_grad,
        sums[2 * width :],
        down_weight_grad,
        small[3],
        small[4],
        small[5],
    )


def solution(mesh):
    in_specs = (
        P("dp", None), P("dp", None), P(None, "mp"), P("mp"), P(None, "mp"), P(None, "mp"), P("mp"),
        P("mp", None), P(), P(), P(), P(None, "mp"), P("mp"), P("mp", None), P(), P(), P(), P("dp", None),
    )
    out_specs = (
        P("dp", None), P("dp", None), P("dp", "mp"), P("mp"), P("dp", "mp"), P("dp", "mp"), P("mp"),
        P("mp", "dp"), P(), P(), P(), P("dp", "mp"), P("mp"), P("mp", "dp"), P(), P(), P(),
    )
    return jax.shard_map(
        functools.partial(per_device, mesh.shape["dp"]),
        mesh=mesh, in_specs=in_specs, out_specs=out_specs, check_vma=False,
    )
```

```python
import functools

import jax
import jax.numpy as jnp
from jax import lax
from jax.experimental import pallas as pl
from jax.experimental.pallas import tpu as pltpu
from jax.sharding import PartitionSpec as P

HD = 64
PAIR = 2 * HD
EPS = 1e-12
GELU_C = 0.7978845608028654
F32 = jnp.float32
BF16 = jnp.bfloat16
CHUNK = 512
VMEM_LIMIT = 67043328
MESH = pl.DeviceIdType.MESH


def mm(a, b):
    return jnp.dot(a, b, preferred_element_type=F32)


def mm_t(a, b):
    return lax.dot_general(a, b, (((1,), (1,)), ((), ())), preferred_element_type=F32)


def t_mm(a, b):
    return lax.dot_general(a, b, (((0,), (0,)), ((), ())), preferred_element_type=F32)


def halves(v):
    lane = lax.broadcasted_iota(jnp.int32, v.shape, 1)
    zero = jnp.zeros_like(v)
    return jnp.where(lane < HD, v, zero), jnp.where(lane < HD, zero, v)


def attention_forward(
    x_ref, w_ref, b_ref, wo_ref, seg_c_ref, seg_r_ref, bo_ref, gain_ref, shift_ref,
    qkv_ref, p_ref, ctx_ref, xhat_ref, rstd_ref, low_ref,
):
    seqs, length = seg_c_ref.shape[0], seg_c_ref.shape[1]
    groups, width = wo_ref.shape[0], wo_ref.shape[1]
    pairs = width // PAIR

    @pl.loop(0, seqs)
    def _(s):
        rows = pl.ds(pl.multiple_of(s * length, length), length)
        x = x_ref[rows, :]
        mask = seg_c_ref[s] == seg_r_ref[s]
        attn = x.astype(F32) + bo_ref[...]
        for g in range(groups):
            y = mm(x, w_ref[g]) + b_ref[g]
            query = (0.125 * y[:, :width]).astype(BF16)
            key = y[:, width : 2 * width].astype(BF16)
            value = y[:, 2 * width :].astype(BF16)
            qkv_ref[g, rows, :width] = query
            qkv_ref[g, rows, width : 2 * width] = key
            qkv_ref[g, rows, 2 * width :] = value
            parts = []
            for p in range(pairs):
                at = slice(p * PAIR, (p + 1) * PAIR)
                k = key[:, at]
                both = None
                for h, (q, v) in enumerate(zip(halves(query[:, at]), halves(value[:, at]))):
                    scores = jnp.where(mask, mm_t(q, k), -1000000000.0)
                    expo = jnp.exp(scores - jnp.max(scores, -1, keepdims=True))
                    probs = (expo * (1.0 / jnp.sum(expo, -1, keepdims=True))).astype(BF16)
                    p_ref[s, (g * pairs + p) * 2 + h] = probs
                    part = mm(probs, v)
                    both = part if both is None else both + part
                parts.append(both.astype(BF16))
            ctx = jnp.concatenate(parts, 1)
            ctx_ref[g, rows, :] = ctx
            attn = attn + mm(ctx, wo_ref[g])
        mean = jnp.mean(attn, -1, keepdims=True)
        centred = attn - mean
        rstd = lax.rsqrt(jnp.mean(centred * centred, -1, keepdims=True) + EPS)
        xhat = centred * rstd
        xhat_ref[rows, :] = xhat
        rstd_ref[rows, :] = rstd
        low_ref[rows, :] = (xhat * gain_ref[...] + shift_ref[...]).astype(BF16)


def norm_backward(xhat, rstd, gain, grad):
    scaled = grad * gain
    return rstd * (
        scaled
        - jnp.mean(scaled, -1, keepdims=True)
        - xhat * jnp.mean(scaled * xhat, -1, keepdims=True)
    )


def add_rows(dst, src, offset, step):
    step = min(step, dst.shape[0])

    @pl.loop(0, dst.shape[0] // step)
    def _(i):
        here = pl.ds(pl.multiple_of(i * step, step), step)
        there = pl.ds(pl.multiple_of(offset + i * step, step), step)
        dst[here, :] = (dst[here, :].astype(F32) + src[there, :].astype(F32)).astype(dst.dtype)


def store_by_owner(dst, value, at, n):
    rows = value.shape[0] // n
    for d in range(n):
        place = (d % 2) * (n // 2) + (d // 2 % 2) * (n // 4) + d // 4
        dst[place * rows : (place + 1) * rows, at] = value[d * rows : (d + 1) * rows, :]


def feed_forward(
    low_ref, xhat_ref, rstd_ref, up_ref, ub_ref, down_ref, vec_ref, cot_ref,
    out_ref, gd_ref, gu_ref, d_resid_ref, small_ref, ubg_ref,
    act_ref, slope_ref, acc_ref, dffn_ref, dffn_t_ref, low_t_ref,
):
    tokens, width = low_ref.shape
    groups, hidden = up_ref.shape[0], up_ref.shape[2]
    step = min(CHUNK, hidden)
    per = hidden // step
    block = 256
    low_t_ref[...] = low_ref[...].T
    acc_ref[...] = jnp.zeros_like(acc_ref)

    @pl.loop(0, groups * per)
    def _(i):
        g = i // per
        at = pl.ds(pl.multiple_of((i % per) * step, step), step)

        @pl.loop(0, tokens // block)
        def _(b):
            rows = pl.ds(pl.multiple_of(b * block, block), block)
            u = mm(low_ref[rows, :], up_ref[g, :, at]) + ub_ref[g, :, at]
            square = u * u
            t = jnp.tanh(GELU_C * (u + 0.044715 * square * u))
            half = 0.5 * (1.0 + t)
            act = (u * half).astype(BF16)
            act_ref[g, rows, at] = act
            slope = half + (0.5 * GELU_C) * u * (1.0 - t * t) * (1.0 + 0.134145 * square)
            slope_ref[g, rows, at] = slope.astype(BF16)
            acc_ref[rows, :] += mm(act, down_ref[g, at, :])

    small_ref[...] = jnp.zeros_like(small_ref)
    attn_gain, attn_shift = vec_ref[0:1, :], vec_ref[1:2, :]
    down_bias = vec_ref[2:3, :]
    ffn_gain, ffn_shift = vec_ref[3:4, :], vec_ref[4:5, :]

    @pl.loop(0, tokens // block)
    def _(b):
        rows = pl.ds(pl.multiple_of(b * block, block), block)
        resid = xhat_ref[rows, :] * attn_gain + attn_shift + acc_ref[rows, :] + down_bias
        centred = resid - jnp.mean(resid, -1, keepdims=True)
        rstd = lax.rsqrt(jnp.mean(centred * centred, -1, keepdims=True) + EPS)
        xhat = centred * rstd
        out_ref[rows, :] = (xhat * ffn_gain + ffn_shift).astype(BF16)
        cot = cot_ref[rows, :].astype(F32)
        grad = norm_backward(xhat, rstd, ffn_gain, cot)
        acc_ref[rows, :] = grad
        dffn_ref[rows, :] = grad.astype(BF16)
        small_ref[3:4, :] += jnp.sum(grad, 0, keepdims=True)
        small_ref[4:5, :] += jnp.sum(cot * xhat, 0, keepdims=True)
        small_ref[5:6, :] += jnp.sum(cot, 0, keepdims=True)

    dffn_t_ref[...] = dffn_ref[...].T

    @pl.loop(0, groups * per)
    def _(i):
        g = i // per
        at = pl.ds(pl.multiple_of((i % per) * step, step), step)
        total = jnp.zeros((1, step), F32)
        for b in range(tokens // block):
            rows = slice(b * block, (b + 1) * block)
            d_upper = mm_t(dffn_ref[rows, :], down_ref[g, at, :]) * slope_ref[g, rows, at].astype(F32)
            total = total + jnp.sum(d_upper, 0, keepdims=True)
            d_low = d_upper.astype(BF16)
            slope_ref[g, rows, at] = d_low
            acc_ref[rows, :] += mm_t(d_low, up_ref[g, :, at])
        ubg_ref[g, :, at] = total
        for b in range(width // block):
            rows = slice(b * block, (b + 1) * block)
            gd_ref[g, rows, at] = mm(dffn_t_ref[rows, :], act_ref[g, :, at]).astype(BF16)
            gu_ref[g, rows, at] = mm(low_t_ref[rows, :], slope_ref[g, :, at]).astype(BF16)

    @pl.loop(0, tokens // block)
    def _(b):
        rows = pl.ds(pl.multiple_of(b * block, block), block)
        d_normed = acc_ref[rows, :]
        xhat = xhat_ref[rows, :]
        grad = norm_backward(xhat, rstd_ref[rows, :], attn_gain, d_normed)
        d_resid_ref[rows, :] = grad
        small_ref[0:1, :] += jnp.sum(grad, 0, keepdims=True)
        small_ref[1:2, :] += jnp.sum(d_normed * xhat, 0, keepdims=True)
        small_ref[2:3, :] += jnp.sum(d_normed, 0, keepdims=True)


def backward_sequence(s, put, d_resid_ref, w_ref, wo_ref, qkv_ref, p_ref, in_ref, dq_ref):
    length, groups, width = p_ref.shape[2], wo_ref.shape[0], wo_ref.shape[1]
    pairs = width // PAIR
    rows = pl.ds(pl.multiple_of(s * length, length), length)
    d_resid = d_resid_ref[rows, :]
    d_attn = d_resid.astype(BF16)
    put(d_attn.T, rows)
    total = d_resid
    for g in range(groups):
        d_ctx = mm_t(d_attn, wo_ref[g]).astype(BF16)
        for p in range(pairs):
            at = slice(p * PAIR, (p + 1) * PAIR)
            q_at, k_at, v_at = (slice(o * width + p * PAIR, o * width + (p + 1) * PAIR) for o in range(3))
            value = qkv_ref[g, rows, v_at]
            q_pair = halves(qkv_ref[g, rows, q_at])
            k_pair = halves(qkv_ref[g, rows, k_at])
            c_pair = halves(d_ctx[:, at])
            dq = dk = dv = None
            for h in range(2):
                low = p_ref[s, (g * pairs + p) * 2 + h]
                probs = low.astype(F32)
                d_probs = mm_t(c_pair[h], value)
                inner = jnp.sum(probs * d_probs, -1, keepdims=True)
                d_scores = (probs * (d_probs - inner)).astype(BF16)
                dv_h = t_mm(low, c_pair[h])
                dq_h = mm(d_scores, k_pair[h])
                dk_h = t_mm(d_scores, q_pair[h])
                dq = dq_h if dq is None else dq + dq_h
                dk = dk_h if dk is None else dk + dk_h
                dv = dv_h if dv is None else dv + dv_h
            dq_ref[g, rows, q_at] = (0.125 * dq).astype(BF16)
            dq_ref[g, rows, k_at] = dk.astype(BF16)
            dq_ref[g, rows, v_at] = dv.astype(BF16)
        total = total + mm_t(dq_ref[g, rows, :], w_ref[g])
    in_ref[rows, :] = total.astype(BF16)


def weight_products(g, x_t_ref, dattn_t_ref, dq_ref, ctx_ref, ga_ref):
    block, wide = 256, dq_ref.shape[2]

    @pl.loop(0, x_t_ref.shape[0] // block)
    def _(b):
        rows = pl.ds(pl.multiple_of(b * block, block), block)
        ga_ref[g, rows, :wide] = mm(x_t_ref[rows, :], dq_ref[g]).astype(BF16)
        ga_ref[g, rows, wide:] = mm(dattn_t_ref[rows, :], ctx_ref[g]).astype(BF16)


def attention_backward_plain(
    x_ref, d_resid_ref, w_ref, wo_ref, qkv_ref, p_ref, ctx_ref,
    in_ref, ga_ref, bg_ref,
    dq_ref, dattn_t_ref, x_t_ref,
):
    groups, width = wo_ref.shape[0], wo_ref.shape[1]
    x_t_ref[...] = x_ref[...].T

    def put(v, at):
        dattn_t_ref[:, at] = v

    @pl.loop(0, p_ref.shape[0])
    def _(s):
        backward_sequence(s, put, d_resid_ref, w_ref, wo_ref, qkv_ref, p_ref, in_ref, dq_ref)

    for g in range(groups):
        bg_ref[g] = jnp.sum(dq_ref[g].astype(F32), 0, keepdims=True)
        weight_products(g, x_t_ref, dattn_t_ref, dq_ref, ctx_ref, ga_ref)


WAYS = ("yzx", "yxz", "yxz", "xyz")


def whole_layer(
    n, x_ref, cot_ref, seg_c_ref, seg_r_ref, bias_ref, vec_ref, wq_hbm, wk_hbm, wv_hbm, wo_hbm, up_hbm, down_hbm,
    out_ref, out_peer_ref, in_ref, in_peer_ref, rd_ref, ru_ref, ra_ref, rb_ref, sums_ref,
    w_ref, wo_ref, up_ref, down_ref, bias_2, qkv_ref, p_ref, ctx_ref, xhat_ref, rstd_ref, low_ref, act_ref, slope_ref,
    acc_ref, dffn_ref, t_low_ref, t_grad_ref, small_ref, *rest_refs,
):
    half, mid, owned, shard = rest_refs[0:4], rest_refs[4:8], rest_refs[8:12], rest_refs[12:16]
    tiny, tiny_1, tiny_2, tiny_x, tiny_z, last = rest_refs[16:22]
    send, recv, send_z, recv_z, send_in, recv_in, g_send, g_recv, g_local = rest_refs[22:]
    seqs, length = seg_c_ref.shape[0], seg_c_ref.shape[1]
    groups, width, model = wo_ref.shape
    hidden = up_ref.shape[2]
    pairs = width // PAIR
    tokens = seqs * length
    step = hidden // 3
    block = 256
    rows_own = model // n
    depth = n // 4
    index = lax.axis_index("dp")
    x_index = lax.axis_index("mp")
    core, line, rest = index % 2, index // 2 % 2, index // 4
    to_core = {"dp": index + 1 - 2 * core}
    to_line = {"dp": index + 2 - 4 * line}
    to_x = {"mp": 1 - x_index}

    def to_rest(k):
        return {"dp": (rest + k) % depth * 4 + index % 4}

    barrier = pltpu.get_barrier_semaphore()
    peers = [to_core, to_line, to_x] + [to_rest(k) for k in range(1, depth)]
    for peer in peers:
        pl.semaphore_signal(barrier, inc=1, device_id=peer, device_id_type=MESH)
    pl.semaphore_wait(barrier, len(peers))

    def remote(src, dst, s, r, device):
        return pltpu.make_async_remote_copy(
            src_ref=src, dst_ref=dst, send_sem=s, recv_sem=r, device_id=device, device_id_type=MESH
        )

    def columns(c):
        return pl.ds(pl.multiple_of(c * step, step), step)

    def ends_of(kind, c, piece):
        if kind < 3:
            size = model // 4
            rows = pl.ds(pl.multiple_of(piece * size, size), size)
            return (wq_hbm, wk_hbm, wv_hbm)[kind].at[rows, :], w_ref.at[1, rows, kind * width : (kind + 1) * width]
        if kind == 3:
            size = width // 4
            rows = pl.ds(pl.multiple_of(piece * size, size), size)
            return wo_hbm.at[rows, :], wo_ref.at[1, rows, :]
        if kind == 4:
            size = model // 4
            rows = pl.ds(pl.multiple_of(piece * size, size), size)
            return up_hbm.at[rows, columns(c)], up_ref.at[1, rows, columns(c)]
        size = step // 4
        rows = pl.ds(pl.multiple_of(c * step + piece * size, size), size)
        return down_hbm.at[rows, :], down_ref.at[1, rows, :]

    def slot(kind, c):
        return kind if kind < 4 else (4 + c if kind == 4 else 7 + c)

    def over_x(kind, c=0):
        src, dst = ends_of(kind, c, 2 * line + core)
        i = slot(kind, c)
        return remote(src, dst, g_send.at[0, i], g_recv.at[0, i], to_x)

    def pass_on(kind, c, hop):
        at = ends_of(kind, c, 2 * (1 - line) + core if hop == 3 else 2 * line + core)[1]
        i = slot(kind, c)
        return remote(at, at, g_send.at[hop, i], g_recv.at[hop, i], to_line if hop == 2 else to_core)

    def first_hop(kind, c=0):
        over_x(kind, c).wait_recv()
        pass_on(kind, c, 2).start()
        pass_on(kind, c, 1).start()

    def second_hop(kind, c=0):
        pass_on(kind, c, 2).wait_recv()
        pass_on(kind, c, 3).start()

    def complete(kind, c=0):
        pass_on(kind, c, 1).wait_recv()
        pass_on(kind, c, 3).wait_recv()

    def sent(kind, c=0):
        over_x(kind, c).wait_send()
        for hop in (1, 2, 3):
            pass_on(kind, c, hop).wait_send()

    bias_over = remote(bias_ref, bias_2, send.at[4, 0], recv.at[4, 0], to_x)
    bias_over.start()
    for kind in range(4):
        over_x(kind).start()
    for c in range(3):
        over_x(4, c).start()
        over_x(5, c).start()
    own_copies = [
        pltpu.make_async_copy(src, dst, g_local.at[i])
        for i, (src, dst) in enumerate(
            [(w, w_ref.at[0, :, o * width : (o + 1) * width]) for o, w in enumerate((wq_hbm, wk_hbm, wv_hbm))]
            + [(wo_hbm, wo_ref.at[0]), (up_hbm, up_ref.at[0]), (down_hbm, down_ref.at[0])]
        )
    ]
    for copy in own_copies:
        copy.start()

    n_half, n_quarter = model // 2, model // 4
    cut = hidden // 2
    sources = (act_ref, slope_ref, up_ref.at[:, :, :cut], up_ref.at[:, :, cut:])

    def by_core(t):
        there = pl.ds(pl.multiple_of((1 - core) * n_half, n_half), n_half)
        return remote(sources[t].at[:, there, :], half[t], send.at[0, t], recv.at[0, t], to_core)

    def quarter_of(place):
        return pl.ds(pl.multiple_of(place * n_quarter, n_quarter), n_quarter)

    def own_rows(place):
        return pl.ds(pl.multiple_of(place * rows_own, rows_own), rows_own)

    def by_first(t):
        if WAYS[t] == "xyz":
            return remote(half[t].at[1], mid[t], send.at[1, t], recv.at[1, t], to_x)
        return remote(half[t].at[:, quarter_of(1 - line), :], mid[t], send.at[1, t], recv.at[1, t], to_line)

    def by_second(t):
        if WAYS[t] == "xyz":
            return remote(mid[t].at[quarter_of(1 - line), :], owned[t], send.at[2, t], recv.at[2, t], to_line)
        if WAYS[t] == "yzx":
            return remote(owned[t].at[1], last, send.at[2, t], recv.at[2, t], to_x)
        return remote(mid[t].at[1], owned[t], send.at[2, t], recv.at[2, t], to_x)

    def by_rest(t, k):
        there = own_rows((rest + k) % depth)
        source = mid[t].at[:, there, :] if WAYS[t] == "yzx" else owned[t].at[there, :]
        return remote(source, shard[t].at[k - 1], send_z.at[t, k - 1], recv_z.at[t, k - 1], to_rest(k))

    def start_rest(t):
        for k in range(1, depth):
            by_rest(t, k).start()

    def rest_sum(t):
        if WAYS[t] == "yzx":
            total = mid[t][:, own_rows(rest), :].astype(F32)
        else:
            total = owned[t][own_rows(rest), :].astype(F32)
        for k in range(1, depth):
            by_rest(t, k).wait_recv()
            total = total + shard[t][k - 1].astype(F32)
        return total

    def after_core(t):
        by_core(t).wait_recv()
        for g in range(groups):
            add_rows(half[t].at[g], sources[t].at[g], core * n_half, 96)
        by_first(t).start()

    def after_first(t):
        by_first(t).wait_recv()
        if WAYS[t] == "xyz":
            add_rows(mid[t], half[t].at[0], 0, 96)
        else:
            for g in range(groups):
                add_rows(mid[t].at[g], half[t].at[g], line * n_quarter, 96)
        if WAYS[t] == "yzx":
            start_rest(t)
        else:
            by_second(t).start()

    def after_second(t, out):
        if WAYS[t] == "yzx":
            total = rest_sum(t)
            out[...] = total[0]
            owned[t][...] = total.astype(BF16)
            by_second(t).start()
            return
        by_second(t).wait_recv()
        if WAYS[t] == "xyz":
            add_rows(owned[t], mid[t], line * n_quarter, 96)
        else:
            add_rows(owned[t], mid[t].at[0], 0, 96)
        start_rest(t)

    def finish(t, out):
        if WAYS[t] == "yzx":
            by_second(t).wait_recv()
            out[...] += last[...].astype(F32)
        else:
            out[...] = rest_sum(t)

    def send_output(b):
        rows = pl.ds(pl.multiple_of(b * length, length), length)
        return remote(out_ref.at[rows, :], out_peer_ref.at[rows, :], send_in.at[1, b], recv_in.at[1, b], to_x)

    def send_input(s):
        rows = pl.ds(pl.multiple_of(s * length, length), length)
        return remote(in_ref.at[rows, :], in_peer_ref.at[rows, :], send_in.at[0, s], recv_in.at[0, s], to_x)

    attn_gain, attn_shift, down_bias = vec_ref[0:1, :], vec_ref[1:2, :], vec_ref[2:3, :]
    ffn_gain, ffn_shift, out_bias = vec_ref[3:4, :], vec_ref[4:5, :], vec_ref[5:6, :]

    def attend(s, g, biases):
        rows = pl.ds(pl.multiple_of(s * length, length), length)
        x = x_ref[rows, :]
        mask = seg_c_ref[s] == seg_r_ref[s]
        y = mm(x, w_ref[g])
        query = (0.125 * (y[:, :width] + biases[0:1, :width])).astype(BF16)
        key = y[:, width : 2 * width].astype(BF16)
        value = (y[:, 2 * width :] + biases[0:1, width : 2 * width]).astype(BF16)
        qkv_ref[g, rows, :width] = query
        qkv_ref[g, rows, width : 2 * width] = key
        qkv_ref[g, rows, 2 * width :] = value
        parts = []
        for p in range(pairs):
            at = slice(p * PAIR, (p + 1) * PAIR)
            k = key[:, at]
            both = None
            for h, (q, v) in enumerate(zip(halves(query[:, at]), halves(value[:, at]))):
                scores = jnp.where(mask, mm_t(q, k), -1000000000.0)
                expo = jnp.exp(scores - jnp.max(scores, -1, keepdims=True))
                probs = (expo * (1.0 / jnp.sum(expo, -1, keepdims=True))).astype(BF16)
                p_ref[s, (g * pairs + p) * 2 + h] = probs
                part = mm(probs, v)
                both = part if both is None else both + part
            parts.append(both.astype(BF16))
        ctx = jnp.concatenate(parts, 1)
        ctx_ref[g, rows, :] = ctx
        return mm(ctx, wo_ref[g])

    for copy in own_copies[:4]:
        copy.wait()

    @pl.loop(0, seqs)
    def _(s):
        rows = pl.ds(pl.multiple_of(s * length, length), length)
        acc_ref[rows, :] = x_ref[rows, :].astype(F32) + out_bias + attend(s, 0, bias_ref)
        for kind in range(3):

            @pl.when(s == min(kind, seqs - 1))
            def _():
                first_hop(kind)

    first_hop(3)
    for kind in range(4):
        second_hop(kind)
    for kind in range(4):
        complete(kind)
    bias_over.wait()

    @pl.loop(0, seqs)
    def _(s):
        rows = pl.ds(pl.multiple_of(s * length, length), length)
        attn = acc_ref[rows, :] + attend(s, 1, bias_2)
        centred = attn - jnp.mean(attn, -1, keepdims=True)
        rstd = lax.rsqrt(jnp.mean(centred * centred, -1, keepdims=True) + EPS)
        xhat = centred * rstd
        xhat_ref[rows, :] = xhat
        rstd_ref[rows, :] = rstd
        low_ref[rows, :] = (xhat * attn_gain + attn_shift).astype(BF16)

        @pl.when(s == 0)
        def _():
            first_hop(4, 0)

        @pl.when(s == 1)
        def _():
            first_hop(5, 0)

        @pl.when(s == 2)
        def _():
            first_hop(4, 1)

    for copy in own_copies[4:]:
        copy.wait()
    store_by_owner(t_low_ref, low_ref[...].T, slice(None), n)

    def expand(c, g, biases):
        at = columns(c)
        bias_at = pl.ds(pl.multiple_of(2 * width + c * step, 128), step)

        @pl.loop(0, tokens // block)
        def _(b):
            rows = pl.ds(pl.multiple_of(b * block, block), block)
            u = mm(low_ref[rows, :], up_ref[g, :, at]) + biases[0:1, bias_at]
            square = u * u
            t = jnp.tanh(GELU_C * (u + 0.044715 * square * u))
            gate = 0.5 * (1.0 + t)
            act = (u * gate).astype(BF16)
            act_ref[g, rows, at] = act
            slope = gate + (0.5 * GELU_C) * u * (1.0 - t * t) * (1.0 + 0.134145 * square)
            slope_ref[g, rows, at] = slope.astype(BF16)
            acc_ref[rows, :] += mm(act, down_ref[g, at, :])

    acc_ref[...] = jnp.zeros_like(acc_ref)

    @pl.loop(0, 3)
    def _(c):
        expand(c, 0, bias_ref)

        @pl.when(c == 0)
        def _():
            second_hop(4, 0)

        @pl.when(c == 1)
        def _():
            second_hop(5, 0)
            first_hop(5, 1)

        @pl.when(c == 2)
        def _():
            second_hop(4, 1)
            first_hop(4, 2)

    @pl.loop(0, 3)
    def _(c):
        complete(4, c)
        complete(5, c)
        expand(c, 1, bias_2)

        @pl.when(c == 0)
        def _():
            first_hop(5, 2)
            second_hop(5, 1)

        @pl.when(c == 1)
        def _():
            second_hop(4, 2)
            second_hop(5, 2)

    small_ref[...] = jnp.zeros_like(small_ref)

    @pl.loop(0, seqs)
    def _(b):
        rows = pl.ds(pl.multiple_of(b * length, length), length)
        resid = xhat_ref[rows, :] * attn_gain + attn_shift + acc_ref[rows, :] + down_bias
        centred = resid - jnp.mean(resid, -1, keepdims=True)
        rstd = lax.rsqrt(jnp.mean(centred * centred, -1, keepdims=True) + EPS)
        xhat = centred * rstd
        out_ref[rows, :] = (xhat * ffn_gain + ffn_shift).astype(BF16)
        cot = cot_ref[rows, :].astype(F32)
        grad = norm_backward(xhat, rstd, ffn_gain, cot)
        acc_ref[rows, :] = grad
        dffn_ref[rows, :] = grad.astype(BF16)
        small_ref[3:4, :] += jnp.sum(grad, 0, keepdims=True)
        small_ref[4:5, :] += jnp.sum(cot * xhat, 0, keepdims=True)
        small_ref[5:6, :] += jnp.sum(cot, 0, keepdims=True)
        send_output(b).start()

    store_by_owner(t_grad_ref, dffn_ref[...].T, slice(None), n)

    def product(left, place, g, at):
        made = [
            mm(left[b * block : (b + 1) * block, :], place[g, :, at]).astype(BF16) for b in range(model // block)
        ]
        for b, value in enumerate(made):
            place[g, b * block : (b + 1) * block, at] = value

    tiny[...] = jnp.zeros_like(tiny)
    for g in range(groups):

        @pl.loop(0, 3)
        def _(c):
            product(t_grad_ref, act_ref, g, columns(c))

    by_core(0).start()
    for g in range(groups):

        @pl.loop(0, 3)
        def _(c):
            at = columns(c)
            total = jnp.zeros((1, step), F32)
            for b in range(tokens // block):
                rows = slice(b * block, (b + 1) * block)
                d_upper = mm_t(dffn_ref[rows, :], down_ref[g, at, :]) * slope_ref[g, rows, at].astype(F32)
                total = total + jnp.sum(d_upper, 0, keepdims=True)
                d_low = d_upper.astype(BF16)
                slope_ref[g, rows, at] = d_low
                acc_ref[rows, :] += mm_t(d_low, up_ref[g, :, at])
            tiny[3 + g, 0:1, at] = total
            product(t_low_ref, slope_ref, g, at)
            if g == 0:

                @pl.when(c == 1)
                def _():
                    after_core(0)

    by_core(1).start()

    @pl.loop(0, seqs)
    def _(b):
        rows = pl.ds(pl.multiple_of(b * length, length), length)
        d_normed = acc_ref[rows, :]
        xhat = xhat_ref[rows, :]
        grad = norm_backward(xhat, rstd_ref[rows, :], attn_gain, d_normed)
        acc_ref[rows, :] = grad
        small_ref[0:1, :] += jnp.sum(grad, 0, keepdims=True)
        small_ref[1:2, :] += jnp.sum(d_normed * xhat, 0, keepdims=True)
        small_ref[2:3, :] += jnp.sum(d_normed, 0, keepdims=True)

    store_by_owner(t_low_ref, x_ref[...].T, slice(None), n)

    @pl.loop(0, seqs)
    def _(s):
        backward_sequence(
            s, lambda v, at: store_by_owner(t_grad_ref, v, at, n),
            acc_ref, w_ref, wo_ref, qkv_ref, p_ref, in_ref, qkv_ref,
        )
        send_input(s).start()

        @pl.when(s == 0)
        def _():
            after_core(1)

        @pl.when(s == min(1, seqs - 1))
        def _():
            after_first(0)

    tiny_core = remote(tiny.at[0:3], tiny_1, send.at[3, 1], recv.at[3, 1], to_core)
    tiny_line = remote(tiny_1, tiny_2, send.at[3, 2], recv.at[3, 2], to_line)
    tiny_over = remote(tiny_2.at[1:3], tiny_x, send.at[3, 3], recv.at[3, 3], to_x)

    def tiny_rest(k):
        return remote(tiny_x, tiny_z.at[k - 1], send_z.at[4, k - 1], recv_z.at[4, k - 1], to_rest(k))

    for g in range(groups):
        column = jnp.sum(qkv_ref[g].astype(F32), 0, keepdims=True)
        tiny[g, 0:1, :width] = column[:, :width]
        tiny[g, 0:1, width : 2 * width] = column[:, 2 * width :]
        tiny[g, 1:2, :] = tiny[3 + g, 0:1, :]
    tiny[2, :, :model] = small_ref[...]
    for kind in range(4):
        sent(kind)
    for c in range(3):
        sent(4, c)
        sent(5, c)
    tiny_core.start()
    for g in range(groups):
        weight_products(g, t_low_ref, t_grad_ref, qkv_ref, ctx_ref, up_ref)
    by_core(2).start()
    by_core(3).start()
    tiny_core.wait_recv()
    tiny_1[...] += tiny[0:3]
    tiny_line.start()
    after_core(2)
    after_core(3)
    tiny_line.wait_recv()
    tiny_2[...] += tiny_1[...]
    tiny_over.start()
    after_first(1)
    after_second(0, rd_ref)
    after_first(3)
    tiny_over.wait_recv()
    tiny_x[0] += tiny_2[0]
    tiny_x[1] += tiny_2[2]
    for k in range(1, depth):
        tiny_rest(k).start()
    after_first(2)
    after_second(1, ru_ref)
    after_second(3, rb_ref)
    finish(0, rd_ref)
    after_second(2, ra_ref)
    total = tiny_x[...]
    for k in range(1, depth):
        tiny_rest(k).wait_recv()
        total = total + tiny_z[k - 1]
    sums_ref[...] = total
    finish(1, ru_ref)
    finish(3, rb_ref)
    finish(2, ra_ref)
    for s in range(seqs):
        send_output(s).wait()
        send_input(s).wait()
    for t in range(4):
        by_core(t).wait_send()
        by_first(t).wait_send()
        by_second(t).wait_send()
        for k in range(1, depth):
            by_rest(t, k).wait_send()
    tiny_core.wait_send()
    tiny_line.wait_send()
    tiny_over.wait_send()
    for k in range(1, depth):
        tiny_rest(k).wait_send()


def call(kernel, outs, scratch, flops, *args, far=(), far_out=(), collective=None):
    shapes = [jax.ShapeDtypeStruct(s, d) for s, d in outs]
    moved = sum(a.size * a.dtype.itemsize for a in args) + sum(s.size * s.dtype.itemsize for s in shapes)
    vmem = pl.BlockSpec(memory_space=pltpu.VMEM)
    return pl.pallas_call(
        kernel,
        out_shape=shapes,
        in_specs=[pl.BlockSpec(memory_space=pl.ANY) if i in far else vmem for i in range(len(args))],
        out_specs=[pl.BlockSpec(memory_space=pl.ANY) if i in far_out else vmem for i in range(len(shapes))],
        scratch_shapes=[pltpu.VMEM(*s) if isinstance(s, tuple) else s for s in scratch],
        compiler_params=pltpu.CompilerParams(
            vmem_limit_bytes=VMEM_LIMIT, collective_id=collective, has_side_effects=collective is not None
        ),
        cost_estimate=pl.CostEstimate(flops=flops, bytes_accessed=moved, transcendentals=0),
    )(*args)


def factors_of(n):
    found = []
    while n > 4 or (n > 1 and len(found) < 2):
        found.append(2)
        n //= 2
    return found + ([n] if n > 1 else [])


def swap(v):
    return lax.ppermute(v, "mp", [(0, 1), (1, 0)])


def shift_dp(v, n, stride, factor, k):
    def target(d):
        i = (d // stride) % factor
        return d + ((i + k) % factor - i) * stride

    return lax.ppermute(v, "dp", [(d, target(d)) for d in range(n)])


def with_peer(own, n):
    core = lax.axis_index("dp") % 2
    half = own.shape[0] // 2
    mine = swap(lax.dynamic_slice_in_dim(own, core * half, half, 0))
    other = shift_dp(mine, n, 1, 2, 1)
    first = core == 0
    peer = jnp.concatenate([jnp.where(first, mine, other), jnp.where(first, other, mine)], 0)
    return jnp.stack([own, peer])


def reduce_to_owner(grad, n):
    index = lax.axis_index("dp")
    rows = grad.shape[1] // n
    left = grad.reshape(2, n, rows, grad.shape[2])
    stride = 1
    for factor in factors_of(n):
        parts = left.reshape(2, left.shape[1] // factor, factor, rows, left.shape[3])
        i = (index // stride) % factor

        def pick(at):
            return lax.dynamic_index_in_dim(parts, at, 2, keepdims=False)

        total = pick(i).astype(F32)
        for k in range(1, factor):
            total = total + shift_dp(pick((i + k) % factor), n, stride, factor, k).astype(F32)
        left = total.astype(BF16)
        stride *= factor
    left = left.reshape(2, rows, left.shape[3])
    return left[0].astype(F32) + swap(left[1]).astype(F32)


def per_device(
    n, layer_input, doc_lengths, q_weight, q_bias, k_weight, v_weight, v_bias, out_weight, out_bias,
    attn_gain, attn_shift, up_weight, up_bias, down_weight, down_bias, ffn_gain, ffn_shift, cotangent,
):
    rows = doc_lengths.shape[0]
    tokens, model = layer_input.shape
    length = tokens // rows
    part = length // 2
    mine = rows * part
    width = q_weight.shape[1]
    hidden = up_weight.shape[1]
    heads = width // HD
    x_index = lax.axis_index("mp")

    ends = jnp.cumsum(doc_lengths, axis=-1, dtype=jnp.int32)
    start = jnp.sum(jnp.where(doc_lengths == part, ends - part, 0), -1)
    place = jnp.arange(length, dtype=jnp.int32)
    segment = jnp.sum((place[None, :, None] >= ends[:, None, :]).astype(jnp.int32), -1, dtype=jnp.int32)
    before = place[None, :part] < start[:, None]
    from_high = before != (x_index == 1)

    def take(v):
        v = v.reshape(rows, 2, part, model)
        return jnp.where(from_high[:, :, None], v[:, 1], v[:, 0]).reshape(mine, model)

    def give(own, other):
        own, other = own.reshape(rows, part, model), other.reshape(rows, part, model)
        low = jnp.where(from_high[:, :, None], other, own)
        high = jnp.where(from_high[:, :, None], own, other)
        return jnp.stack([low, high], 1).reshape(tokens, model)

    seg = jnp.where(from_high, segment[:, part:], segment[:, :part])

    x = take(layer_input)
    cot = take(cotangent)
    own_bias = jnp.concatenate([q_bias, v_bias, up_bias])
    remote = (
        (model // n) % 16 == 0 and n % 4 == 0 and n > 4
        and hidden == 2 * model and 4 * width == hidden and hidden % 384 == 0 and rows >= 3
    )
    if remote:
        depth = n // 4
        dma = pltpu.SemaphoreType.DMA
        wide = (hidden, hidden, model, model)
        quarter = model // 4
        vectors = jnp.stack([attn_gain, attn_shift, down_bias, ffn_gain, ffn_shift, out_bias]).astype(F32)
        output, output_peer, grad_in, grad_in_peer, g_down, g_up, g_first, g_last, sums = call(
            functools.partial(whole_layer, n),
            [((mine, model), BF16)] * 4
            + [((model // n, c), F32) for c in wide]
            + [((2, 8, hidden), F32)],
            [
                ((2, model, 3 * width), BF16),
                ((2, width, model), BF16),
                ((2, model, hidden), BF16),
                ((2, hidden, model), BF16),
                ((1, 2 * width + hidden), F32),
                ((2, mine, 3 * width), BF16),
                ((rows, 2 * heads, part, part), BF16),
                ((2, mine, width), BF16),
                ((mine, model), F32),
                ((mine, 1), F32),
                ((mine, model), BF16),
                ((2, model, hidden), BF16),
                ((2, model, hidden), BF16),
                ((mine, model), F32),
                ((mine, model), BF16),
                ((model, mine), BF16),
                ((model, mine), BF16),
                ((8, model), F32),
            ]
            + [((2, model // 2, c), BF16) for c in wide]
            + [((2 * quarter, c) if w == "xyz" else (2, quarter, c), BF16) for w, c in zip(WAYS, wide)]
            + [((2, model // n, c) if w == "yzx" else (quarter, c), BF16) for w, c in zip(WAYS, wide)]
            + [((depth - 1,) + (2,) * (w == "yzx") + (model // n, c), BF16) for w, c in zip(WAYS, wide)]
            + [
                ((5, 8, hidden), F32),
                ((3, 8, hidden), F32),
                ((3, 8, hidden), F32),
                ((2, 8, hidden), F32),
                ((depth - 1, 2, 8, hidden), F32),
                ((model // n, hidden), BF16),
                dma((5, 4)), dma((5, 4)), dma((5, depth - 1)), dma((5, depth - 1)), dma((2, rows)), dma((2, rows)),
                dma((4, 10)), dma((4, 10)), dma((6,)),
            ],
            2 * mine * model * (24 * width + 12 * hidden),
            x, cot, seg[:, :, None], seg[:, None, :], own_bias.astype(F32)[None], vectors,
            q_weight, k_weight, v_weight, out_weight, up_weight, down_weight,
            far=(6, 7, 8, 9, 10, 11), far_out=(1, 3), collective=0,
        )
        g_attn = jnp.concatenate([g_first, g_last], -1)
        small = sums[1, :, :model]
        sums = jnp.concatenate([sums[0, 0, : 2 * width], sums[0, 1]])
    else:
        w_qkv = with_peer(jnp.concatenate([q_weight, k_weight, v_weight], 1), n)
        w_out = with_peer(out_weight, n)
        w_up = with_peer(up_weight, n)
        w_down = with_peer(down_weight, n)
        bias = jnp.stack([own_bias, swap(own_bias)]).astype(F32)[:, None, :]
        b_qkv = jnp.concatenate([bias[..., :width], jnp.zeros_like(bias[..., :width]), bias[..., width : 2 * width]], -1)
        b_up = bias[..., 2 * width :]
        vectors = jnp.stack([attn_gain, attn_shift, down_bias, ffn_gain, ffn_shift]).astype(F32)

        qkv, probs, ctx, xhat, rstd, low = call(
            attention_forward,
            [
                ((2, mine, 3 * width), BF16),
                ((rows, 2 * heads, part, part), BF16),
                ((2, mine, width), BF16),
                ((mine, model), F32),
                ((mine, 1), F32),
                ((mine, model), BF16),
            ],
            [],
            2 * mine * model * 8 * width,
            x, w_qkv, b_qkv, w_out, seg[:, :, None], seg[:, None, :],
            out_bias.astype(F32)[None], vectors[0:1], vectors[1:2],
        )
        output, g_down, g_up, d_resid, small, up_bias_grad = call(
            feed_forward,
            [
                ((mine, model), BF16),
                ((2, model, hidden), BF16),
                ((2, model, hidden), BF16),
                ((mine, model), F32),
                ((8, model), F32),
                ((2, 1, hidden), F32),
            ],
            [
                ((2, mine, hidden), BF16),
                ((2, mine, hidden), BF16),
                ((mine, model), F32),
                ((mine, model), BF16),
                ((model, mine), BF16),
                ((model, mine), BF16),
            ],
            2 * mine * model * 2 * hidden * 6,
            low, xhat, rstd, w_up, b_up, w_down, vectors, cot,
        )
        scratch = [((2, mine, 3 * width), BF16), ((model, mine), BF16), ((model, mine), BF16)]
        flops = 2 * mine * model * 16 * width
        output_peer = swap(output)
        grad_in, g_attn, bias_grad = call(
            attention_backward_plain,
            [((mine, model), BF16), ((2, model, 4 * width), BF16), ((2, 1, 3 * width), F32)],
            scratch, flops, x, d_resid, w_qkv, w_out, qkv, probs, ctx,
        )
        grad_in_peer = swap(grad_in)
        g_down, g_up, g_attn = (reduce_to_owner(v, n) for v in (g_down, g_up, g_attn))
        sums = jnp.concatenate([bias_grad[:, 0, :width], bias_grad[:, 0, 2 * width :], up_bias_grad[:, 0]], -1)
        sums = jnp.where(x_index == 0, sums, sums[::-1])
        sums, small = lax.psum((sums, small), ("dp", "mp"))
        sums = lax.dynamic_index_in_dim(sums, x_index, 0, keepdims=False)
    layer_output = give(output, output_peer)
    input_grad = give(grad_in, grad_in_peer)
    down_weight_grad = g_down.T
    up_weight_grad = g_up
    return (
        layer_output,
        input_grad,
        g_attn[:, :width],
        sums[:width],
        g_attn[:, width : 2 * width],
        g_attn[:, 2 * width : 3 * width],
        sums[width : 2 * width],
        g_attn[:, 3 * width :].T,
        small[0],
        small[1],
        small[2],
        up_weight_grad,
        sums[2 * width :],
        down_weight_grad,
        small[3],
        small[4],
        small[5],
    )


def solution(mesh):
    in_specs = (
        P("dp", None), P("dp", None), P(None, "mp"), P("mp"), P(None, "mp"), P(None, "mp"), P("mp"),
        P("mp", None), P(), P(), P(), P(None, "mp"), P("mp"), P("mp", None), P(), P(), P(), P("dp", None),
    )
    out_specs = (
        P("dp", None), P("dp", None), P("dp", "mp"), P("mp"), P("dp", "mp"), P("dp", "mp"), P("mp"),
        P("mp", "dp"), P(), P(), P(), P("dp", "mp"), P("mp"), P("mp", "dp"), P(), P(), P(),
    )
    return jax.shard_map(
        functools.partial(per_device, mesh.shape["dp"]),
        mesh=mesh, in_specs=in_specs, out_specs=out_specs, check_vma=False,
    )
```

```python
import functools

import jax
import jax.numpy as jnp
from jax import lax
from jax.experimental import pallas as pl
from jax.experimental.pallas import tpu as pltpu
from jax.sharding import PartitionSpec as P

HD = 64
PAIR = 2 * HD
EPS = 1e-12
GELU_C = 0.7978845608028654
F32 = jnp.float32
BF16 = jnp.bfloat16
CHUNK = 512
VMEM_LIMIT = 67043328
MESH = pl.DeviceIdType.MESH


def mm(a, b):
    return jnp.dot(a, b, preferred_element_type=F32)


def mm_t(a, b):
    return lax.dot_general(a, b, (((1,), (1,)), ((), ())), preferred_element_type=F32)


def t_mm(a, b):
    return lax.dot_general(a, b, (((0,), (0,)), ((), ())), preferred_element_type=F32)


def halves(v):
    lane = lax.broadcasted_iota(jnp.int32, v.shape, 1)
    zero = jnp.zeros_like(v)
    return jnp.where(lane < HD, v, zero), jnp.where(lane < HD, zero, v)


def attention_forward(
    x_ref, w_ref, b_ref, wo_ref, seg_c_ref, seg_r_ref, bo_ref, gain_ref, shift_ref,
    qkv_ref, p_ref, ctx_ref, xhat_ref, rstd_ref, low_ref,
):
    seqs, length = seg_c_ref.shape[0], seg_c_ref.shape[1]
    groups, width = wo_ref.shape[0], wo_ref.shape[1]
    pairs = width // PAIR

    @pl.loop(0, seqs)
    def _(s):
        rows = pl.ds(pl.multiple_of(s * length, length), length)
        x = x_ref[rows, :]
        mask = seg_c_ref[s] == seg_r_ref[s]
        attn = x.astype(F32) + bo_ref[...]
        for g in range(groups):
            y = mm(x, w_ref[g]) + b_ref[g]
            query = (0.125 * y[:, :width]).astype(BF16)
            key = y[:, width : 2 * width].astype(BF16)
            value = y[:, 2 * width :].astype(BF16)
            qkv_ref[g, rows, :width] = query
            qkv_ref[g, rows, width : 2 * width] = key
            qkv_ref[g, rows, 2 * width :] = value
            parts = []
            for p in range(pairs):
                at = slice(p * PAIR, (p + 1) * PAIR)
                k = key[:, at]
                both = None
                for h, (q, v) in enumerate(zip(halves(query[:, at]), halves(value[:, at]))):
                    scores = jnp.where(mask, mm_t(q, k), -1000000000.0)
                    expo = jnp.exp(scores - jnp.max(scores, -1, keepdims=True))
                    probs = (expo * (1.0 / jnp.sum(expo, -1, keepdims=True))).astype(BF16)
                    p_ref[s, (g * pairs + p) * 2 + h] = probs
                    part = mm(probs, v)
                    both = part if both is None else both + part
                parts.append(both.astype(BF16))
            ctx = jnp.concatenate(parts, 1)
            ctx_ref[g, rows, :] = ctx
            attn = attn + mm(ctx, wo_ref[g])
        mean = jnp.mean(attn, -1, keepdims=True)
        centred = attn - mean
        rstd = lax.rsqrt(jnp.mean(centred * centred, -1, keepdims=True) + EPS)
        xhat = centred * rstd
        xhat_ref[rows, :] = xhat
        rstd_ref[rows, :] = rstd
        low_ref[rows, :] = (xhat * gain_ref[...] + shift_ref[...]).astype(BF16)


def norm_backward(xhat, rstd, gain, grad):
    scaled = grad * gain
    return rstd * (
        scaled
        - jnp.mean(scaled, -1, keepdims=True)
        - xhat * jnp.mean(scaled * xhat, -1, keepdims=True)
    )


def add_rows(dst, src, offset, step):
    step = min(step, dst.shape[0])

    @pl.loop(0, dst.shape[0] // step)
    def _(i):
        here = pl.ds(pl.multiple_of(i * step, step), step)
        there = pl.ds(pl.multiple_of(offset + i * step, step), step)
        dst[here, :] = (dst[here, :].astype(F32) + src[there, :].astype(F32)).astype(dst.dtype)


def store_by_owner(dst, value, at, n):
    rows = value.shape[0] // n
    for d in range(n):
        place = (d % 2) * (n // 2) + (d // 2 % 2) * (n // 4) + d // 4
        dst[place * rows : (place + 1) * rows, at] = value[d * rows : (d + 1) * rows, :]


def feed_forward(
    low_ref, xhat_ref, rstd_ref, up_ref, ub_ref, down_ref, vec_ref, cot_ref,
    out_ref, gd_ref, gu_ref, d_resid_ref, small_ref, ubg_ref,
    act_ref, slope_ref, acc_ref, dffn_ref, dffn_t_ref, low_t_ref,
):
    tokens, width = low_ref.shape
    groups, hidden = up_ref.shape[0], up_ref.shape[2]
    step = min(CHUNK, hidden)
    per = hidden // step
    block = 256
    low_t_ref[...] = low_ref[...].T
    acc_ref[...] = jnp.zeros_like(acc_ref)

    @pl.loop(0, groups * per)
    def _(i):
        g = i // per
        at = pl.ds(pl.multiple_of((i % per) * step, step), step)

        @pl.loop(0, tokens // block)
        def _(b):
            rows = pl.ds(pl.multiple_of(b * block, block), block)
            u = mm(low_ref[rows, :], up_ref[g, :, at]) + ub_ref[g, :, at]
            square = u * u
            t = jnp.tanh(GELU_C * (u + 0.044715 * square * u))
            half = 0.5 * (1.0 + t)
            act = (u * half).astype(BF16)
            act_ref[g, rows, at] = act
            slope = half + (0.5 * GELU_C) * u * (1.0 - t * t) * (1.0 + 0.134145 * square)
            slope_ref[g, rows, at] = slope.astype(BF16)
            acc_ref[rows, :] += mm(act, down_ref[g, at, :])

    small_ref[...] = jnp.zeros_like(small_ref)
    attn_gain, attn_shift = vec_ref[0:1, :], vec_ref[1:2, :]
    down_bias = vec_ref[2:3, :]
    ffn_gain, ffn_shift = vec_ref[3:4, :], vec_ref[4:5, :]

    @pl.loop(0, tokens // block)
    def _(b):
        rows = pl.ds(pl.multiple_of(b * block, block), block)
        resid = xhat_ref[rows, :] * attn_gain + attn_shift + acc_ref[rows, :] + down_bias
        centred = resid - jnp.mean(resid, -1, keepdims=True)
        rstd = lax.rsqrt(jnp.mean(centred * centred, -1, keepdims=True) + EPS)
        xhat = centred * rstd
        out_ref[rows, :] = (xhat * ffn_gain + ffn_shift).astype(BF16)
        cot = cot_ref[rows, :].astype(F32)
        grad = norm_backward(xhat, rstd, ffn_gain, cot)
        acc_ref[rows, :] = grad
        dffn_ref[rows, :] = grad.astype(BF16)
        small_ref[3:4, :] += jnp.sum(grad, 0, keepdims=True)
        small_ref[4:5, :] += jnp.sum(cot * xhat, 0, keepdims=True)
        small_ref[5:6, :] += jnp.sum(cot, 0, keepdims=True)

    dffn_t_ref[...] = dffn_ref[...].T

    @pl.loop(0, groups * per)
    def _(i):
        g = i // per
        at = pl.ds(pl.multiple_of((i % per) * step, step), step)
        total = jnp.zeros((1, step), F32)
        for b in range(tokens // block):
            rows = slice(b * block, (b + 1) * block)
            d_upper = mm_t(dffn_ref[rows, :], down_ref[g, at, :]) * slope_ref[g, rows, at].astype(F32)
            total = total + jnp.sum(d_upper, 0, keepdims=True)
            d_low = d_upper.astype(BF16)
            slope_ref[g, rows, at] = d_low
            acc_ref[rows, :] += mm_t(d_low, up_ref[g, :, at])
        ubg_ref[g, :, at] = total
        for b in range(width // block):
            rows = slice(b * block, (b + 1) * block)
            gd_ref[g, rows, at] = mm(dffn_t_ref[rows, :], act_ref[g, :, at]).astype(BF16)
            gu_ref[g, rows, at] = mm(low_t_ref[rows, :], slope_ref[g, :, at]).astype(BF16)

    @pl.loop(0, tokens // block)
    def _(b):
        rows = pl.ds(pl.multiple_of(b * block, block), block)
        d_normed = acc_ref[rows, :]
        xhat = xhat_ref[rows, :]
        grad = norm_backward(xhat, rstd_ref[rows, :], attn_gain, d_normed)
        d_resid_ref[rows, :] = grad
        small_ref[0:1, :] += jnp.sum(grad, 0, keepdims=True)
        small_ref[1:2, :] += jnp.sum(d_normed * xhat, 0, keepdims=True)
        small_ref[2:3, :] += jnp.sum(d_normed, 0, keepdims=True)


def backward_sequence(s, put, d_resid_ref, w_ref, wo_ref, qkv_ref, p_ref, in_ref, dq_ref):
    length, groups, width = p_ref.shape[2], wo_ref.shape[0], wo_ref.shape[1]
    pairs = width // PAIR
    rows = pl.ds(pl.multiple_of(s * length, length), length)
    d_resid = d_resid_ref[rows, :]
    d_attn = d_resid.astype(BF16)
    put(d_attn.T, rows)
    total = d_resid
    for g in range(groups):
        d_ctx = mm_t(d_attn, wo_ref[g]).astype(BF16)
        for p in range(pairs):
            at = slice(p * PAIR, (p + 1) * PAIR)
            q_at, k_at, v_at = (slice(o * width + p * PAIR, o * width + (p + 1) * PAIR) for o in range(3))
            value = qkv_ref[g, rows, v_at]
            q_pair = halves(qkv_ref[g, rows, q_at])
            k_pair = halves(qkv_ref[g, rows, k_at])
            c_pair = halves(d_ctx[:, at])
            dq = dk = dv = None
            for h in range(2):
                low = p_ref[s, (g * pairs + p) * 2 + h]
                probs = low.astype(F32)
                d_probs = mm_t(c_pair[h], value)
                inner = jnp.sum(probs * d_probs, -1, keepdims=True)
                d_scores = (probs * (d_probs - inner)).astype(BF16)
                dv_h = t_mm(low, c_pair[h])
                dq_h = mm(d_scores, k_pair[h])
                dk_h = t_mm(d_scores, q_pair[h])
                dq = dq_h if dq is None else dq + dq_h
                dk = dk_h if dk is None else dk + dk_h
                dv = dv_h if dv is None else dv + dv_h
            dq_ref[g, rows, q_at] = (0.125 * dq).astype(BF16)
            dq_ref[g, rows, k_at] = dk.astype(BF16)
            dq_ref[g, rows, v_at] = dv.astype(BF16)
        total = total + mm_t(dq_ref[g, rows, :], w_ref[g])
    in_ref[rows, :] = total.astype(BF16)


def weight_products(g, x_t_ref, dattn_t_ref, dq_ref, ctx_ref, ga_ref):
    block, wide = 256, dq_ref.shape[2]

    @pl.loop(0, x_t_ref.shape[0] // block)
    def _(b):
        rows = pl.ds(pl.multiple_of(b * block, block), block)
        ga_ref[g, rows, :wide] = mm(x_t_ref[rows, :], dq_ref[g]).astype(BF16)
        ga_ref[g, rows, wide:] = mm(dattn_t_ref[rows, :], ctx_ref[g]).astype(BF16)


def attention_backward_plain(
    x_ref, d_resid_ref, w_ref, wo_ref, qkv_ref, p_ref, ctx_ref,
    in_ref, ga_ref, bg_ref,
    dq_ref, dattn_t_ref, x_t_ref,
):
    groups, width = wo_ref.shape[0], wo_ref.shape[1]
    x_t_ref[...] = x_ref[...].T

    def put(v, at):
        dattn_t_ref[:, at] = v

    @pl.loop(0, p_ref.shape[0])
    def _(s):
        backward_sequence(s, put, d_resid_ref, w_ref, wo_ref, qkv_ref, p_ref, in_ref, dq_ref)

    for g in range(groups):
        bg_ref[g] = jnp.sum(dq_ref[g].astype(F32), 0, keepdims=True)
        weight_products(g, x_t_ref, dattn_t_ref, dq_ref, ctx_ref, ga_ref)


WAYS = ("yzx", "yxz", "yxz", "xyz")


def whole_layer(
    n, doc_ref, x_hbm, cot_hbm, vec_ref, wq_hbm, wk_hbm, wv_hbm, wo_hbm, up_hbm, down_hbm,
    output_hbm, input_hbm, rd_ref, ru_ref, ra_ref, rb_ref, sums_ref,
    x_ref, cot_ref, seg_c_ref, seg_r_ref, out_ref, out_peer_ref, in_peer_ref,
    w_ref, wo_ref, up_ref, down_ref, bias_2, qkv_ref, p_ref, ctx_ref, xhat_ref, rstd_ref, low_ref, act_ref, slope_ref,
    acc_ref, t_low_ref, t_grad_ref, small_ref, *rest_refs,
):
    in_ref, dffn_ref = cot_ref, low_ref
    half, mid, owned, shard = rest_refs[0:4], rest_refs[4:8], rest_refs[8:12], rest_refs[12:16]
    tiny, tiny_1, tiny_2, tiny_x, tiny_z, last = rest_refs[16:22]
    send, recv, send_z, recv_z, send_in, recv_in, g_send, g_recv, g_local, raw, done = rest_refs[22:]
    seqs, length = seg_c_ref.shape[0], seg_c_ref.shape[1]
    groups, width, model = wo_ref.shape
    hidden = up_ref.shape[2]
    pairs = width // PAIR
    tokens = seqs * length
    step = hidden // 3
    block = 256
    rows_own = model // n
    depth = n // 4
    index = lax.axis_index("dp")
    x_index = lax.axis_index("mp")
    core, line, rest = index % 2, index // 2 % 2, index // 4
    to_core = {"dp": index + 1 - 2 * core}
    to_line = {"dp": index + 2 - 4 * line}
    to_x = {"mp": 1 - x_index}

    def to_rest(k):
        return {"dp": (rest + k) % depth * 4 + index % 4}

    barrier = pltpu.get_barrier_semaphore()
    peers = [to_core, to_line, to_x] + [to_rest(k) for k in range(1, depth)]
    for peer in peers:
        pl.semaphore_signal(barrier, inc=1, device_id=peer, device_id_type=MESH)
    pl.semaphore_wait(barrier, len(peers))

    def remote(src, dst, s, r, device):
        return pltpu.make_async_remote_copy(
            src_ref=src, dst_ref=dst, send_sem=s, recv_sem=r, device_id=device, device_id_type=MESH
        )

    def columns(c):
        return pl.ds(pl.multiple_of(c * step, step), step)

    def ends_of(kind, c, piece):
        if kind < 3:
            size = model // 4
            rows = pl.ds(pl.multiple_of(piece * size, size), size)
            return (wq_hbm, wk_hbm, wv_hbm)[kind].at[rows, :], w_ref.at[1, rows, kind * width : (kind + 1) * width]
        if kind == 3:
            size = width // 4
            rows = pl.ds(pl.multiple_of(piece * size, size), size)
            return wo_hbm.at[rows, :], wo_ref.at[1, rows, :]
        if kind == 4:
            size = model // 4
            rows = pl.ds(pl.multiple_of(piece * size, size), size)
            return up_hbm.at[rows, columns(c)], up_ref.at[1, rows, columns(c)]
        size = step // 4
        rows = pl.ds(pl.multiple_of(c * step + piece * size, size), size)
        return down_hbm.at[rows, :], down_ref.at[1, rows, :]

    def slot(kind, c):
        return kind if kind < 4 else (4 + c if kind == 4 else 7 + c)

    def over_x(kind, c=0):
        src, dst = ends_of(kind, c, 2 * line + core)
        i = slot(kind, c)
        return remote(src, dst, g_send.at[0, i], g_recv.at[0, i], to_x)

    def pass_on(kind, c, hop):
        at = ends_of(kind, c, 2 * (1 - line) + core if hop == 3 else 2 * line + core)[1]
        i = slot(kind, c)
        return remote(at, at, g_send.at[hop, i], g_recv.at[hop, i], to_line if hop == 2 else to_core)

    def first_hop(kind, c=0):
        over_x(kind, c).wait_recv()
        pass_on(kind, c, 2).start()
        pass_on(kind, c, 1).start()

    def second_hop(kind, c=0):
        pass_on(kind, c, 2).wait_recv()
        pass_on(kind, c, 3).start()

    def complete(kind, c=0):
        pass_on(kind, c, 1).wait_recv()
        pass_on(kind, c, 3).wait_recv()

    def sent(kind, c=0):
        over_x(kind, c).wait_send()
        for hop in (1, 2, 3):
            pass_on(kind, c, hop).wait_send()

    bias_ref = vec_ref.at[:, 6 * model :]
    bias_over = remote(bias_ref, bias_2, send.at[4, 0], recv.at[4, 0], to_x)
    bias_over.start()
    for kind in range(4):
        over_x(kind).start()
    for c in range(3):
        over_x(4, c).start()
        over_x(5, c).start()
    own_copies = [
        pltpu.make_async_copy(src, dst, g_local.at[i])
        for i, (src, dst) in enumerate(
            [(w, w_ref.at[0, :, o * width : (o + 1) * width]) for o, w in enumerate((wq_hbm, wk_hbm, wv_hbm))]
            + [(wo_hbm, wo_ref.at[0]), (up_hbm, up_ref.at[0]), (down_hbm, down_ref.at[0])]
        )
    ]
    raw_copies = [
        pltpu.make_async_copy(
            source.at[(2 * r + h) * length : (2 * r + h + 1) * length, :],
            act_ref.at[i, r * length : (r + 1) * length, h * model : (h + 1) * model],
            raw.at[i, 2 * r + h],
        )
        for i, source in enumerate((x_hbm, cot_hbm))
        for r in range(seqs)
        for h in range(2)
    ]
    for copy in raw_copies[: 2 * seqs] + own_copies + raw_copies[2 * seqs :]:
        copy.start()

    def starts(s):
        ends, end, start = [], 0, 0
        for d in range(doc_ref.shape[1]):
            size = doc_ref[s, d]
            end = end + size
            ends.append(end)
            start = start + jnp.where(size == length, end - length, 0)
        return start, ends

    def from_high(s, shape, dim):
        place = lax.broadcasted_iota(jnp.int32, shape, dim)
        return (place < starts(s)[0]).astype(jnp.int32) != x_index

    def segments(s, shape, dim):
        place = lax.broadcasted_iota(jnp.int32, shape, dim)
        place = jnp.where(from_high(s, shape, dim), place + length, place)
        segment = jnp.zeros(shape, jnp.int32)
        for end in starts(s)[1]:
            segment = segment + (place >= end).astype(jnp.int32)
        return segment

    def choose(s, i, dst):
        rows = pl.ds(pl.multiple_of(s * length, length), length)
        high = from_high(s, (length, model), 0)
        first, second = act_ref[i, rows, :model].astype(F32), act_ref[i, rows, model:].astype(F32)
        dst[rows, :] = jnp.where(high, second, first).astype(BF16)

    def put_back(s, i, own, other):
        rows = pl.ds(pl.multiple_of(s * length, length), length)
        high = from_high(s, (length, model), 0)
        a, b = own[rows, :].astype(F32), other[rows, :].astype(F32)
        down_ref[i, pl.ds(pl.multiple_of(2 * s * length, length), length), :] = jnp.where(high, b, a).astype(BF16)
        down_ref[i, pl.ds(pl.multiple_of((2 * s + 1) * length, length), length), :] = jnp.where(high, a, b).astype(BF16)

    def put_out(s, i):
        rows = pl.ds(pl.multiple_of(2 * s * length, length), 2 * length)
        return pltpu.make_async_copy(down_ref.at[i, rows, :], (output_hbm, input_hbm)[i].at[rows, :], done.at[i, s])

    n_half, n_quarter = model // 2, model // 4
    cut = hidden // 2
    sources = (act_ref, slope_ref, up_ref.at[:, :, :cut], up_ref.at[:, :, cut:])

    def by_core(t):
        there = pl.ds(pl.multiple_of((1 - core) * n_half, n_half), n_half)
        return remote(sources[t].at[:, there, :], half[t], send.at[0, t], recv.at[0, t], to_core)

    def quarter_of(place):
        return pl.ds(pl.multiple_of(place * n_quarter, n_quarter), n_quarter)

    def own_rows(place):
        return pl.ds(pl.multiple_of(place * rows_own, rows_own), rows_own)

    def by_first(t):
        if WAYS[t] == "xyz":
            return remote(half[t].at[1], mid[t], send.at[1, t], recv.at[1, t], to_x)
        return remote(half[t].at[:, quarter_of(1 - line), :], mid[t], send.at[1, t], recv.at[1, t], to_line)

    def by_second(t):
        if WAYS[t] == "xyz":
            return remote(mid[t].at[quarter_of(1 - line), :], owned[t], send.at[2, t], recv.at[2, t], to_line)
        if WAYS[t] == "yzx":
            return remote(owned[t].at[1], last, send.at[2, t], recv.at[2, t], to_x)
        return remote(mid[t].at[1], owned[t], send.at[2, t], recv.at[2, t], to_x)

    def by_rest(t, k):
        there = own_rows((rest + k) % depth)
        source = mid[t].at[:, there, :] if WAYS[t] == "yzx" else owned[t].at[there, :]
        return remote(source, shard[t].at[k - 1], send_z.at[t, k - 1], recv_z.at[t, k - 1], to_rest(k))

    def start_rest(t):
        for k in range(1, depth):
            by_rest(t, k).start()

    def rest_sum(t):
        if WAYS[t] == "yzx":
            total = mid[t][:, own_rows(rest), :].astype(F32)
        else:
            total = owned[t][own_rows(rest), :].astype(F32)
        for k in range(1, depth):
            by_rest(t, k).wait_recv()
            total = total + shard[t][k - 1].astype(F32)
        return total

    def after_core(t):
        by_core(t).wait_recv()
        for g in range(groups):
            add_rows(half[t].at[g], sources[t].at[g], core * n_half, 96)
        by_first(t).start()

    def after_first(t):
        by_first(t).wait_recv()
        if WAYS[t] == "xyz":
            add_rows(mid[t], half[t].at[0], 0, 96)
        else:
            for g in range(groups):
                add_rows(mid[t].at[g], half[t].at[g], line * n_quarter, 96)
        if WAYS[t] == "yzx":
            start_rest(t)
        else:
            by_second(t).start()

    def after_second(t, out):
        if WAYS[t] == "yzx":
            total = rest_sum(t)
            out[...] = total[0]
            owned[t][...] = total.astype(BF16)
            by_second(t).start()
            return
        by_second(t).wait_recv()
        if WAYS[t] == "xyz":
            add_rows(owned[t], mid[t], line * n_quarter, 96)
        else:
            add_rows(owned[t], mid[t].at[0], 0, 96)
        start_rest(t)

    def finish(t, out):
        if WAYS[t] == "yzx":
            by_second(t).wait_recv()
            out[...] += last[...].astype(F32)
        else:
            out[...] = rest_sum(t)

    def send_output(b):
        rows = pl.ds(pl.multiple_of(b * length, length), length)
        return remote(out_ref.at[rows, :], out_peer_ref.at[rows, :], send_in.at[1, b], recv_in.at[1, b], to_x)

    def send_input(s):
        rows = pl.ds(pl.multiple_of(s * length, length), length)
        return remote(in_ref.at[rows, :], in_peer_ref.at[rows, :], send_in.at[0, s], recv_in.at[0, s], to_x)

    attn_gain, attn_shift, down_bias, ffn_gain, ffn_shift, out_bias = (
        vec_ref[:, i * model : (i + 1) * model] for i in range(6)
    )

    def attend(s, g, biases):
        rows = pl.ds(pl.multiple_of(s * length, length), length)
        x = x_ref[rows, :]
        mask = seg_c_ref[s] == seg_r_ref[s]
        y = mm(x, w_ref[g])
        query = (0.125 * (y[:, :width] + biases[0:1, :width])).astype(BF16)
        key = y[:, width : 2 * width].astype(BF16)
        value = (y[:, 2 * width :] + biases[0:1, width : 2 * width]).astype(BF16)
        qkv_ref[g, rows, :width] = query
        qkv_ref[g, rows, width : 2 * width] = key
        qkv_ref[g, rows, 2 * width :] = value
        parts = []
        for p in range(pairs):
            at = slice(p * PAIR, (p + 1) * PAIR)
            k = key[:, at]
            both = None
            for h, (q, v) in enumerate(zip(halves(query[:, at]), halves(value[:, at]))):
                scores = jnp.where(mask, mm_t(q, k), -1000000000.0)
                expo = jnp.exp(scores - jnp.max(scores, -1, keepdims=True))
                probs = (expo * (1.0 / jnp.sum(expo, -1, keepdims=True))).astype(BF16)
                p_ref[s, (g * pairs + p) * 2 + h] = probs
                part = mm(probs, v)
                both = part if both is None else both + part
            parts.append(both.astype(BF16))
        ctx = jnp.concatenate(parts, 1)
        ctx_ref[g, rows, :] = ctx
        return mm(ctx, wo_ref[g])

    for copy in raw_copies[: 2 * seqs] + own_copies[:4]:
        copy.wait()

    @pl.loop(0, seqs)
    def _(s):
        rows = pl.ds(pl.multiple_of(s * length, length), length)
        choose(s, 0, x_ref)
        seg_c_ref[s] = segments(s, (length, 1), 0)
        seg_r_ref[s] = segments(s, (1, length), 1)
        acc_ref[rows, :] = x_ref[rows, :].astype(F32) + out_bias + attend(s, 0, bias_ref)
        for kind in range(3):

            @pl.when(s == min(kind, seqs - 1))
            def _():
                first_hop(kind)

    for copy in raw_copies[2 * seqs :]:
        copy.wait()

    @pl.loop(0, seqs)
    def _(s):
        choose(s, 1, cot_ref)

    first_hop(3)
    for kind in range(4):
        second_hop(kind)
    for kind in range(4):
        complete(kind)
    bias_over.wait()

    @pl.loop(0, seqs)
    def _(s):
        rows = pl.ds(pl.multiple_of(s * length, length), length)
        attn = acc_ref[rows, :] + attend(s, 1, bias_2)
        centred = attn - jnp.mean(attn, -1, keepdims=True)
        rstd = lax.rsqrt(jnp.mean(centred * centred, -1, keepdims=True) + EPS)
        xhat = centred * rstd
        xhat_ref[rows, :] = xhat
        rstd_ref[rows, :] = rstd
        low_ref[rows, :] = (xhat * attn_gain + attn_shift).astype(BF16)

        @pl.when(s == 0)
        def _():
            first_hop(4, 0)

        @pl.when(s == 1)
        def _():
            first_hop(5, 0)

        @pl.when(s == 2)
        def _():
            first_hop(4, 1)

    for copy in own_copies[4:]:
        copy.wait()
    store_by_owner(t_low_ref, low_ref[...].T, slice(None), n)

    def expand(c, g, biases):
        at = columns(c)
        bias_at = pl.ds(pl.multiple_of(2 * width + c * step, 128), step)

        @pl.loop(0, tokens // block)
        def _(b):
            rows = pl.ds(pl.multiple_of(b * block, block), block)
            u = mm(low_ref[rows, :], up_ref[g, :, at]) + biases[0:1, bias_at]
            square = u * u
            t = jnp.tanh(GELU_C * (u + 0.044715 * square * u))
            gate = 0.5 * (1.0 + t)
            act = (u * gate).astype(BF16)
            act_ref[g, rows, at] = act
            slope = gate + (0.5 * GELU_C) * u * (1.0 - t * t) * (1.0 + 0.134145 * square)
            slope_ref[g, rows, at] = slope.astype(BF16)
            acc_ref[rows, :] += mm(act, down_ref[g, at, :])

    acc_ref[...] = jnp.zeros_like(acc_ref)

    @pl.loop(0, 3)
    def _(c):
        expand(c, 0, bias_ref)

        @pl.when(c == 0)
        def _():
            second_hop(4, 0)

        @pl.when(c == 1)
        def _():
            second_hop(5, 0)
            first_hop(5, 1)

        @pl.when(c == 2)
        def _():
            second_hop(4, 1)
            first_hop(4, 2)

    @pl.loop(0, 3)
    def _(c):
        complete(4, c)
        complete(5, c)
        expand(c, 1, bias_2)

        @pl.when(c == 0)
        def _():
            first_hop(5, 2)
            second_hop(5, 1)

        @pl.when(c == 1)
        def _():
            second_hop(4, 2)
            second_hop(5, 2)

    small_ref[...] = jnp.zeros_like(small_ref)

    @pl.loop(0, seqs)
    def _(b):
        rows = pl.ds(pl.multiple_of(b * length, length), length)
        resid = xhat_ref[rows, :] * attn_gain + attn_shift + acc_ref[rows, :] + down_bias
        centred = resid - jnp.mean(resid, -1, keepdims=True)
        rstd = lax.rsqrt(jnp.mean(centred * centred, -1, keepdims=True) + EPS)
        xhat = centred * rstd
        out_ref[rows, :] = (xhat * ffn_gain + ffn_shift).astype(BF16)
        cot = cot_ref[rows, :].astype(F32)
        grad = norm_backward(xhat, rstd, ffn_gain, cot)
        acc_ref[rows, :] = grad
        dffn_ref[rows, :] = grad.astype(BF16)
        small_ref[3:4, :] += jnp.sum(grad, 0, keepdims=True)
        small_ref[4:5, :] += jnp.sum(cot * xhat, 0, keepdims=True)
        small_ref[5:6, :] += jnp.sum(cot, 0, keepdims=True)
        send_output(b).start()

    store_by_owner(t_grad_ref, dffn_ref[...].T, slice(None), n)

    def product(left, place, g, at):
        made = [
            mm(left[b * block : (b + 1) * block, :], place[g, :, at]).astype(BF16) for b in range(model // block)
        ]
        for b, value in enumerate(made):
            place[g, b * block : (b + 1) * block, at] = value

    tiny[...] = jnp.zeros_like(tiny)
    for g in range(groups):

        @pl.loop(0, 3)
        def _(c):
            product(t_grad_ref, act_ref, g, columns(c))

    by_core(0).start()
    for g in range(groups):

        @pl.loop(0, 3)
        def _(c):
            at = columns(c)
            total = jnp.zeros((1, step), F32)
            for b in range(tokens // block):
                rows = slice(b * block, (b + 1) * block)
                d_upper = mm_t(dffn_ref[rows, :], down_ref[g, at, :]) * slope_ref[g, rows, at].astype(F32)
                total = total + jnp.sum(d_upper, 0, keepdims=True)
                d_low = d_upper.astype(BF16)
                slope_ref[g, rows, at] = d_low
                acc_ref[rows, :] += mm_t(d_low, up_ref[g, :, at])
            tiny[3 + g, 0:1, at] = total
            product(t_low_ref, slope_ref, g, at)
            if g == 0:

                @pl.when(c == 1)
                def _():
                    after_core(0)

    by_core(1).start()

    @pl.loop(0, seqs)
    def _(b):
        rows = pl.ds(pl.multiple_of(b * length, length), length)
        d_normed = acc_ref[rows, :]
        xhat = xhat_ref[rows, :]
        grad = norm_backward(xhat, rstd_ref[rows, :], attn_gain, d_normed)
        acc_ref[rows, :] = grad
        small_ref[0:1, :] += jnp.sum(grad, 0, keepdims=True)
        small_ref[1:2, :] += jnp.sum(d_normed * xhat, 0, keepdims=True)
        small_ref[2:3, :] += jnp.sum(d_normed, 0, keepdims=True)

    store_by_owner(t_low_ref, x_ref[...].T, slice(None), n)

    @pl.loop(0, seqs)
    def _(s):
        backward_sequence(
            s, lambda v, at: store_by_owner(t_grad_ref, v, at, n),
            acc_ref, w_ref, wo_ref, qkv_ref, p_ref, in_ref, qkv_ref,
        )
        send_input(s).start()

        @pl.when(s == 0)
        def _():
            after_core(1)

        @pl.when(s == min(1, seqs - 1))
        def _():
            after_first(0)

    tiny_core = remote(tiny.at[0:3], tiny_1, send.at[3, 1], recv.at[3, 1], to_core)
    tiny_line = remote(tiny_1, tiny_2, send.at[3, 2], recv.at[3, 2], to_line)
    tiny_over = remote(tiny_2.at[1:3], tiny_x, send.at[3, 3], recv.at[3, 3], to_x)

    def tiny_rest(k):
        return remote(tiny_x, tiny_z.at[k - 1], send_z.at[4, k - 1], recv_z.at[4, k - 1], to_rest(k))

    for g in range(groups):
        column = jnp.sum(qkv_ref[g].astype(F32), 0, keepdims=True)
        tiny[g, 0:1, :width] = column[:, :width]
        tiny[g, 0:1, width : 2 * width] = column[:, 2 * width :]
        tiny[g, 1:2, :] = tiny[3 + g, 0:1, :]
    tiny[2, :, :model] = small_ref[...]
    for kind in range(4):
        sent(kind)
    for c in range(3):
        sent(4, c)
        sent(5, c)
    tiny_core.start()
    for g in range(groups):
        weight_products(g, t_low_ref, t_grad_ref, qkv_ref, ctx_ref, up_ref)
    by_core(2).start()
    by_core(3).start()
    tiny_core.wait_recv()
    tiny_1[...] += tiny[0:3]
    tiny_line.start()
    after_core(2)
    after_core(3)
    for i, (one, own, other) in enumerate(
        ((send_output, out_ref, out_peer_ref), (send_input, in_ref, in_peer_ref))
    ):

        @pl.loop(0, seqs)
        def _(s):
            one(s).wait_recv()
            put_back(s, i, own, other)
            put_out(s, i).start()

    tiny_line.wait_recv()
    tiny_2[...] += tiny_1[...]
    tiny_over.start()
    after_first(1)
    after_second(0, rd_ref)
    after_first(3)
    tiny_over.wait_recv()
    tiny_x[0] += tiny_2[0]
    tiny_x[1] += tiny_2[2]
    for k in range(1, depth):
        tiny_rest(k).start()
    after_first(2)
    after_second(1, ru_ref)
    after_second(3, rb_ref)
    finish(0, rd_ref)
    after_second(2, ra_ref)
    total = tiny_x[...]
    for k in range(1, depth):
        tiny_rest(k).wait_recv()
        total = total + tiny_z[k - 1]
    sums_ref[...] = total
    finish(1, ru_ref)
    finish(3, rb_ref)
    finish(2, ra_ref)
    for s in range(seqs):
        send_output(s).wait_send()
        send_input(s).wait_send()
        for i in range(2):
            put_out(s, i).wait()
    for t in range(4):
        by_core(t).wait_send()
        by_first(t).wait_send()
        by_second(t).wait_send()
        for k in range(1, depth):
            by_rest(t, k).wait_send()
    tiny_core.wait_send()
    tiny_line.wait_send()
    tiny_over.wait_send()
    for k in range(1, depth):
        tiny_rest(k).wait_send()


def call(kernel, outs, scratch, flops, *args, scalar=(), far=(), far_out=(), collective=None):
    shapes = [jax.ShapeDtypeStruct(s, d) for s, d in outs]
    moved = sum(a.size * a.dtype.itemsize for a in args) + sum(s.size * s.dtype.itemsize for s in shapes)
    vmem = pl.BlockSpec(memory_space=pltpu.VMEM)
    return pl.pallas_call(
        kernel,
        out_shape=shapes,
        in_specs=[
            pl.BlockSpec(memory_space=pltpu.SMEM if i in scalar else pl.ANY if i in far else pltpu.VMEM)
            for i in range(len(args))
        ],
        out_specs=[pl.BlockSpec(memory_space=pl.ANY) if i in far_out else vmem for i in range(len(shapes))],
        scratch_shapes=[pltpu.VMEM(*s) if isinstance(s, tuple) else s for s in scratch],
        compiler_params=pltpu.CompilerParams(
            vmem_limit_bytes=VMEM_LIMIT, collective_id=collective, has_side_effects=collective is not None
        ),
        cost_estimate=pl.CostEstimate(flops=flops, bytes_accessed=moved, transcendentals=0),
    )(*args)


def factors_of(n):
    found = []
    while n > 4 or (n > 1 and len(found) < 2):
        found.append(2)
        n //= 2
    return found + ([n] if n > 1 else [])


def swap(v):
    return lax.ppermute(v, "mp", [(0, 1), (1, 0)])


def shift_dp(v, n, stride, factor, k):
    def target(d):
        i = (d // stride) % factor
        return d + ((i + k) % factor - i) * stride

    return lax.ppermute(v, "dp", [(d, target(d)) for d in range(n)])


def with_peer(own, n):
    core = lax.axis_index("dp") % 2
    half = own.shape[0] // 2
    mine = swap(lax.dynamic_slice_in_dim(own, core * half, half, 0))
    other = shift_dp(mine, n, 1, 2, 1)
    first = core == 0
    peer = jnp.concatenate([jnp.where(first, mine, other), jnp.where(first, other, mine)], 0)
    return jnp.stack([own, peer])


def reduce_to_owner(grad, n):
    index = lax.axis_index("dp")
    rows = grad.shape[1] // n
    left = grad.reshape(2, n, rows, grad.shape[2])
    stride = 1
    for factor in factors_of(n):
        parts = left.reshape(2, left.shape[1] // factor, factor, rows, left.shape[3])
        i = (index // stride) % factor

        def pick(at):
            return lax.dynamic_index_in_dim(parts, at, 2, keepdims=False)

        total = pick(i).astype(F32)
        for k in range(1, factor):
            total = total + shift_dp(pick((i + k) % factor), n, stride, factor, k).astype(F32)
        left = total.astype(BF16)
        stride *= factor
    left = left.reshape(2, rows, left.shape[3])
    return left[0].astype(F32) + swap(left[1]).astype(F32)


def per_device(
    n, layer_input, doc_lengths, q_weight, q_bias, k_weight, v_weight, v_bias, out_weight, out_bias,
    attn_gain, attn_shift, up_weight, up_bias, down_weight, down_bias, ffn_gain, ffn_shift, cotangent,
):
    rows = doc_lengths.shape[0]
    tokens, model = layer_input.shape
    length = tokens // rows
    part = length // 2
    mine = rows * part
    width = q_weight.shape[1]
    hidden = up_weight.shape[1]
    heads = width // HD
    x_index = lax.axis_index("mp")

    remote = (
        (model // n) % 16 == 0 and n % 4 == 0 and n > 4
        and hidden == 2 * model and 4 * width == hidden and hidden % 384 == 0 and rows >= 3 and mine == model
    )
    if remote:
        depth = n // 4
        dma = pltpu.SemaphoreType.DMA
        wide = (hidden, hidden, model, model)
        quarter = model // 4
        vectors = jnp.concatenate(
            [attn_gain, attn_shift, down_bias, ffn_gain, ffn_shift, out_bias, q_bias, v_bias, up_bias]
        ).astype(F32)[None]
        layer_output, input_grad, g_down, g_up, g_first, g_last, sums = call(
            functools.partial(whole_layer, n),
            [((tokens, model), BF16)] * 2
            + [((model // n, c), F32) for c in wide]
            + [((2, 8, hidden), F32)],
            [
                ((mine, model), BF16),
                ((mine, model), BF16),
                ((rows, part, 1), jnp.int32),
                ((rows, 1, part), jnp.int32),
                ((mine, model), BF16),
                ((mine, model), BF16),
                ((mine, model), BF16),
                ((2, model, 3 * width), BF16),
                ((2, width, model), BF16),
                ((2, model, hidden), BF16),
                ((2, hidden, model), BF16),
                ((1, 2 * width + hidden), F32),
                ((2, mine, 3 * width), BF16),
                ((rows, 2 * heads, part, part), BF16),
                ((2, mine, width), BF16),
                ((mine, model), F32),
                ((mine, 1), F32),
                ((mine, model), BF16),
                ((2, model, hidden), BF16),
                ((2, model, hidden), BF16),
                ((mine, model), F32),
                ((model, mine), BF16),
                ((model, mine), BF16),
                ((8, model), F32),
            ]
            + [((2, model // 2, c), BF16) for c in wide]
            + [((2 * quarter, c) if w == "xyz" else (2, quarter, c), BF16) for w, c in zip(WAYS, wide)]
            + [((2, model // n, c) if w == "yzx" else (quarter, c), BF16) for w, c in zip(WAYS, wide)]
            + [((depth - 1,) + (2,) * (w == "yzx") + (model // n, c), BF16) for w, c in zip(WAYS, wide)]
            + [
                ((5, 8, hidden), F32),
                ((3, 8, hidden), F32),
                ((3, 8, hidden), F32),
                ((2, 8, hidden), F32),
                ((depth - 1, 2, 8, hidden), F32),
                ((model // n, hidden), BF16),
                dma((5, 4)), dma((5, 4)), dma((5, depth - 1)), dma((5, depth - 1)), dma((2, rows)), dma((2, rows)),
                dma((4, 10)), dma((4, 10)), dma((6,)), dma((2, 2 * rows)), dma((2, rows)),
            ],
            2 * mine * model * (24 * width + 12 * hidden),
            doc_lengths, layer_input, cotangent, vectors,
            q_weight, k_weight, v_weight, out_weight, up_weight, down_weight,
            scalar=(0,), far=(1, 2, 4, 5, 6, 7, 8, 9), far_out=(0, 1), collective=0,
        )
        g_attn = jnp.concatenate([g_first, g_last], -1)
        small = sums[1, :, :model]
        sums = jnp.concatenate([sums[0, 0, : 2 * width], sums[0, 1]])
    else:
        ends = jnp.cumsum(doc_lengths, axis=-1, dtype=jnp.int32)
        start = jnp.sum(jnp.where(doc_lengths == part, ends - part, 0), -1)
        place = jnp.arange(length, dtype=jnp.int32)
        segment = jnp.sum((place[None, :, None] >= ends[:, None, :]).astype(jnp.int32), -1, dtype=jnp.int32)
        before = place[None, :part] < start[:, None]
        from_high = before != (x_index == 1)

        def take(v):
            v = v.reshape(rows, 2, part, model)
            return jnp.where(from_high[:, :, None], v[:, 1], v[:, 0]).reshape(mine, model)

        def give(own, other):
            own, other = own.reshape(rows, part, model), other.reshape(rows, part, model)
            low = jnp.where(from_high[:, :, None], other, own)
            high = jnp.where(from_high[:, :, None], own, other)
            return jnp.stack([low, high], 1).reshape(tokens, model)

        seg = jnp.where(from_high, segment[:, part:], segment[:, :part])
        x = take(layer_input)
        cot = take(cotangent)
        own_bias = jnp.concatenate([q_bias, v_bias, up_bias])
        w_qkv = with_peer(jnp.concatenate([q_weight, k_weight, v_weight], 1), n)
        w_out = with_peer(out_weight, n)
        w_up = with_peer(up_weight, n)
        w_down = with_peer(down_weight, n)
        bias = jnp.stack([own_bias, swap(own_bias)]).astype(F32)[:, None, :]
        b_qkv = jnp.concatenate([bias[..., :width], jnp.zeros_like(bias[..., :width]), bias[..., width : 2 * width]], -1)
        b_up = bias[..., 2 * width :]
        vectors = jnp.stack([attn_gain, attn_shift, down_bias, ffn_gain, ffn_shift]).astype(F32)

        qkv, probs, ctx, xhat, rstd, low = call(
            attention_forward,
            [
                ((2, mine, 3 * width), BF16),
                ((rows, 2 * heads, part, part), BF16),
                ((2, mine, width), BF16),
                ((mine, model), F32),
                ((mine, 1), F32),
                ((mine, model), BF16),
            ],
            [],
            2 * mine * model * 8 * width,
            x, w_qkv, b_qkv, w_out, seg[:, :, None], seg[:, None, :],
            out_bias.astype(F32)[None], vectors[0:1], vectors[1:2],
        )
        output, g_down, g_up, d_resid, small, up_bias_grad = call(
            feed_forward,
            [
                ((mine, model), BF16),
                ((2, model, hidden), BF16),
                ((2, model, hidden), BF16),
                ((mine, model), F32),
                ((8, model), F32),
                ((2, 1, hidden), F32),
            ],
            [
                ((2, mine, hidden), BF16),
                ((2, mine, hidden), BF16),
                ((mine, model), F32),
                ((mine, model), BF16),
                ((model, mine), BF16),
                ((model, mine), BF16),
            ],
            2 * mine * model * 2 * hidden * 6,
            low, xhat, rstd, w_up, b_up, w_down, vectors, cot,
        )
        scratch = [((2, mine, 3 * width), BF16), ((model, mine), BF16), ((model, mine), BF16)]
        flops = 2 * mine * model * 16 * width
        output_peer = swap(output)
        grad_in, g_attn, bias_grad = call(
            attention_backward_plain,
            [((mine, model), BF16), ((2, model, 4 * width), BF16), ((2, 1, 3 * width), F32)],
            scratch, flops, x, d_resid, w_qkv, w_out, qkv, probs, ctx,
        )
        grad_in_peer = swap(grad_in)
        g_down, g_up, g_attn = (reduce_to_owner(v, n) for v in (g_down, g_up, g_attn))
        sums = jnp.concatenate([bias_grad[:, 0, :width], bias_grad[:, 0, 2 * width :], up_bias_grad[:, 0]], -1)
        sums = jnp.where(x_index == 0, sums, sums[::-1])
        sums, small = lax.psum((sums, small), ("dp", "mp"))
        sums = lax.dynamic_index_in_dim(sums, x_index, 0, keepdims=False)
        layer_output = give(output, output_peer)
        input_grad = give(grad_in, grad_in_peer)
    down_weight_grad = g_down.T
    up_weight_grad = g_up
    return (
        layer_output,
        input_grad,
        g_attn[:, :width],
        sums[:width],
        g_attn[:, width : 2 * width],
        g_attn[:, 2 * width : 3 * width],
        sums[width : 2 * width],
        g_attn[:, 3 * width :].T,
        small[0],
        small[1],
        small[2],
        up_weight_grad,
        sums[2 * width :],
        down_weight_grad,
        small[3],
        small[4],
        small[5],
    )


def solution(mesh):
    in_specs = (
        P("dp", None), P("dp", None), P(None, "mp"), P("mp"), P(None, "mp"), P(None, "mp"), P("mp"),
        P("mp", None), P(), P(), P(), P(None, "mp"), P("mp"), P("mp", None), P(), P(), P(), P("dp", None),
    )
    out_specs = (
        P("dp", None), P("dp", None), P("dp", "mp"), P("mp"), P("dp", "mp"), P("dp", "mp"), P("mp"),
        P("mp", "dp"), P(), P(), P(), P("dp", "mp"), P("mp"), P("mp", "dp"), P(), P(), P(),
    )
    return jax.shard_map(
        functools.partial(per_device, mesh.shape["dp"]),
        mesh=mesh, in_specs=in_specs, out_specs=out_specs, check_vma=False,
    )
```

```python
import functools

import jax
import jax.numpy as jnp
from jax import lax
from jax.experimental import pallas as pl
from jax.experimental.pallas import tpu as pltpu
from jax.sharding import PartitionSpec as P

HD = 64
PAIR = 2 * HD
EPS = 1e-12
GELU_C = 0.7978845608028654
F32 = jnp.float32
BF16 = jnp.bfloat16
CHUNK = 512
VMEM_LIMIT = 67043328
MESH = pl.DeviceIdType.MESH


def mm(a, b):
    return jnp.dot(a, b, preferred_element_type=F32)


def mm_t(a, b):
    return lax.dot_general(a, b, (((1,), (1,)), ((), ())), preferred_element_type=F32)


def t_mm(a, b):
    return lax.dot_general(a, b, (((0,), (0,)), ((), ())), preferred_element_type=F32)


def halves(v):
    lane = lax.broadcasted_iota(jnp.int32, v.shape, 1)
    zero = jnp.zeros_like(v)
    return jnp.where(lane < HD, v, zero), jnp.where(lane < HD, zero, v)


def attention_forward(
    x_ref, w_ref, b_ref, wo_ref, seg_c_ref, seg_r_ref, bo_ref, gain_ref, shift_ref,
    qkv_ref, p_ref, ctx_ref, xhat_ref, rstd_ref, low_ref,
):
    seqs, length = seg_c_ref.shape[0], seg_c_ref.shape[1]
    groups, width = wo_ref.shape[0], wo_ref.shape[1]
    pairs = width // PAIR

    @pl.loop(0, seqs)
    def _(s):
        rows = pl.ds(pl.multiple_of(s * length, length), length)
        x = x_ref[rows, :]
        mask = seg_c_ref[s] == seg_r_ref[s]
        attn = x.astype(F32) + bo_ref[...]
        for g in range(groups):
            y = mm(x, w_ref[g]) + b_ref[g]
            query = (0.125 * y[:, :width]).astype(BF16)
            key = y[:, width : 2 * width].astype(BF16)
            value = y[:, 2 * width :].astype(BF16)
            qkv_ref[g, rows, :width] = query
            qkv_ref[g, rows, width : 2 * width] = key
            qkv_ref[g, rows, 2 * width :] = value
            parts = []
            for p in range(pairs):
                at = slice(p * PAIR, (p + 1) * PAIR)
                k = key[:, at]
                both = None
                for h, (q, v) in enumerate(zip(halves(query[:, at]), halves(value[:, at]))):
                    scores = jnp.where(mask, mm_t(q, k), -1000000000.0)
                    expo = jnp.exp(scores - jnp.max(scores, -1, keepdims=True))
                    probs = (expo * (1.0 / jnp.sum(expo, -1, keepdims=True))).astype(BF16)
                    p_ref[s, (g * pairs + p) * 2 + h] = probs
                    part = mm(probs, v)
                    both = part if both is None else both + part
                parts.append(both.astype(BF16))
            ctx = jnp.concatenate(parts, 1)
            ctx_ref[g, rows, :] = ctx
            attn = attn + mm(ctx, wo_ref[g])
        mean = jnp.mean(attn, -1, keepdims=True)
        centred = attn - mean
        rstd = lax.rsqrt(jnp.mean(centred * centred, -1, keepdims=True) + EPS)
        xhat = centred * rstd
        xhat_ref[rows, :] = xhat
        rstd_ref[rows, :] = rstd
        low_ref[rows, :] = (xhat * gain_ref[...] + shift_ref[...]).astype(BF16)


def norm_backward(xhat, rstd, gain, grad):
    scaled = grad * gain
    return rstd * (
        scaled
        - jnp.mean(scaled, -1, keepdims=True)
        - xhat * jnp.mean(scaled * xhat, -1, keepdims=True)
    )


def store_by_owner(dst, value, at, n):
    rows = value.shape[0] // n
    for d in range(n):
        place = d % 2 * 8 + d // 2 % 2 * 4 + d // 4 % 2 * 2 + d // 8
        dst[place * rows : (place + 1) * rows, at] = value[d * rows : (d + 1) * rows, :]


def feed_forward(
    low_ref, xhat_ref, rstd_ref, up_ref, ub_ref, down_ref, vec_ref, cot_ref,
    out_ref, gd_ref, gu_ref, d_resid_ref, small_ref, ubg_ref,
    act_ref, slope_ref, acc_ref, dffn_ref, dffn_t_ref, low_t_ref,
):
    tokens, width = low_ref.shape
    groups, hidden = up_ref.shape[0], up_ref.shape[2]
    step = min(CHUNK, hidden)
    per = hidden // step
    block = 256
    low_t_ref[...] = low_ref[...].T
    acc_ref[...] = jnp.zeros_like(acc_ref)

    @pl.loop(0, groups * per)
    def _(i):
        g = i // per
        at = pl.ds(pl.multiple_of((i % per) * step, step), step)

        @pl.loop(0, tokens // block)
        def _(b):
            rows = pl.ds(pl.multiple_of(b * block, block), block)
            u = mm(low_ref[rows, :], up_ref[g, :, at]) + ub_ref[g, :, at]
            square = u * u
            t = jnp.tanh(GELU_C * (u + 0.044715 * square * u))
            half = 0.5 * (1.0 + t)
            act = (u * half).astype(BF16)
            act_ref[g, rows, at] = act
            slope = half + (0.5 * GELU_C) * u * (1.0 - t * t) * (1.0 + 0.134145 * square)
            slope_ref[g, rows, at] = slope.astype(BF16)
            acc_ref[rows, :] += mm(act, down_ref[g, at, :])

    small_ref[...] = jnp.zeros_like(small_ref)
    attn_gain, attn_shift = vec_ref[0:1, :], vec_ref[1:2, :]
    down_bias = vec_ref[2:3, :]
    ffn_gain, ffn_shift = vec_ref[3:4, :], vec_ref[4:5, :]

    @pl.loop(0, tokens // block)
    def _(b):
        rows = pl.ds(pl.multiple_of(b * block, block), block)
        resid = xhat_ref[rows, :] * attn_gain + attn_shift + acc_ref[rows, :] + down_bias
        centred = resid - jnp.mean(resid, -1, keepdims=True)
        rstd = lax.rsqrt(jnp.mean(centred * centred, -1, keepdims=True) + EPS)
        xhat = centred * rstd
        out_ref[rows, :] = (xhat * ffn_gain + ffn_shift).astype(BF16)
        cot = cot_ref[rows, :].astype(F32)
        grad = norm_backward(xhat, rstd, ffn_gain, cot)
        acc_ref[rows, :] = grad
        dffn_ref[rows, :] = grad.astype(BF16)
        small_ref[3:4, :] += jnp.sum(grad, 0, keepdims=True)
        small_ref[4:5, :] += jnp.sum(cot * xhat, 0, keepdims=True)
        small_ref[5:6, :] += jnp.sum(cot, 0, keepdims=True)

    dffn_t_ref[...] = dffn_ref[...].T

    @pl.loop(0, groups * per)
    def _(i):
        g = i // per
        at = pl.ds(pl.multiple_of((i % per) * step, step), step)
        total = jnp.zeros((1, step), F32)
        for b in range(tokens // block):
            rows = slice(b * block, (b + 1) * block)
            d_upper = mm_t(dffn_ref[rows, :], down_ref[g, at, :]) * slope_ref[g, rows, at].astype(F32)
            total = total + jnp.sum(d_upper, 0, keepdims=True)
            d_low = d_upper.astype(BF16)
            slope_ref[g, rows, at] = d_low
            acc_ref[rows, :] += mm_t(d_low, up_ref[g, :, at])
        ubg_ref[g, :, at] = total
        for b in range(width // block):
            rows = slice(b * block, (b + 1) * block)
            gd_ref[g, rows, at] = mm(dffn_t_ref[rows, :], act_ref[g, :, at]).astype(BF16)
            gu_ref[g, rows, at] = mm(low_t_ref[rows, :], slope_ref[g, :, at]).astype(BF16)

    @pl.loop(0, tokens // block)
    def _(b):
        rows = pl.ds(pl.multiple_of(b * block, block), block)
        d_normed = acc_ref[rows, :]
        xhat = xhat_ref[rows, :]
        grad = norm_backward(xhat, rstd_ref[rows, :], attn_gain, d_normed)
        d_resid_ref[rows, :] = grad
        small_ref[0:1, :] += jnp.sum(grad, 0, keepdims=True)
        small_ref[1:2, :] += jnp.sum(d_normed * xhat, 0, keepdims=True)
        small_ref[2:3, :] += jnp.sum(d_normed, 0, keepdims=True)


def backward_sequence(s, put, d_resid_ref, w_ref, wo_ref, qkv_ref, p_ref, in_ref, dq_ref):
    length, groups, width = p_ref.shape[2], wo_ref.shape[0], wo_ref.shape[1]
    pairs = width // PAIR
    rows = pl.ds(pl.multiple_of(s * length, length), length)
    d_resid = d_resid_ref[rows, :]
    d_attn = d_resid.astype(BF16)
    put(d_attn.T, rows)
    total = d_resid
    for g in range(groups):
        d_ctx = mm_t(d_attn, wo_ref[g]).astype(BF16)
        for p in range(pairs):
            at = slice(p * PAIR, (p + 1) * PAIR)
            q_at, k_at, v_at = (slice(o * width + p * PAIR, o * width + (p + 1) * PAIR) for o in range(3))
            value = qkv_ref[g, rows, v_at]
            q_pair = halves(qkv_ref[g, rows, q_at])
            k_pair = halves(qkv_ref[g, rows, k_at])
            c_pair = halves(d_ctx[:, at])
            dq = dk = dv = None
            for h in range(2):
                low = p_ref[s, (g * pairs + p) * 2 + h]
                probs = low.astype(F32)
                d_probs = mm_t(c_pair[h], value)
                inner = jnp.sum(probs * d_probs, -1, keepdims=True)
                d_scores = (probs * (d_probs - inner)).astype(BF16)
                dv_h = t_mm(low, c_pair[h])
                dq_h = mm(d_scores, k_pair[h])
                dk_h = t_mm(d_scores, q_pair[h])
                dq = dq_h if dq is None else dq + dq_h
                dk = dk_h if dk is None else dk + dk_h
                dv = dv_h if dv is None else dv + dv_h
            dq_ref[g, rows, q_at] = (0.125 * dq).astype(BF16)
            dq_ref[g, rows, k_at] = dk.astype(BF16)
            dq_ref[g, rows, v_at] = dv.astype(BF16)
        total = total + mm_t(dq_ref[g, rows, :], w_ref[g])
    in_ref[rows, :] = total.astype(BF16)


def weight_products(g, x_t_ref, dattn_t_ref, dq_ref, ctx_ref, ga_ref):
    block, wide = 256, dq_ref.shape[2]

    @pl.loop(0, x_t_ref.shape[0] // block)
    def _(b):
        rows = pl.ds(pl.multiple_of(b * block, block), block)
        ga_ref[g, rows, :wide] = mm(x_t_ref[rows, :], dq_ref[g]).astype(BF16)
        ga_ref[g, rows, wide:] = mm(dattn_t_ref[rows, :], ctx_ref[g]).astype(BF16)


def attention_backward_plain(
    x_ref, d_resid_ref, w_ref, wo_ref, qkv_ref, p_ref, ctx_ref,
    in_ref, ga_ref, bg_ref,
    dq_ref, dattn_t_ref, x_t_ref,
):
    groups, width = wo_ref.shape[0], wo_ref.shape[1]
    x_t_ref[...] = x_ref[...].T

    def put(v, at):
        dattn_t_ref[:, at] = v

    @pl.loop(0, p_ref.shape[0])
    def _(s):
        backward_sequence(s, put, d_resid_ref, w_ref, wo_ref, qkv_ref, p_ref, in_ref, dq_ref)

    for g in range(groups):
        bg_ref[g] = jnp.sum(dq_ref[g].astype(F32), 0, keepdims=True)
        weight_products(g, x_t_ref, dattn_t_ref, dq_ref, ctx_ref, ga_ref)


def whole_layer(
    n, doc_ref, x_hbm, cot_hbm, vec_ref, wq_hbm, wk_hbm, wv_hbm, wo_hbm, up_hbm, down_hbm,
    output_hbm, input_hbm, rd_ref, ru_ref, ra_ref, sums_ref,
    x_ref, cot_ref, seg_c_ref, seg_r_ref, out_ref, out_peer_ref, in_peer_ref,
    w_ref, wo_ref, up_ref, down_ref, bias_2, qkv_ref, p_ref, ctx_ref, xhat_ref, rstd_ref, low_ref, act_ref, slope_ref,
    acc_ref, t_low_ref, t_grad_ref, small_ref, *rest_refs,
):
    in_ref, dffn_ref = cot_ref, low_ref
    level_0, level_1, level_2, level_3, level_4, tiny, tiny_1, tiny_2, tiny_x, tiny_z = rest_refs[:10]
    send, recv, send_0, recv_0, send_z, recv_z, send_in, recv_in, g_send, g_recv, g_local, raw, done = rest_refs[10:]
    seqs, length = seg_c_ref.shape[0], seg_c_ref.shape[1]
    groups, width, model = wo_ref.shape
    hidden = up_ref.shape[2]
    pairs = width // PAIR
    tokens = seqs * length
    step = hidden // 3
    block = 256
    rows_own = model // n
    depth = n // 4
    index = lax.axis_index("dp")
    x_index = lax.axis_index("mp")
    core, line, rest = index % 2, index // 2 % 2, index // 4
    to_core = {"dp": index + 1 - 2 * core}
    to_line = {"dp": index + 2 - 4 * line}
    to_x = {"mp": 1 - x_index}

    near, far = rest % 2, rest // 2
    to_near = {"dp": index + 4 - 8 * near}
    to_far = {"dp": index + 8 - 16 * far}

    def to_rest(k):
        return {"dp": (rest + k) % depth * 4 + index % 4}

    barrier = pltpu.get_barrier_semaphore()
    peers = [to_core, to_line, to_x] + [to_rest(k) for k in range(1, depth)]
    for peer in peers:
        pl.semaphore_signal(barrier, inc=1, device_id=peer, device_id_type=MESH)
    pl.semaphore_wait(barrier, len(peers))

    def remote(src, dst, s, r, device):
        return pltpu.make_async_remote_copy(
            src_ref=src, dst_ref=dst, send_sem=s, recv_sem=r, device_id=device, device_id_type=MESH
        )

    def columns(c):
        return pl.ds(pl.multiple_of(c * step, step), step)

    def ends_of(kind, c, piece):
        if kind < 3:
            size = model // 4
            rows = pl.ds(pl.multiple_of(piece * size, size), size)
            return (wq_hbm, wk_hbm, wv_hbm)[kind].at[rows, :], w_ref.at[1, rows, kind * width : (kind + 1) * width]
        if kind == 3:
            size = width // 4
            rows = pl.ds(pl.multiple_of(piece * size, size), size)
            return wo_hbm.at[rows, :], wo_ref.at[1, rows, :]
        if kind == 4:
            size = model // 4
            rows = pl.ds(pl.multiple_of(piece * size, size), size)
            return up_hbm.at[rows, columns(c)], up_ref.at[1, rows, columns(c)]
        size = step // 4
        rows = pl.ds(pl.multiple_of(c * step + piece * size, size), size)
        return down_hbm.at[rows, :], down_ref.at[1, rows, :]

    def slot(kind, c):
        return kind if kind < 4 else (4 + c if kind == 4 else 7 + c)

    def over_x(kind, c=0):
        src, dst = ends_of(kind, c, 2 * line + core)
        i = slot(kind, c)
        return remote(src, dst, g_send.at[0, i], g_recv.at[0, i], to_x)

    def pass_on(kind, c, hop):
        at = ends_of(kind, c, 2 * (1 - line) + core if hop == 3 else 2 * line + core)[1]
        i = slot(kind, c)
        return remote(at, at, g_send.at[hop, i], g_recv.at[hop, i], to_line if hop == 2 else to_core)

    def first_hop(kind, c=0):
        over_x(kind, c).wait_recv()
        pass_on(kind, c, 2).start()
        pass_on(kind, c, 1).start()

    def second_hop(kind, c=0):
        pass_on(kind, c, 2).wait_recv()
        pass_on(kind, c, 3).start()

    def complete(kind, c=0):
        pass_on(kind, c, 1).wait_recv()
        pass_on(kind, c, 3).wait_recv()

    def sent(kind, c=0):
        over_x(kind, c).wait_send()
        for hop in (1, 2, 3):
            pass_on(kind, c, hop).wait_send()

    bias_ref = vec_ref.at[:, 6 * model :]
    bias_over = remote(bias_ref, bias_2, send.at[3, 0], recv.at[3, 0], to_x)
    bias_over.start()
    for kind in range(4):
        over_x(kind).start()
    for c in range(3):
        over_x(4, c).start()
        over_x(5, c).start()
    own_copies = [
        pltpu.make_async_copy(src, dst, g_local.at[i])
        for i, (src, dst) in enumerate(
            [(w, w_ref.at[0, :, o * width : (o + 1) * width]) for o, w in enumerate((wq_hbm, wk_hbm, wv_hbm))]
            + [(wo_hbm, wo_ref.at[0]), (up_hbm, up_ref.at[0]), (down_hbm, down_ref.at[0])]
        )
    ]
    raw_copies = [
        pltpu.make_async_copy(
            source.at[(2 * r + h) * length : (2 * r + h + 1) * length, :],
            act_ref.at[i, r * length : (r + 1) * length, h * model : (h + 1) * model],
            raw.at[i, 2 * r + h],
        )
        for i, source in enumerate((x_hbm, cot_hbm))
        for r in range(seqs)
        for h in range(2)
    ]
    for copy in raw_copies[: 2 * seqs] + own_copies + raw_copies[2 * seqs :]:
        copy.start()

    def starts(s):
        ends, end, start = [], 0, 0
        for d in range(doc_ref.shape[1]):
            size = doc_ref[s, d]
            end = end + size
            ends.append(end)
            start = start + jnp.where(size == length, end - length, 0)
        return start, ends

    def from_high(s, shape, dim):
        place = lax.broadcasted_iota(jnp.int32, shape, dim)
        return (place < starts(s)[0]).astype(jnp.int32) != x_index

    def segments(s, shape, dim):
        place = lax.broadcasted_iota(jnp.int32, shape, dim)
        place = jnp.where(from_high(s, shape, dim), place + length, place)
        segment = jnp.zeros(shape, jnp.int32)
        for end in starts(s)[1]:
            segment = segment + (place >= end).astype(jnp.int32)
        return segment

    def choose(s, i, dst):
        rows = pl.ds(pl.multiple_of(s * length, length), length)
        high = from_high(s, (length, model), 0)
        first, second = act_ref[i, rows, :model].astype(F32), act_ref[i, rows, model:].astype(F32)
        dst[rows, :] = jnp.where(high, second, first).astype(BF16)

    def put_back(s, i, own, other):
        rows = pl.ds(pl.multiple_of(s * length, length), length)
        high = from_high(s, (length, model), 0)
        a, b = own[rows, :].astype(F32), other[rows, :].astype(F32)
        down_ref[i, pl.ds(pl.multiple_of(2 * s * length, length), length), :] = jnp.where(high, b, a).astype(BF16)
        down_ref[i, pl.ds(pl.multiple_of((2 * s + 1) * length, length), length), :] = jnp.where(high, a, b).astype(BF16)

    def put_out(s, i):
        rows = pl.ds(pl.multiple_of(2 * s * length, length), 2 * length)
        return pltpu.make_async_copy(down_ref.at[i, rows, :], (output_hbm, input_hbm)[i].at[rows, :], done.at[i, s])

    cut = hidden // 2
    size = model // 8
    sources = (act_ref, slope_ref, up_ref)

    def source(t, where, block):
        rows = pl.ds(pl.multiple_of((where * 4 + block) * size, size), size)
        return sources[t // 2].at[:, rows, t % 2 * cut : (t % 2 + 1) * cut]

    def by_core(t, block):
        return remote(
            source(t, 1 - core, block), level_0.at[t, :, block // 2, block % 2],
            send_0.at[t, block], recv_0.at[t, block], to_core,
        )

    def start_core(t):
        for block in range(4):
            by_core(t, block).start()

    def by_first(t):
        if t % 2 == 0:
            return remote(level_0.at[t, :, 1 - line], level_1.at[t], send.at[1, t], recv.at[1, t], to_line)
        return remote(level_0.at[t, :, :, 1 - near], level_1.at[t], send.at[1, t], recv.at[1, t], to_near)

    def by_second(t):
        if t % 2 == 0:
            return remote(level_1.at[t, :, 1 - near], level_2.at[t], send.at[2, t], recv.at[2, t], to_near)
        return remote(level_1.at[t, :, 1 - line], level_2.at[t], send.at[2, t], recv.at[2, t], to_line)

    def by_x(t):
        return remote(level_2.at[t, 1], level_3.at[t], send.at[0, t], recv.at[0, t], to_x)

    def far_rows(place):
        return pl.ds(pl.multiple_of(place * rows_own, rows_own), rows_own)

    def by_far(t):
        return remote(level_3.at[t, far_rows(1 - far), :], level_4.at[t], send.at[4, t], recv.at[4, t], to_far)

    def join(a, b):
        return (a.astype(F32) + b.astype(F32)).astype(BF16)

    def after_core(t):
        for block in range(4):
            by_core(t, block).wait_recv()
            for g in range(groups):
                i, j = block // 2, block % 2
                level_0[t, g, i, j] = join(level_0[t, g, i, j], source(t, core, block)[g])
        by_first(t).start()

    def after_first(t):
        by_first(t).wait_recv()
        for g in range(groups):
            for i in range(2):
                kept = level_0[t, g, line, i] if t % 2 == 0 else level_0[t, g, i, near]
                level_1[t, g, i] = join(level_1[t, g, i], kept)
        by_second(t).start()

    def after_second(t):
        by_second(t).wait_recv()
        for g in range(groups):
            level_2[t, g] = join(level_2[t, g], level_1[t, g, near if t % 2 == 0 else line])
        by_x(t).start()

    def after_x(t):
        by_x(t).wait_recv()
        level_3[t] = join(level_3[t], level_2[t, 0])
        by_far(t).start()

    def finish(t, out):
        by_far(t).wait_recv()
        out[:, t % 2 * cut : (t % 2 + 1) * cut] = level_3[t, far_rows(far), :].astype(F32) + level_4[t].astype(F32)

    def send_output(b):
        rows = pl.ds(pl.multiple_of(b * length, length), length)
        return remote(out_ref.at[rows, :], out_peer_ref.at[rows, :], send_in.at[1, b], recv_in.at[1, b], to_x)

    def send_input(s):
        rows = pl.ds(pl.multiple_of(s * length, length), length)
        return remote(in_ref.at[rows, :], in_peer_ref.at[rows, :], send_in.at[0, s], recv_in.at[0, s], to_x)

    attn_gain, attn_shift, down_bias, ffn_gain, ffn_shift, out_bias = (
        vec_ref[:, i * model : (i + 1) * model] for i in range(6)
    )

    def attend(s, g, biases):
        rows = pl.ds(pl.multiple_of(s * length, length), length)
        x = x_ref[rows, :]
        mask = seg_c_ref[s] == seg_r_ref[s]
        y = mm(x, w_ref[g])
        query = (0.125 * (y[:, :width] + biases[0:1, :width])).astype(BF16)
        key = y[:, width : 2 * width].astype(BF16)
        value = (y[:, 2 * width :] + biases[0:1, width : 2 * width]).astype(BF16)
        qkv_ref[g, rows, :width] = query
        qkv_ref[g, rows, width : 2 * width] = key
        qkv_ref[g, rows, 2 * width :] = value
        parts = []
        for p in range(pairs):
            at = slice(p * PAIR, (p + 1) * PAIR)
            k = key[:, at]
            both = None
            for h, (q, v) in enumerate(zip(halves(query[:, at]), halves(value[:, at]))):
                scores = jnp.where(mask, mm_t(q, k), -1000000000.0)
                expo = jnp.exp(scores - jnp.max(scores, -1, keepdims=True))
                probs = (expo * (1.0 / jnp.sum(expo, -1, keepdims=True))).astype(BF16)
                p_ref[s, (g * pairs + p) * 2 + h] = probs
                part = mm(probs, v)
                both = part if both is None else both + part
            parts.append(both.astype(BF16))
        ctx = jnp.concatenate(parts, 1)
        ctx_ref[g, rows, :] = ctx
        return mm(ctx, wo_ref[g])

    for copy in raw_copies[: 2 * seqs] + own_copies[:4]:
        copy.wait()

    @pl.loop(0, seqs)
    def _(s):
        rows = pl.ds(pl.multiple_of(s * length, length), length)
        choose(s, 0, x_ref)
        seg_c_ref[s] = segments(s, (length, 1), 0)
        seg_r_ref[s] = segments(s, (1, length), 1)
        acc_ref[rows, :] = x_ref[rows, :].astype(F32) + out_bias + attend(s, 0, bias_ref)
        for kind in range(3):

            @pl.when(s == min(kind, seqs - 1))
            def _():
                first_hop(kind)

    for copy in raw_copies[2 * seqs :]:
        copy.wait()

    @pl.loop(0, seqs)
    def _(s):
        choose(s, 1, cot_ref)

    first_hop(3)
    for kind in range(4):
        second_hop(kind)
    for kind in range(4):
        complete(kind)
    bias_over.wait()

    @pl.loop(0, seqs)
    def _(s):
        rows = pl.ds(pl.multiple_of(s * length, length), length)
        attn = acc_ref[rows, :] + attend(s, 1, bias_2)
        centred = attn - jnp.mean(attn, -1, keepdims=True)
        rstd = lax.rsqrt(jnp.mean(centred * centred, -1, keepdims=True) + EPS)
        xhat = centred * rstd
        xhat_ref[rows, :] = xhat
        rstd_ref[rows, :] = rstd
        low_ref[rows, :] = (xhat * attn_gain + attn_shift).astype(BF16)

        @pl.when(s == 0)
        def _():
            first_hop(4, 0)

        @pl.when(s == 1)
        def _():
            first_hop(5, 0)

        @pl.when(s == 2)
        def _():
            first_hop(4, 1)

    for copy in own_copies[4:]:
        copy.wait()
    store_by_owner(t_low_ref, low_ref[...].T, slice(None), n)

    def expand(c, g, biases):
        at = columns(c)
        bias_at = pl.ds(pl.multiple_of(2 * width + c * step, 128), step)

        @pl.loop(0, tokens // block)
        def _(b):
            rows = pl.ds(pl.multiple_of(b * block, block), block)
            u = mm(low_ref[rows, :], up_ref[g, :, at]) + biases[0:1, bias_at]
            square = u * u
            t = jnp.tanh(GELU_C * (u + 0.044715 * square * u))
            gate = 0.5 * (1.0 + t)
            act = (u * gate).astype(BF16)
            act_ref[g, rows, at] = act
            slope = gate + (0.5 * GELU_C) * u * (1.0 - t * t) * (1.0 + 0.134145 * square)
            slope_ref[g, rows, at] = slope.astype(BF16)
            acc_ref[rows, :] += mm(act, down_ref[g, at, :])

    acc_ref[...] = jnp.zeros_like(acc_ref)

    @pl.loop(0, 3)
    def _(c):
        expand(c, 0, bias_ref)

        @pl.when(c == 0)
        def _():
            second_hop(4, 0)

        @pl.when(c == 1)
        def _():
            second_hop(5, 0)
            first_hop(5, 1)

        @pl.when(c == 2)
        def _():
            second_hop(4, 1)
            first_hop(4, 2)

    @pl.loop(0, 3)
    def _(c):
        complete(4, c)
        complete(5, c)
        expand(c, 1, bias_2)

        @pl.when(c == 0)
        def _():
            first_hop(5, 2)
            second_hop(5, 1)

        @pl.when(c == 1)
        def _():
            second_hop(4, 2)
            second_hop(5, 2)

    small_ref[...] = jnp.zeros_like(small_ref)

    @pl.loop(0, seqs)
    def _(b):
        rows = pl.ds(pl.multiple_of(b * length, length), length)
        resid = xhat_ref[rows, :] * attn_gain + attn_shift + acc_ref[rows, :] + down_bias
        centred = resid - jnp.mean(resid, -1, keepdims=True)
        rstd = lax.rsqrt(jnp.mean(centred * centred, -1, keepdims=True) + EPS)
        xhat = centred * rstd
        out_ref[rows, :] = (xhat * ffn_gain + ffn_shift).astype(BF16)
        cot = cot_ref[rows, :].astype(F32)
        grad = norm_backward(xhat, rstd, ffn_gain, cot)
        acc_ref[rows, :] = grad
        dffn_ref[rows, :] = grad.astype(BF16)
        small_ref[3:4, :] += jnp.sum(grad, 0, keepdims=True)
        small_ref[4:5, :] += jnp.sum(cot * xhat, 0, keepdims=True)
        small_ref[5:6, :] += jnp.sum(cot, 0, keepdims=True)
        send_output(b).start()

    store_by_owner(t_grad_ref, dffn_ref[...].T, slice(None), n)

    def product(left, place, g, at):
        made = [
            mm(left[b * block : (b + 1) * block, :], place[g, :, at]).astype(BF16) for b in range(model // block)
        ]
        for b, value in enumerate(made):
            place[g, b * block : (b + 1) * block, at] = value

    tiny[...] = jnp.zeros_like(tiny)
    for g in range(groups):

        @pl.loop(0, 3)
        def _(c):
            product(t_grad_ref, act_ref, g, columns(c))

    start_core(0)
    start_core(1)
    for g in range(groups):

        @pl.loop(0, 3)
        def _(c):
            at = columns(c)
            total = jnp.zeros((1, step), F32)
            for b in range(tokens // block):
                rows = slice(b * block, (b + 1) * block)
                d_upper = mm_t(dffn_ref[rows, :], down_ref[g, at, :]) * slope_ref[g, rows, at].astype(F32)
                total = total + jnp.sum(d_upper, 0, keepdims=True)
                d_low = d_upper.astype(BF16)
                slope_ref[g, rows, at] = d_low
                acc_ref[rows, :] += mm_t(d_low, up_ref[g, :, at])
            tiny[3 + g, 0:1, at] = total
            product(t_low_ref, slope_ref, g, at)
            if g == 0:

                @pl.when(c == 1)
                def _():
                    after_core(0)
                    after_core(1)

    start_core(2)
    start_core(3)

    @pl.loop(0, seqs)
    def _(b):
        rows = pl.ds(pl.multiple_of(b * length, length), length)
        d_normed = acc_ref[rows, :]
        xhat = xhat_ref[rows, :]
        grad = norm_backward(xhat, rstd_ref[rows, :], attn_gain, d_normed)
        acc_ref[rows, :] = grad
        small_ref[0:1, :] += jnp.sum(grad, 0, keepdims=True)
        small_ref[1:2, :] += jnp.sum(d_normed * xhat, 0, keepdims=True)
        small_ref[2:3, :] += jnp.sum(d_normed, 0, keepdims=True)

    store_by_owner(t_low_ref, x_ref[...].T, slice(None), n)

    @pl.loop(0, seqs)
    def _(s):
        backward_sequence(
            s, lambda v, at: store_by_owner(t_grad_ref, v, at, n),
            acc_ref, w_ref, wo_ref, qkv_ref, p_ref, in_ref, qkv_ref,
        )
        send_input(s).start()

        @pl.when(s == 0)
        def _():
            after_first(0)
            after_first(1)
            after_core(2)
            after_core(3)

        @pl.when(s == 1)
        def _():
            after_second(0)
            after_second(1)

        @pl.when(s == 2)
        def _():
            after_first(2)
            after_first(3)

    tiny_core = remote(tiny.at[0:3], tiny_1, send.at[3, 1], recv.at[3, 1], to_core)
    tiny_line = remote(tiny_1, tiny_2, send.at[3, 2], recv.at[3, 2], to_line)
    tiny_over = remote(tiny_2.at[1:3], tiny_x, send.at[3, 3], recv.at[3, 3], to_x)

    def tiny_rest(k):
        return remote(tiny_x, tiny_z.at[k - 1], send_z.at[k - 1], recv_z.at[k - 1], to_rest(k))

    for g in range(groups):
        column = jnp.sum(qkv_ref[g].astype(F32), 0, keepdims=True)
        tiny[g, 0:1, :width] = column[:, :width]
        tiny[g, 0:1, width : 2 * width] = column[:, 2 * width :]
        tiny[g, 1:2, :] = tiny[3 + g, 0:1, :]
    tiny[2, :, :model] = small_ref[...]
    for kind in range(4):
        sent(kind)
    for c in range(3):
        sent(4, c)
        sent(5, c)
    tiny_core.start()
    for g in range(groups):
        weight_products(g, t_low_ref, t_grad_ref, qkv_ref, ctx_ref, up_ref)
    start_core(4)
    start_core(5)
    tiny_core.wait_recv()
    tiny_1[...] += tiny[0:3]
    tiny_line.start()
    after_core(4)
    after_core(5)
    after_second(2)
    after_second(3)
    tiny_line.wait_recv()
    tiny_2[...] += tiny_1[...]
    tiny_over.start()
    for i, (one, own, other) in enumerate(
        ((send_output, out_ref, out_peer_ref), (send_input, in_ref, in_peer_ref))
    ):

        @pl.loop(0, seqs)
        def _(s):
            one(s).wait_recv()
            put_back(s, i, own, other)
            put_out(s, i).start()

    after_x(0)
    after_x(1)
    after_first(4)
    after_first(5)
    after_x(2)
    after_x(3)
    tiny_over.wait_recv()
    tiny_x[0] += tiny_2[0]
    tiny_x[1] += tiny_2[2]
    for k in range(1, depth):
        tiny_rest(k).start()
    after_second(4)
    after_second(5)
    finish(0, rd_ref)
    finish(1, rd_ref)
    finish(2, ru_ref)
    finish(3, ru_ref)
    total = tiny_x[...]
    for k in range(1, depth):
        tiny_rest(k).wait_recv()
        total = total + tiny_z[k - 1]
    sums_ref[...] = total
    after_x(4)
    after_x(5)
    finish(4, ra_ref)
    finish(5, ra_ref)
    for s in range(seqs):
        send_output(s).wait_send()
        send_input(s).wait_send()
        for i in range(2):
            put_out(s, i).wait()
    for t in range(6):
        for block in range(4):
            by_core(t, block).wait_send()
        by_first(t).wait_send()
        by_second(t).wait_send()
        by_x(t).wait_send()
        by_far(t).wait_send()
    tiny_core.wait_send()
    tiny_line.wait_send()
    tiny_over.wait_send()
    for k in range(1, depth):
        tiny_rest(k).wait_send()


def call(kernel, outs, scratch, flops, *args, scalar=(), far=(), far_out=(), collective=None):
    shapes = [jax.ShapeDtypeStruct(s, d) for s, d in outs]
    moved = sum(a.size * a.dtype.itemsize for a in args) + sum(s.size * s.dtype.itemsize for s in shapes)
    vmem = pl.BlockSpec(memory_space=pltpu.VMEM)
    return pl.pallas_call(
        kernel,
        out_shape=shapes,
        in_specs=[
            pl.BlockSpec(memory_space=pltpu.SMEM if i in scalar else pl.ANY if i in far else pltpu.VMEM)
            for i in range(len(args))
        ],
        out_specs=[pl.BlockSpec(memory_space=pl.ANY) if i in far_out else vmem for i in range(len(shapes))],
        scratch_shapes=[pltpu.VMEM(*s) if isinstance(s, tuple) else s for s in scratch],
        compiler_params=pltpu.CompilerParams(
            vmem_limit_bytes=VMEM_LIMIT, collective_id=collective, has_side_effects=collective is not None
        ),
        cost_estimate=pl.CostEstimate(flops=flops, bytes_accessed=moved, transcendentals=0),
    )(*args)


def factors_of(n):
    found = []
    while n > 4 or (n > 1 and len(found) < 2):
        found.append(2)
        n //= 2
    return found + ([n] if n > 1 else [])


def swap(v):
    return lax.ppermute(v, "mp", [(0, 1), (1, 0)])


def shift_dp(v, n, stride, factor, k):
    def target(d):
        i = (d // stride) % factor
        return d + ((i + k) % factor - i) * stride

    return lax.ppermute(v, "dp", [(d, target(d)) for d in range(n)])


def with_peer(own, n):
    core = lax.axis_index("dp") % 2
    half = own.shape[0] // 2
    mine = swap(lax.dynamic_slice_in_dim(own, core * half, half, 0))
    other = shift_dp(mine, n, 1, 2, 1)
    first = core == 0
    peer = jnp.concatenate([jnp.where(first, mine, other), jnp.where(first, other, mine)], 0)
    return jnp.stack([own, peer])


def reduce_to_owner(grad, n):
    index = lax.axis_index("dp")
    rows = grad.shape[1] // n
    left = grad.reshape(2, n, rows, grad.shape[2])
    stride = 1
    for factor in factors_of(n):
        parts = left.reshape(2, left.shape[1] // factor, factor, rows, left.shape[3])
        i = (index // stride) % factor

        def pick(at):
            return lax.dynamic_index_in_dim(parts, at, 2, keepdims=False)

        total = pick(i).astype(F32)
        for k in range(1, factor):
            total = total + shift_dp(pick((i + k) % factor), n, stride, factor, k).astype(F32)
        left = total.astype(BF16)
        stride *= factor
    left = left.reshape(2, rows, left.shape[3])
    return left[0].astype(F32) + swap(left[1]).astype(F32)


def per_device(
    n, layer_input, doc_lengths, q_weight, q_bias, k_weight, v_weight, v_bias, out_weight, out_bias,
    attn_gain, attn_shift, up_weight, up_bias, down_weight, down_bias, ffn_gain, ffn_shift, cotangent,
):
    rows = doc_lengths.shape[0]
    tokens, model = layer_input.shape
    length = tokens // rows
    part = length // 2
    mine = rows * part
    width = q_weight.shape[1]
    hidden = up_weight.shape[1]
    heads = width // HD
    x_index = lax.axis_index("mp")

    remote = (
        (model // n) % 16 == 0 and n == 16
        and hidden == 2 * model and 4 * width == hidden and hidden % 384 == 0 and rows >= 3 and mine == model
    )
    if remote:
        depth = n // 4
        dma = pltpu.SemaphoreType.DMA
        eighth = model // 8
        vectors = jnp.concatenate(
            [attn_gain, attn_shift, down_bias, ffn_gain, ffn_shift, out_bias, q_bias, v_bias, up_bias]
        ).astype(F32)[None]
        layer_output, input_grad, g_down, g_up, g_attn, sums = call(
            functools.partial(whole_layer, n),
            [((tokens, model), BF16)] * 2
            + [((model // n, hidden), F32)] * 3
            + [((2, 8, hidden), F32)],
            [
                ((mine, model), BF16),
                ((mine, model), BF16),
                ((rows, part, 1), jnp.int32),
                ((rows, 1, part), jnp.int32),
                ((mine, model), BF16),
                ((mine, model), BF16),
                ((mine, model), BF16),
                ((2, model, 3 * width), BF16),
                ((2, width, model), BF16),
                ((2, model, hidden), BF16),
                ((2, hidden, model), BF16),
                ((1, 2 * width + hidden), F32),
                ((2, mine, 3 * width), BF16),
                ((rows, 2 * heads, part, part), BF16),
                ((2, mine, width), BF16),
                ((mine, model), F32),
                ((mine, 1), F32),
                ((mine, model), BF16),
                ((2, model, hidden), BF16),
                ((2, model, hidden), BF16),
                ((mine, model), F32),
                ((model, mine), BF16),
                ((model, mine), BF16),
                ((8, model), F32),
            ]
            + [
                ((6, 2, 2, 2, eighth, model), BF16),
                ((6, 2, 2, eighth, model), BF16),
                ((6, 2, eighth, model), BF16),
                ((6, eighth, model), BF16),
                ((6, model // n, model), BF16),
                ((5, 8, hidden), F32),
                ((3, 8, hidden), F32),
                ((3, 8, hidden), F32),
                ((2, 8, hidden), F32),
                ((depth - 1, 2, 8, hidden), F32),
                dma((5, 6)), dma((5, 6)), dma((6, 4)), dma((6, 4)), dma((depth - 1,)), dma((depth - 1,)), dma((2, rows)), dma((2, rows)),
                dma((4, 10)), dma((4, 10)), dma((6,)), dma((2, 2 * rows)), dma((2, rows)),
            ],
            2 * mine * model * (24 * width + 12 * hidden),
            doc_lengths, layer_input, cotangent, vectors,
            q_weight, k_weight, v_weight, out_weight, up_weight, down_weight,
            scalar=(0,), far=(1, 2, 4, 5, 6, 7, 8, 9), far_out=(0, 1), collective=0,
        )
        small = sums[1, :, :model]
        sums = jnp.concatenate([sums[0, 0, : 2 * width], sums[0, 1]])
    else:
        ends = jnp.cumsum(doc_lengths, axis=-1, dtype=jnp.int32)
        start = jnp.sum(jnp.where(doc_lengths == part, ends - part, 0), -1)
        place = jnp.arange(length, dtype=jnp.int32)
        segment = jnp.sum((place[None, :, None] >= ends[:, None, :]).astype(jnp.int32), -1, dtype=jnp.int32)
        before = place[None, :part] < start[:, None]
        from_high = before != (x_index == 1)

        def take(v):
            v = v.reshape(rows, 2, part, model)
            return jnp.where(from_high[:, :, None], v[:, 1], v[:, 0]).reshape(mine, model)

        def give(own, other):
            own, other = own.reshape(rows, part, model), other.reshape(rows, part, model)
            low = jnp.where(from_high[:, :, None], other, own)
            high = jnp.where(from_high[:, :, None], own, other)
            return jnp.stack([low, high], 1).reshape(tokens, model)

        seg = jnp.where(from_high, segment[:, part:], segment[:, :part])
        x = take(layer_input)
        cot = take(cotangent)
        own_bias = jnp.concatenate([q_bias, v_bias, up_bias])
        w_qkv = with_peer(jnp.concatenate([q_weight, k_weight, v_weight], 1), n)
        w_out = with_peer(out_weight, n)
        w_up = with_peer(up_weight, n)
        w_down = with_peer(down_weight, n)
        bias = jnp.stack([own_bias, swap(own_bias)]).astype(F32)[:, None, :]
        b_qkv = jnp.concatenate([bias[..., :width], jnp.zeros_like(bias[..., :width]), bias[..., width : 2 * width]], -1)
        b_up = bias[..., 2 * width :]
        vectors = jnp.stack([attn_gain, attn_shift, down_bias, ffn_gain, ffn_shift]).astype(F32)

        qkv, probs, ctx, xhat, rstd, low = call(
            attention_forward,
            [
                ((2, mine, 3 * width), BF16),
                ((rows, 2 * heads, part, part), BF16),
                ((2, mine, width), BF16),
                ((mine, model), F32),
                ((mine, 1), F32),
                ((mine, model), BF16),
            ],
            [],
            2 * mine * model * 8 * width,
            x, w_qkv, b_qkv, w_out, seg[:, :, None], seg[:, None, :],
            out_bias.astype(F32)[None], vectors[0:1], vectors[1:2],
        )
        output, g_down, g_up, d_resid, small, up_bias_grad = call(
            feed_forward,
            [
                ((mine, model), BF16),
                ((2, model, hidden), BF16),
                ((2, model, hidden), BF16),
                ((mine, model), F32),
                ((8, model), F32),
                ((2, 1, hidden), F32),
            ],
            [
                ((2, mine, hidden), BF16),
                ((2, mine, hidden), BF16),
                ((mine, model), F32),
                ((mine, model), BF16),
                ((model, mine), BF16),
                ((model, mine), BF16),
            ],
            2 * mine * model * 2 * hidden * 6,
            low, xhat, rstd, w_up, b_up, w_down, vectors, cot,
        )
        scratch = [((2, mine, 3 * width), BF16), ((model, mine), BF16), ((model, mine), BF16)]
        flops = 2 * mine * model * 16 * width
        output_peer = swap(output)
        grad_in, g_attn, bias_grad = call(
            attention_backward_plain,
            [((mine, model), BF16), ((2, model, 4 * width), BF16), ((2, 1, 3 * width), F32)],
            scratch, flops, x, d_resid, w_qkv, w_out, qkv, probs, ctx,
        )
        grad_in_peer = swap(grad_in)
        g_down, g_up, g_attn = (reduce_to_owner(v, n) for v in (g_down, g_up, g_attn))
        sums = jnp.concatenate([bias_grad[:, 0, :width], bias_grad[:, 0, 2 * width :], up_bias_grad[:, 0]], -1)
        sums = jnp.where(x_index == 0, sums, sums[::-1])
        sums, small = lax.psum((sums, small), ("dp", "mp"))
        sums = lax.dynamic_index_in_dim(sums, x_index, 0, keepdims=False)
        layer_output = give(output, output_peer)
        input_grad = give(grad_in, grad_in_peer)
    down_weight_grad = g_down.T
    up_weight_grad = g_up
    return (
        layer_output,
        input_grad,
        g_attn[:, :width],
        sums[:width],
        g_attn[:, width : 2 * width],
        g_attn[:, 2 * width : 3 * width],
        sums[width : 2 * width],
        g_attn[:, 3 * width :].T,
        small[0],
        small[1],
        small[2],
        up_weight_grad,
        sums[2 * width :],
        down_weight_grad,
        small[3],
        small[4],
        small[5],
    )


def solution(mesh):
    in_specs = (
        P("dp", None), P("dp", None), P(None, "mp"), P("mp"), P(None, "mp"), P(None, "mp"), P("mp"),
        P("mp", None), P(), P(), P(), P(None, "mp"), P("mp"), P("mp", None), P(), P(), P(), P("dp", None),
    )
    out_specs = (
        P("dp", None), P("dp", None), P("dp", "mp"), P("mp"), P("dp", "mp"), P("dp", "mp"), P("mp"),
        P("mp", "dp"), P(), P(), P(), P("dp", "mp"), P("mp"), P("mp", "dp"), P(), P(), P(),
    )
    return jax.shard_map(
        functools.partial(per_device, mesh.shape["dp"]),
        mesh=mesh, in_specs=in_specs, out_specs=out_specs, check_vma=False,
    )
```

```python
import functools

import jax
import jax.numpy as jnp
from jax import lax
from jax.experimental import pallas as pl
from jax.experimental.pallas import tpu as pltpu
from jax.sharding import PartitionSpec as P

HD = 64
PAIR = 2 * HD
EPS = 1e-12
GELU_C = 0.7978845608028654
F32 = jnp.float32
BF16 = jnp.bfloat16
CHUNK = 512
VMEM_LIMIT = 67043328
MESH = pl.DeviceIdType.MESH


def mm(a, b):
    return jnp.dot(a, b, preferred_element_type=F32)


def mm_t(a, b):
    return lax.dot_general(a, b, (((1,), (1,)), ((), ())), preferred_element_type=F32)


def t_mm(a, b):
    return lax.dot_general(a, b, (((0,), (0,)), ((), ())), preferred_element_type=F32)


def halves(v):
    lane = lax.broadcasted_iota(jnp.int32, v.shape, 1)
    zero = jnp.zeros_like(v)
    return jnp.where(lane < HD, v, zero), jnp.where(lane < HD, zero, v)


def attention_forward(
    x_ref, w_ref, b_ref, wo_ref, seg_c_ref, seg_r_ref, bo_ref, gain_ref, shift_ref,
    qkv_ref, p_ref, ctx_ref, xhat_ref, rstd_ref, low_ref,
):
    seqs, length = seg_c_ref.shape[0], seg_c_ref.shape[1]
    groups, width = wo_ref.shape[0], wo_ref.shape[1]
    pairs = width // PAIR

    @pl.loop(0, seqs)
    def _(s):
        rows = pl.ds(pl.multiple_of(s * length, length), length)
        x = x_ref[rows, :]
        mask = seg_c_ref[s] == seg_r_ref[s]
        attn = x.astype(F32) + bo_ref[...]
        for g in range(groups):
            y = mm(x, w_ref[g]) + b_ref[g]
            query = (0.125 * y[:, :width]).astype(BF16)
            key = y[:, width : 2 * width].astype(BF16)
            value = y[:, 2 * width :].astype(BF16)
            qkv_ref[g, rows, :width] = query
            qkv_ref[g, rows, width : 2 * width] = key
            qkv_ref[g, rows, 2 * width :] = value
            parts = []
            for p in range(pairs):
                at = slice(p * PAIR, (p + 1) * PAIR)
                k = key[:, at]
                both = None
                for h, (q, v) in enumerate(zip(halves(query[:, at]), halves(value[:, at]))):
                    scores = jnp.where(mask, mm_t(q, k), -1000000000.0)
                    expo = jnp.exp(scores - jnp.max(scores, -1, keepdims=True))
                    probs = (expo * (1.0 / jnp.sum(expo, -1, keepdims=True))).astype(BF16)
                    p_ref[s, (g * pairs + p) * 2 + h] = probs
                    part = mm(probs, v)
                    both = part if both is None else both + part
                parts.append(both.astype(BF16))
            ctx = jnp.concatenate(parts, 1)
            ctx_ref[g, rows, :] = ctx
            attn = attn + mm(ctx, wo_ref[g])
        mean = jnp.mean(attn, -1, keepdims=True)
        centred = attn - mean
        rstd = lax.rsqrt(jnp.mean(centred * centred, -1, keepdims=True) + EPS)
        xhat = centred * rstd
        xhat_ref[rows, :] = xhat
        rstd_ref[rows, :] = rstd
        low_ref[rows, :] = (xhat * gain_ref[...] + shift_ref[...]).astype(BF16)


def norm_backward(xhat, rstd, gain, grad):
    scaled = grad * gain
    return rstd * (
        scaled
        - jnp.mean(scaled, -1, keepdims=True)
        - xhat * jnp.mean(scaled * xhat, -1, keepdims=True)
    )


def store_by_owner(dst, value, at, n):
    rows = value.shape[0] // n
    for d in range(n):
        place = d % 2 * 8 + d // 2 % 2 * 4 + d // 4 % 2 * 2 + d // 8
        dst[place * rows : (place + 1) * rows, at] = value[d * rows : (d + 1) * rows, :]


def feed_forward(
    low_ref, xhat_ref, rstd_ref, up_ref, ub_ref, down_ref, vec_ref, cot_ref,
    out_ref, gd_ref, gu_ref, d_resid_ref, small_ref, ubg_ref,
    act_ref, slope_ref, acc_ref, dffn_ref, dffn_t_ref, low_t_ref,
):
    tokens, width = low_ref.shape
    groups, hidden = up_ref.shape[0], up_ref.shape[2]
    step = min(CHUNK, hidden)
    per = hidden // step
    block = 256
    low_t_ref[...] = low_ref[...].T
    acc_ref[...] = jnp.zeros_like(acc_ref)

    @pl.loop(0, groups * per)
    def _(i):
        g = i // per
        at = pl.ds(pl.multiple_of((i % per) * step, step), step)

        @pl.loop(0, tokens // block)
        def _(b):
            rows = pl.ds(pl.multiple_of(b * block, block), block)
            u = mm(low_ref[rows, :], up_ref[g, :, at]) + ub_ref[g, :, at]
            square = u * u
            t = jnp.tanh(GELU_C * (u + 0.044715 * square * u))
            half = 0.5 * (1.0 + t)
            act = (u * half).astype(BF16)
            act_ref[g, rows, at] = act
            slope = half + (0.5 * GELU_C) * u * (1.0 - t * t) * (1.0 + 0.134145 * square)
            slope_ref[g, rows, at] = slope.astype(BF16)
            acc_ref[rows, :] += mm(act, down_ref[g, at, :])

    small_ref[...] = jnp.zeros_like(small_ref)
    attn_gain, attn_shift = vec_ref[0:1, :], vec_ref[1:2, :]
    down_bias = vec_ref[2:3, :]
    ffn_gain, ffn_shift = vec_ref[3:4, :], vec_ref[4:5, :]

    @pl.loop(0, tokens // block)
    def _(b):
        rows = pl.ds(pl.multiple_of(b * block, block), block)
        resid = xhat_ref[rows, :] * attn_gain + attn_shift + acc_ref[rows, :] + down_bias
        centred = resid - jnp.mean(resid, -1, keepdims=True)
        rstd = lax.rsqrt(jnp.mean(centred * centred, -1, keepdims=True) + EPS)
        xhat = centred * rstd
        out_ref[rows, :] = (xhat * ffn_gain + ffn_shift).astype(BF16)
        cot = cot_ref[rows, :].astype(F32)
        grad = norm_backward(xhat, rstd, ffn_gain, cot)
        acc_ref[rows, :] = grad
        dffn_ref[rows, :] = grad.astype(BF16)
        small_ref[3:4, :] += jnp.sum(grad, 0, keepdims=True)
        small_ref[4:5, :] += jnp.sum(cot * xhat, 0, keepdims=True)
        small_ref[5:6, :] += jnp.sum(cot, 0, keepdims=True)

    dffn_t_ref[...] = dffn_ref[...].T

    @pl.loop(0, groups * per)
    def _(i):
        g = i // per
        at = pl.ds(pl.multiple_of((i % per) * step, step), step)
        total = jnp.zeros((1, step), F32)
        for b in range(tokens // block):
            rows = slice(b * block, (b + 1) * block)
            d_upper = mm_t(dffn_ref[rows, :], down_ref[g, at, :]) * slope_ref[g, rows, at].astype(F32)
            total = total + jnp.sum(d_upper, 0, keepdims=True)
            d_low = d_upper.astype(BF16)
            slope_ref[g, rows, at] = d_low
            acc_ref[rows, :] += mm_t(d_low, up_ref[g, :, at])
        ubg_ref[g, :, at] = total
        for b in range(width // block):
            rows = slice(b * block, (b + 1) * block)
            gd_ref[g, rows, at] = mm(dffn_t_ref[rows, :], act_ref[g, :, at]).astype(BF16)
            gu_ref[g, rows, at] = mm(low_t_ref[rows, :], slope_ref[g, :, at]).astype(BF16)

    @pl.loop(0, tokens // block)
    def _(b):
        rows = pl.ds(pl.multiple_of(b * block, block), block)
        d_normed = acc_ref[rows, :]
        xhat = xhat_ref[rows, :]
        grad = norm_backward(xhat, rstd_ref[rows, :], attn_gain, d_normed)
        d_resid_ref[rows, :] = grad
        small_ref[0:1, :] += jnp.sum(grad, 0, keepdims=True)
        small_ref[1:2, :] += jnp.sum(d_normed * xhat, 0, keepdims=True)
        small_ref[2:3, :] += jnp.sum(d_normed, 0, keepdims=True)


def backward_sequence(s, put, d_resid_ref, w_ref, wo_ref, qkv_ref, p_ref, in_ref, dq_ref):
    length, groups, width = p_ref.shape[2], wo_ref.shape[0], wo_ref.shape[1]
    pairs = width // PAIR
    rows = pl.ds(pl.multiple_of(s * length, length), length)
    d_resid = d_resid_ref[rows, :]
    d_attn = d_resid.astype(BF16)
    put(d_attn.T, rows)
    total = d_resid
    for g in range(groups):
        d_ctx = mm_t(d_attn, wo_ref[g]).astype(BF16)
        for p in range(pairs):
            at = slice(p * PAIR, (p + 1) * PAIR)
            q_at, k_at, v_at = (slice(o * width + p * PAIR, o * width + (p + 1) * PAIR) for o in range(3))
            value = qkv_ref[g, rows, v_at]
            q_pair = halves(qkv_ref[g, rows, q_at])
            k_pair = halves(qkv_ref[g, rows, k_at])
            c_pair = halves(d_ctx[:, at])
            dq = dk = dv = None
            for h in range(2):
                low = p_ref[s, (g * pairs + p) * 2 + h]
                probs = low.astype(F32)
                d_probs = mm_t(c_pair[h], value)
                inner = jnp.sum(probs * d_probs, -1, keepdims=True)
                d_scores = (probs * (d_probs - inner)).astype(BF16)
                dv_h = t_mm(low, c_pair[h])
                dq_h = mm(d_scores, k_pair[h])
                dk_h = t_mm(d_scores, q_pair[h])
                dq = dq_h if dq is None else dq + dq_h
                dk = dk_h if dk is None else dk + dk_h
                dv = dv_h if dv is None else dv + dv_h
            dq_ref[g, rows, q_at] = (0.125 * dq).astype(BF16)
            dq_ref[g, rows, k_at] = dk.astype(BF16)
            dq_ref[g, rows, v_at] = dv.astype(BF16)
        total = total + mm_t(dq_ref[g, rows, :], w_ref[g])
    in_ref[rows, :] = total.astype(BF16)


def weight_products(g, x_t_ref, dattn_t_ref, dq_ref, ctx_ref, ga_ref):
    block, wide = 256, dq_ref.shape[2]

    @pl.loop(0, x_t_ref.shape[0] // block)
    def _(b):
        rows = pl.ds(pl.multiple_of(b * block, block), block)
        ga_ref[g, rows, :wide] = mm(x_t_ref[rows, :], dq_ref[g]).astype(BF16)
        ga_ref[g, rows, wide:] = mm(dattn_t_ref[rows, :], ctx_ref[g]).astype(BF16)


def attention_backward_plain(
    x_ref, d_resid_ref, w_ref, wo_ref, qkv_ref, p_ref, ctx_ref,
    in_ref, ga_ref, bg_ref,
    dq_ref, dattn_t_ref, x_t_ref,
):
    groups, width = wo_ref.shape[0], wo_ref.shape[1]
    x_t_ref[...] = x_ref[...].T

    def put(v, at):
        dattn_t_ref[:, at] = v

    @pl.loop(0, p_ref.shape[0])
    def _(s):
        backward_sequence(s, put, d_resid_ref, w_ref, wo_ref, qkv_ref, p_ref, in_ref, dq_ref)

    for g in range(groups):
        bg_ref[g] = jnp.sum(dq_ref[g].astype(F32), 0, keepdims=True)
        weight_products(g, x_t_ref, dattn_t_ref, dq_ref, ctx_ref, ga_ref)


def whole_layer(
    n, doc_ref, x_hbm, cot_hbm, wq_hbm, wk_hbm, wv_hbm, wo_hbm, up_hbm, down_hbm,
    v_0, v_1, v_2, v_3, v_4, v_5, v_6, v_7, v_8,
    output_hbm, input_hbm, rd_ref, ru_ref, ra_ref, sums_ref,
    x_ref, cot_ref, vec_ref, seg_c_ref, seg_r_ref, out_ref, out_peer_ref, in_peer_ref,
    w_ref, wo_ref, up_ref, down_ref, bias_2, qkv_ref, p_ref, ctx_ref, xhat_ref, rstd_ref, low_ref, act_ref, slope_ref,
    acc_ref, t_low_ref, t_grad_ref, small_ref, *rest_refs,
):
    in_ref, dffn_ref = cot_ref, low_ref
    level_0, level_1, level_2, level_3, level_4, ubg_ref = rest_refs[:6]
    tiny, tiny_1, tiny_2, tiny_x, tiny_n, tiny_f = rest_refs[6:12]
    send, recv, send_0, recv_0, send_in, recv_in, g_send, g_recv, g_local, raw, done = rest_refs[12:]
    seqs, length = seg_c_ref.shape[0], seg_c_ref.shape[1]
    groups, width, model = wo_ref.shape
    hidden = up_ref.shape[2]
    pairs = width // PAIR
    tokens = seqs * length
    step = hidden // 3
    block = 256
    rows_own = model // n
    depth = n // 4
    index = lax.axis_index("dp")
    x_index = lax.axis_index("mp")
    core, line, rest = index % 2, index // 2 % 2, index // 4
    to_core = {"dp": index + 1 - 2 * core}
    to_line = {"dp": index + 2 - 4 * line}
    to_x = {"mp": 1 - x_index}

    near, far = rest % 2, rest // 2
    to_near = {"dp": index + 4 - 8 * near}
    to_far = {"dp": index + 8 - 16 * far}

    def to_rest(k):
        return {"dp": (rest + k) % depth * 4 + index % 4}

    barrier = pltpu.get_barrier_semaphore()
    peers = [to_core, to_line, to_x] + [to_rest(k) for k in range(1, depth)]
    for peer in peers:
        pl.semaphore_signal(barrier, inc=1, device_id=peer, device_id_type=MESH)
    pl.semaphore_wait(barrier, len(peers))

    def remote(src, dst, s, r, device):
        return pltpu.make_async_remote_copy(
            src_ref=src, dst_ref=dst, send_sem=s, recv_sem=r, device_id=device, device_id_type=MESH
        )

    def columns(c):
        return pl.ds(pl.multiple_of(c * step, step), step)

    def ends_of(kind, c, piece):
        if kind < 3:
            size = model // 4
            rows = pl.ds(pl.multiple_of(piece * size, size), size)
            return (wq_hbm, wk_hbm, wv_hbm)[kind].at[rows, :], w_ref.at[1, rows, kind * width : (kind + 1) * width]
        if kind == 3:
            size = width // 4
            rows = pl.ds(pl.multiple_of(piece * size, size), size)
            return wo_hbm.at[rows, :], wo_ref.at[1, rows, :]
        if kind == 4:
            size = model // 4
            rows = pl.ds(pl.multiple_of(piece * size, size), size)
            return up_hbm.at[rows, columns(c)], up_ref.at[1, rows, columns(c)]
        size = step // 4
        rows = pl.ds(pl.multiple_of(c * step + piece * size, size), size)
        return down_hbm.at[rows, :], down_ref.at[1, rows, :]

    def slot(kind, c):
        return kind if kind < 4 else (4 + c if kind == 4 else 7 + c)

    def over_x(kind, c=0):
        src, dst = ends_of(kind, c, 2 * line + core)
        i = slot(kind, c)
        return remote(src, dst, g_send.at[0, i], g_recv.at[0, i], to_x)

    def pass_on(kind, c, hop):
        at = ends_of(kind, c, 2 * (1 - line) + core if hop == 3 else 2 * line + core)[1]
        i = slot(kind, c)
        return remote(at, at, g_send.at[hop, i], g_recv.at[hop, i], to_line if hop == 2 else to_core)

    def first_hop(kind, c=0):
        over_x(kind, c).wait_recv()
        pass_on(kind, c, 2).start()
        pass_on(kind, c, 1).start()

    def second_hop(kind, c=0):
        pass_on(kind, c, 2).wait_recv()
        pass_on(kind, c, 3).start()

    def complete(kind, c=0):
        pass_on(kind, c, 1).wait_recv()
        pass_on(kind, c, 3).wait_recv()

    def sent(kind, c=0):
        over_x(kind, c).wait_send()
        for hop in (1, 2, 3):
            pass_on(kind, c, hop).wait_send()

    place = 0
    for v in (v_0, v_1, v_2, v_3, v_4, v_5, v_6, v_7, v_8):
        vec_ref[0:1, place : place + v.shape[0]] = v[...].astype(F32).reshape(1, v.shape[0])
        place += v.shape[0]
    bias_ref = vec_ref.at[:, 6 * model :]
    bias_over = remote(bias_ref, bias_2, send.at[3, 0], recv.at[3, 0], to_x)
    bias_over.start()
    for kind in range(4):
        over_x(kind).start()
    for c in range(3):
        over_x(4, c).start()
        over_x(5, c).start()
    own_copies = [
        pltpu.make_async_copy(src, dst, g_local.at[i])
        for i, (src, dst) in enumerate(
            [(w, w_ref.at[0, :, o * width : (o + 1) * width]) for o, w in enumerate((wq_hbm, wk_hbm, wv_hbm))]
            + [(wo_hbm, wo_ref.at[0]), (up_hbm, up_ref.at[0]), (down_hbm, down_ref.at[0])]
        )
    ]
    raw_copies = [
        pltpu.make_async_copy(
            source.at[(2 * r + h) * length : (2 * r + h + 1) * length, :],
            act_ref.at[i, r * length : (r + 1) * length, h * model : (h + 1) * model],
            raw.at[i, 2 * r + h],
        )
        for i, source in enumerate((x_hbm, cot_hbm))
        for r in range(seqs)
        for h in range(2)
    ]
    for copy in raw_copies[: 2 * seqs] + own_copies + raw_copies[2 * seqs :]:
        copy.start()

    def starts(s):
        ends, end, start = [], 0, 0
        for d in range(doc_ref.shape[1]):
            size = doc_ref[s, d]
            end = end + size
            ends.append(end)
            start = start + jnp.where(size == length, end - length, 0)
        return start, ends

    def from_high(s, shape, dim):
        place = lax.broadcasted_iota(jnp.int32, shape, dim)
        return (place < starts(s)[0]).astype(jnp.int32) != x_index

    def segments(s, shape, dim):
        place = lax.broadcasted_iota(jnp.int32, shape, dim)
        place = jnp.where(from_high(s, shape, dim), place + length, place)
        segment = jnp.zeros(shape, jnp.int32)
        for end in starts(s)[1]:
            segment = segment + (place >= end).astype(jnp.int32)
        return segment

    def choose(s, i, dst):
        rows = pl.ds(pl.multiple_of(s * length, length), length)
        high = from_high(s, (length, model), 0)
        first, second = act_ref[i, rows, :model].astype(F32), act_ref[i, rows, model:].astype(F32)
        dst[rows, :] = jnp.where(high, second, first).astype(BF16)

    def put_back(s, i, own, other):
        rows = pl.ds(pl.multiple_of(s * length, length), length)
        high = from_high(s, (length, model), 0)
        a, b = own[rows, :].astype(F32), other[rows, :].astype(F32)
        down_ref[i, pl.ds(pl.multiple_of(2 * s * length, length), length), :] = jnp.where(high, b, a).astype(BF16)
        down_ref[i, pl.ds(pl.multiple_of((2 * s + 1) * length, length), length), :] = jnp.where(high, a, b).astype(BF16)

    def put_out(s, i):
        rows = pl.ds(pl.multiple_of(2 * s * length, length), 2 * length)
        return pltpu.make_async_copy(down_ref.at[i, rows, :], (output_hbm, input_hbm)[i].at[rows, :], done.at[i, s])

    cut = hidden // 2
    size = model // 8
    sources = (act_ref, slope_ref, up_ref)

    def source(t, where, block):
        rows = pl.ds(pl.multiple_of((where * 4 + block) * size, size), size)
        return sources[t // 2].at[:, rows, t % 2 * cut : (t % 2 + 1) * cut]

    def by_core(t, block):
        return remote(
            source(t, 1 - core, block), level_0.at[t, :, block // 2, block % 2],
            send_0.at[t, block], recv_0.at[t, block], to_core,
        )

    def start_core(t):
        for block in range(4):
            by_core(t, block).start()

    def by_first(t):
        if t % 2 == 0:
            return remote(level_0.at[t, :, 1 - line], level_1.at[t], send.at[1, t], recv.at[1, t], to_line)
        return remote(level_0.at[t, :, :, 1 - near], level_1.at[t], send.at[1, t], recv.at[1, t], to_near)

    def by_second(t):
        if t % 2 == 0:
            return remote(level_1.at[t, :, 1 - near], level_2.at[t], send.at[2, t], recv.at[2, t], to_near)
        return remote(level_1.at[t, :, 1 - line], level_2.at[t], send.at[2, t], recv.at[2, t], to_line)

    def by_x(t):
        return remote(level_2.at[t, 1], level_3.at[t], send.at[0, t], recv.at[0, t], to_x)

    def far_rows(place):
        return pl.ds(pl.multiple_of(place * rows_own, rows_own), rows_own)

    def by_far(t):
        return remote(level_3.at[t, far_rows(1 - far), :], level_4.at[t], send.at[4, t], recv.at[4, t], to_far)

    def join(a, b):
        return (a.astype(F32) + b.astype(F32)).astype(BF16)

    def after_core(t):
        for block in range(4):
            by_core(t, block).wait_recv()
            for g in range(groups):
                i, j = block // 2, block % 2
                level_0[t, g, i, j] = join(level_0[t, g, i, j], source(t, core, block)[g])
        by_first(t).start()

    def after_first(t):
        by_first(t).wait_recv()
        for g in range(groups):
            for i in range(2):
                kept = level_0[t, g, line, i] if t % 2 == 0 else level_0[t, g, i, near]
                level_1[t, g, i] = join(level_1[t, g, i], kept)
        by_second(t).start()

    def after_second(t):
        by_second(t).wait_recv()
        for g in range(groups):
            level_2[t, g] = join(level_2[t, g], level_1[t, g, near if t % 2 == 0 else line])
        by_x(t).start()

    def after_x(t):
        by_x(t).wait_recv()
        level_3[t] = join(level_3[t], level_2[t, 0])
        by_far(t).start()

    def finish(t, out):
        by_far(t).wait_recv()
        out[:, t % 2 * cut : (t % 2 + 1) * cut] = level_3[t, far_rows(far), :].astype(F32) + level_4[t].astype(F32)

    def send_output(b):
        rows = pl.ds(pl.multiple_of(b * length, length), length)
        return remote(out_ref.at[rows, :], out_peer_ref.at[rows, :], send_in.at[1, b], recv_in.at[1, b], to_x)

    def send_input(s):
        rows = pl.ds(pl.multiple_of(s * length, length), length)
        return remote(in_ref.at[rows, :], in_peer_ref.at[rows, :], send_in.at[0, s], recv_in.at[0, s], to_x)

    attn_gain, attn_shift, down_bias, ffn_gain, ffn_shift, out_bias = (
        vec_ref[:, i * model : (i + 1) * model] for i in range(6)
    )

    def attend(s, g, biases):
        rows = pl.ds(pl.multiple_of(s * length, length), length)
        x = x_ref[rows, :]
        mask = seg_c_ref[s] == seg_r_ref[s]
        y = mm(x, w_ref[g])
        query = (0.125 * (y[:, :width] + biases[0:1, :width])).astype(BF16)
        key = y[:, width : 2 * width].astype(BF16)
        value = (y[:, 2 * width :] + biases[0:1, width : 2 * width]).astype(BF16)
        qkv_ref[g, rows, :width] = query
        qkv_ref[g, rows, width : 2 * width] = key
        qkv_ref[g, rows, 2 * width :] = value
        parts = []
        for p in range(pairs):
            at = slice(p * PAIR, (p + 1) * PAIR)
            k = key[:, at]
            both = None
            for h, (q, v) in enumerate(zip(halves(query[:, at]), halves(value[:, at]))):
                scores = jnp.where(mask, mm_t(q, k), -1000000000.0)
                expo = jnp.exp(scores - jnp.max(scores, -1, keepdims=True))
                probs = (expo * (1.0 / jnp.sum(expo, -1, keepdims=True))).astype(BF16)
                p_ref[s, (g * pairs + p) * 2 + h] = probs
                part = mm(probs, v)
                both = part if both is None else both + part
            parts.append(both.astype(BF16))
        ctx = jnp.concatenate(parts, 1)
        ctx_ref[g, rows, :] = ctx
        return mm(ctx, wo_ref[g])

    for copy in raw_copies[: 2 * seqs] + own_copies[:4]:
        copy.wait()

    @pl.loop(0, seqs)
    def _(s):
        rows = pl.ds(pl.multiple_of(s * length, length), length)
        choose(s, 0, x_ref)
        seg_c_ref[s] = segments(s, (length, 1), 0)
        seg_r_ref[s] = segments(s, (1, length), 1)
        acc_ref[rows, :] = x_ref[rows, :].astype(F32) + out_bias + attend(s, 0, bias_ref)
        for kind in range(3):

            @pl.when(s == min(kind, seqs - 1))
            def _():
                first_hop(kind)

    for copy in raw_copies[2 * seqs :]:
        copy.wait()

    @pl.loop(0, seqs)
    def _(s):
        choose(s, 1, cot_ref)

    first_hop(3)
    for kind in range(4):
        second_hop(kind)
    for kind in range(4):
        complete(kind)
    bias_over.wait()

    @pl.loop(0, seqs)
    def _(s):
        rows = pl.ds(pl.multiple_of(s * length, length), length)
        attn = acc_ref[rows, :] + attend(s, 1, bias_2)
        centred = attn - jnp.mean(attn, -1, keepdims=True)
        rstd = lax.rsqrt(jnp.mean(centred * centred, -1, keepdims=True) + EPS)
        xhat = centred * rstd
        xhat_ref[rows, :] = xhat
        rstd_ref[rows, :] = rstd
        low_ref[rows, :] = (xhat * attn_gain + attn_shift).astype(BF16)

        @pl.when(s == 0)
        def _():
            first_hop(4, 0)

        @pl.when(s == 1)
        def _():
            first_hop(5, 0)

        @pl.when(s == 2)
        def _():
            first_hop(4, 1)

    for copy in own_copies[4:]:
        copy.wait()
    store_by_owner(t_low_ref, low_ref[...].T, slice(None), n)

    def expand(c, g, biases):
        at = columns(c)
        bias_at = pl.ds(pl.multiple_of(2 * width + c * step, 128), step)

        @pl.loop(0, tokens // block)
        def _(b):
            rows = pl.ds(pl.multiple_of(b * block, block), block)
            u = mm(low_ref[rows, :], up_ref[g, :, at]) + biases[0:1, bias_at]
            square = u * u
            t = jnp.tanh(GELU_C * (u + 0.044715 * square * u))
            gate = 0.5 * (1.0 + t)
            act = (u * gate).astype(BF16)
            act_ref[g, rows, at] = act
            slope = gate + (0.5 * GELU_C) * u * (1.0 - t * t) * (1.0 + 0.134145 * square)
            slope_ref[g, rows, at] = slope.astype(BF16)
            acc_ref[rows, :] += mm(act, down_ref[g, at, :])

    acc_ref[...] = jnp.zeros_like(acc_ref)

    @pl.loop(0, 3)
    def _(c):
        expand(c, 0, bias_ref)

        @pl.when(c == 0)
        def _():
            second_hop(4, 0)

        @pl.when(c == 1)
        def _():
            second_hop(5, 0)
            first_hop(5, 1)

        @pl.when(c == 2)
        def _():
            second_hop(4, 1)
            first_hop(4, 2)

    @pl.loop(0, 3)
    def _(c):
        complete(4, c)
        complete(5, c)
        expand(c, 1, bias_2)

        @pl.when(c == 0)
        def _():
            first_hop(5, 2)
            second_hop(5, 1)

        @pl.when(c == 1)
        def _():
            second_hop(4, 2)
            second_hop(5, 2)

    small_ref[...] = jnp.zeros_like(small_ref)

    @pl.loop(0, seqs)
    def _(b):
        rows = pl.ds(pl.multiple_of(b * length, length), length)
        resid = xhat_ref[rows, :] * attn_gain + attn_shift + acc_ref[rows, :] + down_bias
        centred = resid - jnp.mean(resid, -1, keepdims=True)
        rstd = lax.rsqrt(jnp.mean(centred * centred, -1, keepdims=True) + EPS)
        xhat = centred * rstd
        out_ref[rows, :] = (xhat * ffn_gain + ffn_shift).astype(BF16)
        cot = cot_ref[rows, :].astype(F32)
        grad = norm_backward(xhat, rstd, ffn_gain, cot)
        acc_ref[rows, :] = grad
        dffn_ref[rows, :] = grad.astype(BF16)
        small_ref[3:4, :] += jnp.sum(grad, 0, keepdims=True)
        small_ref[4:5, :] += jnp.sum(cot * xhat, 0, keepdims=True)
        small_ref[5:6, :] += jnp.sum(cot, 0, keepdims=True)
        send_output(b).start()

    store_by_owner(t_grad_ref, dffn_ref[...].T, slice(None), n)

    def product(left, place, g, at):
        made = [
            mm(left[b * block : (b + 1) * block, :], place[g, :, at]).astype(BF16) for b in range(model // block)
        ]
        for b, value in enumerate(made):
            place[g, b * block : (b + 1) * block, at] = value

    tiny[...] = jnp.zeros_like(tiny)
    for g in range(groups):

        @pl.loop(0, 3)
        def _(c):
            product(t_grad_ref, act_ref, g, columns(c))

    start_core(0)
    start_core(1)
    for g in range(groups):

        @pl.loop(0, 3)
        def _(c):
            at = columns(c)
            total = jnp.zeros((1, step), F32)
            for b in range(tokens // block):
                rows = slice(b * block, (b + 1) * block)
                d_upper = mm_t(dffn_ref[rows, :], down_ref[g, at, :]) * slope_ref[g, rows, at].astype(F32)
                total = total + jnp.sum(d_upper, 0, keepdims=True)
                d_low = d_upper.astype(BF16)
                slope_ref[g, rows, at] = d_low
                acc_ref[rows, :] += mm_t(d_low, up_ref[g, :, at])
            ubg_ref[g, 0:1, at] = total
            product(t_low_ref, slope_ref, g, at)
            if g == 0:

                @pl.when(c == 1)
                def _():
                    after_core(0)
                    after_core(1)

    start_core(2)
    start_core(3)

    @pl.loop(0, seqs)
    def _(b):
        rows = pl.ds(pl.multiple_of(b * length, length), length)
        d_normed = acc_ref[rows, :]
        xhat = xhat_ref[rows, :]
        grad = norm_backward(xhat, rstd_ref[rows, :], attn_gain, d_normed)
        acc_ref[rows, :] = grad
        small_ref[0:1, :] += jnp.sum(grad, 0, keepdims=True)
        small_ref[1:2, :] += jnp.sum(d_normed * xhat, 0, keepdims=True)
        small_ref[2:3, :] += jnp.sum(d_normed, 0, keepdims=True)

    store_by_owner(t_low_ref, x_ref[...].T, slice(None), n)

    @pl.loop(0, seqs)
    def _(s):
        backward_sequence(
            s, lambda v, at: store_by_owner(t_grad_ref, v, at, n),
            acc_ref, w_ref, wo_ref, qkv_ref, p_ref, in_ref, qkv_ref,
        )
        send_input(s).start()

        @pl.when(s == 0)
        def _():
            after_first(0)
            after_first(1)
            after_core(2)
            after_core(3)

        @pl.when(s == 1)
        def _():
            after_second(0)
            after_second(1)

    tiny_core = remote(tiny, tiny_1, send.at[3, 1], recv.at[3, 1], to_core)
    tiny_line = remote(tiny_1, tiny_2, send.at[3, 2], recv.at[3, 2], to_line)
    tiny_over = remote(tiny_2.at[1:3], tiny_x, send.at[3, 3], recv.at[3, 3], to_x)

    tiny_near = remote(tiny_x, tiny_n, send.at[3, 4], recv.at[3, 4], to_near)
    tiny_far = remote(tiny_n, tiny_f, send.at[3, 5], recv.at[3, 5], to_far)

    for g in range(groups):
        column = jnp.sum(qkv_ref[g].astype(F32), 0, keepdims=True)
        tiny[g, 0:1, :width] = column[:, :width]
        tiny[g, 0:1, width : 2 * width] = column[:, 2 * width :]
        tiny[g, 1:2, :] = ubg_ref[g, 0:1, :model]
        tiny[g, 2:3, :] = ubg_ref[g, 0:1, model:]
    tiny[2] = small_ref[...]
    for kind in range(4):
        sent(kind)
    for c in range(3):
        sent(4, c)
        sent(5, c)
    tiny_core.start()

    def products(left, right, first, columns_of):
        for g in range(groups):

            @pl.loop(0, model // block)
            def _(b):
                rows = pl.ds(pl.multiple_of(b * block, block), block)
                made = mm(left[rows, :], right[g, :, columns_of]).astype(BF16)
                up_ref[g, rows, first : first + made.shape[1]] = made

    products(t_low_ref, qkv_ref, 0, slice(0, cut))
    start_core(4)
    after_first(2)
    after_first(3)
    products(t_low_ref, qkv_ref, cut, slice(cut, 3 * width))
    products(t_grad_ref, ctx_ref, 3 * width, slice(None))
    start_core(5)
    tiny_core.wait_recv()
    tiny_1[...] += tiny[...]
    tiny_line.start()
    after_core(4)
    after_x(0)
    after_x(1)
    after_core(5)
    tiny_line.wait_recv()
    tiny_2[...] += tiny_1[...]
    tiny_over.start()
    after_second(2)
    after_second(3)
    for i, (one, own, other) in enumerate(
        ((send_output, out_ref, out_peer_ref), (send_input, in_ref, in_peer_ref))
    ):

        @pl.loop(0, seqs)
        def _(s):
            one(s).wait_recv()
            put_back(s, i, own, other)
            put_out(s, i).start()

    tiny_over.wait_recv()
    tiny_x[0] += tiny_2[0]
    tiny_x[1] += tiny_2[2]
    tiny_near.start()
    after_x(2)
    after_x(3)
    finish(0, rd_ref)
    finish(1, rd_ref)
    after_first(4)
    after_first(5)
    tiny_near.wait_recv()
    tiny_n[...] += tiny_x[...]
    tiny_far.start()
    finish(2, ru_ref)
    finish(3, ru_ref)
    after_second(4)
    after_second(5)
    tiny_far.wait_recv()
    total = tiny_n[...] + tiny_f[...]
    for i in range(3):
        sums_ref[0:1, i * model : (i + 1) * model] = total[0, i : i + 1, :]
    for i in range(6):
        sums_ref[0:1, (3 + i) * model : (4 + i) * model] = total[1, i : i + 1, :]
    after_x(4)
    after_x(5)
    finish(4, ra_ref)
    finish(5, ra_ref)
    for s in range(seqs):
        send_output(s).wait_send()
        send_input(s).wait_send()
        for i in range(2):
            put_out(s, i).wait()
    for t in range(6):
        for block in range(4):
            by_core(t, block).wait_send()
        by_first(t).wait_send()
        by_second(t).wait_send()
        by_x(t).wait_send()
        by_far(t).wait_send()
    tiny_core.wait_send()
    tiny_line.wait_send()
    tiny_over.wait_send()
    tiny_near.wait_send()
    tiny_far.wait_send()


def call(kernel, outs, scratch, flops, *args, scalar=(), far=(), far_out=(), collective=None):
    shapes = [jax.ShapeDtypeStruct(s, d) for s, d in outs]
    moved = sum(a.size * a.dtype.itemsize for a in args) + sum(s.size * s.dtype.itemsize for s in shapes)
    vmem = pl.BlockSpec(memory_space=pltpu.VMEM)
    return pl.pallas_call(
        kernel,
        out_shape=shapes,
        in_specs=[
            pl.BlockSpec(memory_space=pltpu.SMEM if i in scalar else pl.ANY if i in far else pltpu.VMEM)
            for i in range(len(args))
        ],
        out_specs=[pl.BlockSpec(memory_space=pl.ANY) if i in far_out else vmem for i in range(len(shapes))],
        scratch_shapes=[pltpu.VMEM(*s) if isinstance(s, tuple) else s for s in scratch],
        compiler_params=pltpu.CompilerParams(
            vmem_limit_bytes=VMEM_LIMIT, collective_id=collective, has_side_effects=collective is not None
        ),
        cost_estimate=pl.CostEstimate(flops=flops, bytes_accessed=moved, transcendentals=0),
    )(*args)


def factors_of(n):
    found = []
    while n > 4 or (n > 1 and len(found) < 2):
        found.append(2)
        n //= 2
    return found + ([n] if n > 1 else [])


def swap(v):
    return lax.ppermute(v, "mp", [(0, 1), (1, 0)])


def shift_dp(v, n, stride, factor, k):
    def target(d):
        i = (d // stride) % factor
        return d + ((i + k) % factor - i) * stride

    return lax.ppermute(v, "dp", [(d, target(d)) for d in range(n)])


def with_peer(own, n):
    core = lax.axis_index("dp") % 2
    half = own.shape[0] // 2
    mine = swap(lax.dynamic_slice_in_dim(own, core * half, half, 0))
    other = shift_dp(mine, n, 1, 2, 1)
    first = core == 0
    peer = jnp.concatenate([jnp.where(first, mine, other), jnp.where(first, other, mine)], 0)
    return jnp.stack([own, peer])


def reduce_to_owner(grad, n):
    index = lax.axis_index("dp")
    rows = grad.shape[1] // n
    left = grad.reshape(2, n, rows, grad.shape[2])
    stride = 1
    for factor in factors_of(n):
        parts = left.reshape(2, left.shape[1] // factor, factor, rows, left.shape[3])
        i = (index // stride) % factor

        def pick(at):
            return lax.dynamic_index_in_dim(parts, at, 2, keepdims=False)

        total = pick(i).astype(F32)
        for k in range(1, factor):
            total = total + shift_dp(pick((i + k) % factor), n, stride, factor, k).astype(F32)
        left = total.astype(BF16)
        stride *= factor
    left = left.reshape(2, rows, left.shape[3])
    return left[0].astype(F32) + swap(left[1]).astype(F32)


def per_device(
    n, layer_input, doc_lengths, q_weight, q_bias, k_weight, v_weight, v_bias, out_weight, out_bias,
    attn_gain, attn_shift, up_weight, up_bias, down_weight, down_bias, ffn_gain, ffn_shift, cotangent,
):
    rows = doc_lengths.shape[0]
    tokens, model = layer_input.shape
    length = tokens // rows
    part = length // 2
    mine = rows * part
    width = q_weight.shape[1]
    hidden = up_weight.shape[1]
    heads = width // HD
    x_index = lax.axis_index("mp")

    remote = (
        (model // n) % 16 == 0 and n == 16
        and hidden == 2 * model and 4 * width == hidden and hidden % 384 == 0 and rows >= 3 and mine == model
    )
    if remote:
        dma = pltpu.SemaphoreType.DMA
        eighth = model // 8
        layer_output, input_grad, g_down, g_up, g_attn, sums = call(
            functools.partial(whole_layer, n),
            [((tokens, model), BF16)] * 2
            + [((model // n, hidden), F32)] * 3
            + [((1, 6 * model + 2 * width + hidden), F32)],
            [
                ((mine, model), BF16),
                ((mine, model), BF16),
                ((1, 6 * model + 2 * width + hidden), F32),
                ((rows, part, 1), jnp.int32),
                ((rows, 1, part), jnp.int32),
                ((mine, model), BF16),
                ((mine, model), BF16),
                ((mine, model), BF16),
                ((2, model, 3 * width), BF16),
                ((2, width, model), BF16),
                ((2, model, hidden), BF16),
                ((2, hidden, model), BF16),
                ((1, 2 * width + hidden), F32),
                ((2, mine, 3 * width), BF16),
                ((rows, 2 * heads, part, part), BF16),
                ((2, mine, width), BF16),
                ((mine, model), F32),
                ((mine, 1), F32),
                ((mine, model), BF16),
                ((2, model, hidden), BF16),
                ((2, model, hidden), BF16),
                ((mine, model), F32),
                ((model, mine), BF16),
                ((model, mine), BF16),
                ((8, model), F32),
            ]
            + [
                ((6, 2, 2, 2, eighth, model), BF16),
                ((6, 2, 2, eighth, model), BF16),
                ((6, 2, eighth, model), BF16),
                ((6, eighth, model), BF16),
                ((6, model // n, model), BF16),
                ((2, 1, hidden), F32),
                ((3, 8, model), F32),
                ((3, 8, model), F32),
                ((3, 8, model), F32),
                ((2, 8, model), F32),
                ((2, 8, model), F32),
                ((2, 8, model), F32),
                dma((5, 6)), dma((5, 6)), dma((6, 4)), dma((6, 4)), dma((2, rows)), dma((2, rows)),
                dma((4, 10)), dma((4, 10)), dma((6,)), dma((2, 2 * rows)), dma((2, rows)),
            ],
            2 * mine * model * (24 * width + 12 * hidden),
            doc_lengths, layer_input, cotangent,
            q_weight, k_weight, v_weight, out_weight, up_weight, down_weight,
            attn_gain, attn_shift, down_bias, ffn_gain, ffn_shift, out_bias, q_bias, v_bias, up_bias,
            scalar=(0,), far=(1, 2, 3, 4, 5, 6, 7, 8), far_out=(0, 1), collective=0,
        )
        sums = sums[0]
        small = [sums[2 * width + hidden + i * model :][:model] for i in range(6)]
    else:
        ends = jnp.cumsum(doc_lengths, axis=-1, dtype=jnp.int32)
        start = jnp.sum(jnp.where(doc_lengths == part, ends - part, 0), -1)
        place = jnp.arange(length, dtype=jnp.int32)
        segment = jnp.sum((place[None, :, None] >= ends[:, None, :]).astype(jnp.int32), -1, dtype=jnp.int32)
        before = place[None, :part] < start[:, None]
        from_high = before != (x_index == 1)

        def take(v):
            v = v.reshape(rows, 2, part, model)
            return jnp.where(from_high[:, :, None], v[:, 1], v[:, 0]).reshape(mine, model)

        def give(own, other):
            own, other = own.reshape(rows, part, model), other.reshape(rows, part, model)
            low = jnp.where(from_high[:, :, None], other, own)
            high = jnp.where(from_high[:, :, None], own, other)
            return jnp.stack([low, high], 1).reshape(tokens, model)

        seg = jnp.where(from_high, segment[:, part:], segment[:, :part])
        x = take(layer_input)
        cot = take(cotangent)
        own_bias = jnp.concatenate([q_bias, v_bias, up_bias])
        w_qkv = with_peer(jnp.concatenate([q_weight, k_weight, v_weight], 1), n)
        w_out = with_peer(out_weight, n)
        w_up = with_peer(up_weight, n)
        w_down = with_peer(down_weight, n)
        bias = jnp.stack([own_bias, swap(own_bias)]).astype(F32)[:, None, :]
        b_qkv = jnp.concatenate([bias[..., :width], jnp.zeros_like(bias[..., :width]), bias[..., width : 2 * width]], -1)
        b_up = bias[..., 2 * width :]
        vectors = jnp.stack([attn_gain, attn_shift, down_bias, ffn_gain, ffn_shift]).astype(F32)

        qkv, probs, ctx, xhat, rstd, low = call(
            attention_forward,
            [
                ((2, mine, 3 * width), BF16),
                ((rows, 2 * heads, part, part), BF16),
                ((2, mine, width), BF16),
                ((mine, model), F32),
                ((mine, 1), F32),
                ((mine, model), BF16),
            ],
            [],
            2 * mine * model * 8 * width,
            x, w_qkv, b_qkv, w_out, seg[:, :, None], seg[:, None, :],
            out_bias.astype(F32)[None], vectors[0:1], vectors[1:2],
        )
        output, g_down, g_up, d_resid, small, up_bias_grad = call(
            feed_forward,
            [
                ((mine, model), BF16),
                ((2, model, hidden), BF16),
                ((2, model, hidden), BF16),
                ((mine, model), F32),
                ((8, model), F32),
                ((2, 1, hidden), F32),
            ],
            [
                ((2, mine, hidden), BF16),
                ((2, mine, hidden), BF16),
                ((mine, model), F32),
                ((mine, model), BF16),
                ((model, mine), BF16),
                ((model, mine), BF16),
            ],
            2 * mine * model * 2 * hidden * 6,
            low, xhat, rstd, w_up, b_up, w_down, vectors, cot,
        )
        scratch = [((2, mine, 3 * width), BF16), ((model, mine), BF16), ((model, mine), BF16)]
        flops = 2 * mine * model * 16 * width
        output_peer = swap(output)
        grad_in, g_attn, bias_grad = call(
            attention_backward_plain,
            [((mine, model), BF16), ((2, model, 4 * width), BF16), ((2, 1, 3 * width), F32)],
            scratch, flops, x, d_resid, w_qkv, w_out, qkv, probs, ctx,
        )
        grad_in_peer = swap(grad_in)
        g_down, g_up, g_attn = (reduce_to_owner(v, n) for v in (g_down, g_up, g_attn))
        sums = jnp.concatenate([bias_grad[:, 0, :width], bias_grad[:, 0, 2 * width :], up_bias_grad[:, 0]], -1)
        sums = jnp.where(x_index == 0, sums, sums[::-1])
        sums, small = lax.psum((sums, small), ("dp", "mp"))
        sums = lax.dynamic_index_in_dim(sums, x_index, 0, keepdims=False)
        layer_output = give(output, output_peer)
        input_grad = give(grad_in, grad_in_peer)
    down_weight_grad = g_down.T
    up_weight_grad = g_up
    return (
        layer_output,
        input_grad,
        g_attn[:, :width],
        sums[:width],
        g_attn[:, width : 2 * width],
        g_attn[:, 2 * width : 3 * width],
        sums[width : 2 * width],
        g_attn[:, 3 * width :].T,
        small[0],
        small[1],
        small[2],
        up_weight_grad,
        sums[2 * width : 2 * width + hidden],
        down_weight_grad,
        small[3],
        small[4],
        small[5],
    )


def solution(mesh):
    in_specs = (
        P("dp", None), P("dp", None), P(None, "mp"), P("mp"), P(None, "mp"), P(None, "mp"), P("mp"),
        P("mp", None), P(), P(), P(), P(None, "mp"), P("mp"), P("mp", None), P(), P(), P(), P("dp", None),
    )
    out_specs = (
        P("dp", None), P("dp", None), P("dp", "mp"), P("mp"), P("dp", "mp"), P("dp", "mp"), P("mp"),
        P("mp", "dp"), P(), P(), P(), P("dp", "mp"), P("mp"), P("mp", "dp"), P(), P(), P(),
    )
    return jax.shard_map(
        functools.partial(per_device, mesh.shape["dp"]),
        mesh=mesh, in_specs=in_specs, out_specs=out_specs, check_vma=False,
    )
```
